16 devices in a mesh: terms: 16 (over z, y, x, core).
Axes of the slice: x: 2, y: 2, z: 2, core: 2. Of those that a mesh axis runs over, the one named last changes fastest.
Arguments:
- wavefunction: float32 [640, 16, 640], replicated
- left_env: bfloat16 [32, 640, 640], P('terms')
- pair_ops: bfloat16 [32, 16, 16], P('terms')
- right_env: bfloat16 [32, 640, 640], P('terms')
- full_term: int32 [32], P('terms')
Outputs:
- output 1: float32 [7, 640, 16, 640], P(None, 'terms')
- output 2: float32 [6], replicated
- output 3: float32 [6], replicated
All inputs are finite; a program needn't handle non-finite values.
Results may differ from the reference program's by a relative error of at most 0.011385.
Values are sent between devices in bfloat16 or wider.
A program may use at most 1 GiB of HBM per device.

```python
import jax
import jax.numpy as jnp
from jax import lax

BOND_DIM = 640
PHYS_DIM = 4
TERMS_DEV = 2
NUM_DEV = 16
NUM_TERMS = 32
LANCZOS_STEPS = 6

PAIR_DIM = PHYS_DIM * PHYS_DIM
VEC_SIZE = BOND_DIM * PAIR_DIM * BOND_DIM


def normal_sym(rng_key, num_mats, mat_size):
    raw_draw = jax.random.normal(rng_key, (num_mats, mat_size, mat_size), jnp.float32)
    return (raw_draw + jnp.swapaxes(raw_draw, 1, 2)) * (2.0 * mat_size) ** -0.5


def draw_flags(rng_key):
    count_key, pick_key, order_key = jax.random.split(rng_key, 3)
    block_counts = jax.random.randint(count_key, (NUM_DEV,), 0, TERMS_DEV + 1)
    picked = jax.random.permutation(pick_key, NUM_DEV)
    block_counts = block_counts.at[picked[0]].set(TERMS_DEV).at[picked[1]].set(0)
    rank_table = jax.vmap(lambda sub_key: jax.random.permutation(sub_key, TERMS_DEV))(jax.random.split(order_key, NUM_DEV))
    return (rank_table < block_counts[:, None]).astype(jnp.int32).reshape(NUM_TERMS)


def setup_inputs(seed: int = 0) -> dict:
    wave_key, left_key, pair_key, right_key, flag_key = jax.random.split(jax.random.key(seed), 5)
    diag_shift = (2.0 / NUM_TERMS ** 0.5) ** 0.5
    wavefunction = jax.random.normal(wave_key, (BOND_DIM, PAIR_DIM, BOND_DIM), jnp.float32)
    left_env = (normal_sym(left_key, NUM_TERMS, BOND_DIM) + diag_shift * jnp.eye(BOND_DIM, dtype=jnp.float32)).astype(jnp.bfloat16)
    pair_ops = ((normal_sym(pair_key, NUM_TERMS, PAIR_DIM) + diag_shift * jnp.eye(PAIR_DIM, dtype=jnp.float32)) * NUM_TERMS ** -0.5).astype(jnp.bfloat16)
    right_env = normal_sym(right_key, NUM_TERMS, BOND_DIM).astype(jnp.bfloat16)
    full_term = draw_flags(flag_key)
    return {'wavefunction': wavefunction, 'left_env': left_env, 'pair_ops': pair_ops, 'right_env': right_env, 'full_term': full_term}


def apply_term(vec_bf, term_data):
    left_env, pair_op, right_env, flag_val = term_data
    flat_vec = vec_bf.reshape(BOND_DIM * PAIR_DIM, BOND_DIM)
    right_done = jnp.dot(flat_vec, right_env.T, preferred_element_type=jnp.float32).astype(jnp.bfloat16)
    right_done = jnp.where(flag_val == 1, right_done.reshape(BOND_DIM, PAIR_DIM, BOND_DIM), vec_bf)
    pair_in = right_done.transpose(1, 0, 2).reshape(PAIR_DIM, BOND_DIM * BOND_DIM)
    pair_done = jnp.dot(pair_op, pair_in, preferred_element_type=jnp.float32).astype(jnp.bfloat16)
    left_in = pair_done.reshape(PAIR_DIM, BOND_DIM, BOND_DIM).transpose(1, 0, 2).reshape(BOND_DIM, PAIR_DIM * BOND_DIM)
    return jnp.dot(left_env, left_in, preferred_element_type=jnp.float32).reshape(BOND_DIM, PAIR_DIM, BOND_DIM)


def apply_hamiltonian(vector, left_env, pair_ops, right_env, full_term):
    vec_bf = vector.astype(jnp.bfloat16)

    def add_term(running_sum, term_data):
        return running_sum + apply_term(vec_bf, term_data), None

    start_sum = jnp.zeros((BOND_DIM, PAIR_DIM, BOND_DIM), jnp.float32)
    total_sum, unused = lax.scan(add_term, start_sum, (left_env, pair_ops, right_env, full_term))
    return total_sum


def reference(wavefunction, left_env, pair_ops, right_env, full_term):
    first_vec = wavefunction / jnp.sqrt(jnp.sum(wavefunction * wavefunction) / VEC_SIZE)

    def lanczos_step(state_in, unused):
        current, previous, beta_prev = state_in
        sigma_vec = apply_hamiltonian(current, left_env, pair_ops, right_env, full_term)
        alpha_now = jnp.sum(sigma_vec * current) / VEC_SIZE
        residual = sigma_vec - alpha_now * current - beta_prev * previous
        beta_now = jnp.sqrt(jnp.sum(residual * residual) / VEC_SIZE)
        following = residual / beta_now
        return (following, current, beta_now), (following, alpha_now, beta_now)

    start_state = (first_vec, jnp.zeros_like(first_vec), jnp.zeros((), jnp.float32))
    final_state, outputs = lax.scan(lanczos_step, start_state, None, length=LANCZOS_STEPS)
    vectors, alpha_diag, beta_offdiag = outputs
    krylov = jnp.concatenate([first_vec[None], vectors], axis=0)
    return krylov, alpha_diag, beta_offdiag
```

```python
import functools
import jax
import jax.numpy as jnp
from jax import lax
from jax.experimental import pallas as pl
from jax.sharding import PartitionSpec as P
from jax.experimental.pallas import tpu as pltpu

LANCZOS_STEPS = 6
AXIS_NAME = 'terms'
BOND = 640
PAIR = 16
TERMS = 32
DEVS = 16
SLAB = BOND // DEVS
CHUNKS = 5
LANES = 128
VEC_SIZE = BOND * PAIR * BOND
bf = jnp.bfloat16
f32 = jnp.float32
MESH = pl.DeviceIdType.MESH
PART_PAIRS = ((0, 3), (3, 6), (6, 8))
PART_AXES = ((0, 1, 2), (1, 2, 0), (2, 0, 1))


def lanczos_kernel(psi_hbm, rc, wi, left_hbm, krylov, alphas, betas, u, lft, y, zb, acc, cur, prev, ar,
                   load_sem, out_sem, ici_send, ici_recv, d2d_send, d2d_recv, ar_send, ar_recv):
    me = lax.axis_index(AXIS_NAME)
    core = lax.rem(me, 2)
    place = (lax.rem(me // 2, 2), lax.rem(me // 4, 2), me // 8)
    across = tuple(me + (2 << n) * (1 - 2 * place[n]) for n in range(3))
    partner = me + 1 - 2 * core

    def view(ch, pairs, gathered, flipped=None):
        idx = []
        for n in (2, 1, 0):
            if n in gathered:
                idx.append(slice(None))
            elif n == flipped:
                idx.append(1 - place[n])
            else:
                idx.append(place[n])
        return u.at[(ch, slice(pairs[0], pairs[1])) + tuple(idx) + (core,)]

    def remote(ref, dst_ref, send, recv, dev):
        return pltpu.make_async_remote_copy(src_ref=ref, dst_ref=dst_ref, send_sem=send, recv_sem=recv, device_id=(dev,), device_id_type=MESH)

    def ici(ch, part, stage):
        axes = PART_AXES[part]
        ref = view(ch, PART_PAIRS[part], axes[:stage])
        return remote(ref, ref, ici_send.at[ch, part, stage], ici_recv.at[ch, part, stage], across[axes[stage]])

    def ici_in(ch, part, stage):
        axes = PART_AXES[part]
        ref = view(ch, PART_PAIRS[part], axes[:stage], axes[stage])
        return remote(ref, ref, ici_send.at[ch, part, stage], ici_recv.at[ch, part, stage], across[axes[stage]])

    def d2d(ch, part, stage):
        axes = PART_AXES[part]
        ref = view(ch, PART_PAIRS[part], axes[:stage], axes[stage])
        return remote(ref, ref, d2d_send.at[ch, 3 * part + stage], d2d_recv.at[ch, 3 * part + stage], partner)

    def d2d_own(ch):
        ref = view(ch, (0, 8), ())
        return remote(ref, ref, d2d_send.at[ch, 9], d2d_recv.at[ch, 9], partner)

    def first_sends(ch):
        for part in range(3):
            ici(ch, part, 0).start()
        d2d_own(ch).start()

    def forward(ch, stage):
        for part in range(3):
            ici_in(ch, part, stage).wait_recv()
            if stage < 2:
                ici(ch, part, stage + 1).start()
            d2d(ch, part, stage).start()

    def chunk_ready(ch):
        for part in range(3):
            for stage in range(3):
                d2d(ch, part, stage).wait_recv()
        d2d_own(ch).wait_recv()

    def drain_sends(ch):
        for part in range(3):
            for stage in range(3):
                ici(ch, part, stage).wait_send()
                d2d(ch, part, stage).wait_send()
        d2d_own(ch).wait_send()

    def all_sum(which, partial):
        ar[which, me] = partial
        for off in range(1, DEVS):
            dev = lax.rem(me + off, DEVS)
            ref = ar.at[which, me]
            remote(ref, ref, ar_send.at[which, off], ar_recv.at[which, me], dev).start()
        for off in range(1, DEVS):
            dev = lax.rem(me + off, DEVS)
            ref = ar.at[which, dev]
            remote(ref, ref, ar_send.at[which, off], ar_recv.at[which, dev], dev).wait_recv()
        total = jnp.sum(jnp.sum(ar[which], axis=0))
        for off in range(1, DEVS):
            dev = lax.rem(me + off, DEVS)
            ref = ar.at[which, me]
            remote(ref, ref, ar_send.at[which, off], ar_recv.at[which, me], dev).wait_send()
        return total

    def fold(vals):
        return jnp.sum(vals.reshape(80, 8, 5, 128).transpose(0, 2, 1, 3).reshape(400, 8, 128), axis=0)

    def dot_rows(fn):
        def body(g, tot):
            rows = pl.ds(pl.multiple_of(g * 16, 16), 16)
            val = fn(rows)
            for r in range(2):
                for c in range(5):
                    tot = tot + val[8 * r:8 * r + 8, 128 * c:128 * c + 128]
            return tot
        return lax.fori_loop(0, 40, body, jnp.zeros((8, 128), f32))

    def write_u():
        for ch in range(CHUNKS):
            lanes = slice(128 * ch, 128 * ch + 128)
            for i in range(8):
                dst = u.at[ch, i, place[2], place[1], place[0], core]
                dst[0:16] = cur[32 * i:32 * i + 16, lanes].astype(bf)
                dst[16:32] = cur[256 + 32 * i:256 + 32 * i + 16, lanes].astype(bf)
                dst[32:48] = cur[32 * i + 16:32 * i + 32, lanes].astype(bf)
                dst[48:64] = cur[256 + 32 * i + 16:256 + 32 * i + 32, lanes].astype(bf)
                dst[64:80] = cur[512 + 16 * i:512 + 16 * i + 16, lanes].astype(bf)

    def right_phase(ch):
        @pl.loop(0, 2)
        def _(g):
            for par in range(2):
                rhs = []
                for n in range(4):
                    i = g * 4 + n
                    a = u[ch, i, :, :, :, :, 32 * par:32 * par + 32, :].reshape(512, 128)
                    m = u[ch, i, :, :, :, :, 64:80, :].reshape(256, 128)
                    rhs.append(jnp.concatenate([a, m], axis=0))
                rhs = jnp.concatenate(rhs, axis=1)
                lhs = jnp.concatenate([rc[:, 0:512], rc[:, 512 + 256 * par:768 + 256 * par]], axis=1)
                o = jnp.dot(lhs, rhs, preferred_element_type=f32).astype(bf)
                for n in range(4):
                    y[2 * (g * 4 + n) + par] = o[:, 128 * n:128 * n + 128]

    def pair_left_phase(ch, groups):
        @pl.loop(*groups)
        def _(kg):
            for s in range(2):
                k = kg * 2 + s
                row = pl.multiple_of(k * 80, 16)
                tile = [y[:, pl.ds(row + 16 * t, 16), :].reshape(256, 128) for t in range(5)]
                z01 = jnp.dot(wi[k, 0], jnp.concatenate([tile[0], tile[1]], axis=1), preferred_element_type=f32).astype(bf)
                z2 = jnp.dot(wi[k, 1], tile[2], preferred_element_type=f32).reshape(16, 2, 8, 128)
                z34 = jnp.dot(wi[k, 2], jnp.concatenate([tile[3], tile[4]], axis=1), preferred_element_type=f32).astype(bf)
                zb[s, 0:256, 0:128] = z01[:, 0:128]
                zb[s, 256:512, 0:128] = z01[:, 128:256]
                zb[s, 512:640, 0:128] = z2[:, 0].reshape(128, 128).astype(bf)
                zb[s, 0:256, 128:256] = z34[:, 0:128]
                zb[s, 256:512, 128:256] = z34[:, 128:256]
                zb[s, 512:640, 128:256] = z2[:, 1].reshape(128, 128).astype(bf)
            lhs = jnp.concatenate([zb[0], zb[1]], axis=1)
            c0 = pl.multiple_of(ch * 128, 128)
            rhs = jnp.concatenate([lft[kg * 4 + n, pl.ds(c0, 128), :] for n in range(4)], axis=0)
            acc[...] += jnp.dot(lhs, rhs, preferred_element_type=f32)

    left_load = pltpu.make_async_copy(left_hbm, lft, load_sem.at[0])
    left_load.start()
    psi_load = pltpu.make_async_copy(psi_hbm, cur, load_sem.at[1])
    psi_load.start()
    barrier = pltpu.get_barrier_semaphore()
    for off in range(1, DEVS):
        pl.semaphore_signal(barrier, inc=1, device_id=(lax.rem(me + off, DEVS),), device_id_type=MESH)
    pl.semaphore_wait(barrier, DEVS - 1)
    psi_load.wait()
    norm = jnp.sqrt(all_sum(1, dot_rows(lambda rows: cur[rows, :] * cur[rows, :])) / VEC_SIZE)
    betas[0, LANCZOS_STEPS] = norm
    prev[...] = jnp.zeros_like(prev)

    @pl.loop(0, 40)
    def _(g):
        rows = pl.ds(pl.multiple_of(g * 16, 16), 16)
        cur[rows, :] = cur[rows, :] / norm

    write_u()
    left_load.wait()

    def step(j, beta_prev):
        acc[...] = jnp.zeros_like(acc)
        first_sends(0)
        first_sends(1)
        forward(0, 0)
        first_sends(2)
        forward(0, 1)
        forward(1, 0)
        forward(0, 2)
        chunk_ready(0)

        @pl.loop(0, CHUNKS)
        def _(ch):
            @pl.when(ch + 1 < CHUNKS)
            def _():
                forward(ch + 1, 1)

            @pl.when(ch + 2 < CHUNKS)
            def _():
                forward(ch + 2, 0)

            @pl.when(ch + 3 < CHUNKS)
            def _():
                first_sends(ch + 3)

            right_phase(ch)
            pair_left_phase(ch, (0, 4))

            @pl.when(ch + 1 < CHUNKS)
            def _():
                forward(ch + 1, 2)

            pair_left_phase(ch, (4, 8))

            @pl.when(ch + 1 < CHUNKS)
            def _():
                chunk_ready(ch + 1)

        @pl.loop(0, CHUNKS)
        def _(ch):
            drain_sends(ch)

        alpha = all_sum(0, dot_rows(lambda rows: acc[rows, :] * cur[rows, :])) / VEC_SIZE

        def residual(rows):
            w = acc[rows, :] - alpha * cur[rows, :] - beta_prev * prev[rows, :]
            acc[rows, :] = w
            return w * w

        beta = jnp.sqrt(all_sum(1, dot_rows(residual)) / VEC_SIZE)
        alphas[0, j] = alpha
        betas[0, j] = beta

        @pl.when(j > 0)
        def _():
            pltpu.make_async_copy(cur, krylov.at[0], out_sem).wait()

        @pl.loop(0, 40)
        def _(g):
            rows = pl.ds(pl.multiple_of(g * 16, 16), 16)
            prev[rows, :] = cur[rows, :]
            cur[rows, :] = acc[rows, :] / beta

        pltpu.make_async_copy(cur, krylov.at[j], out_sem).start()

        @pl.when(j + 1 < LANCZOS_STEPS)
        def _():
            write_u()

        return beta

    lax.fori_loop(0, LANCZOS_STEPS, step, jnp.zeros((), f32))
    pltpu.make_async_copy(cur, krylov.at[0], out_sem).wait()


def run_lanczos(psi_slab, rc, wi, left_all):
    vmem = pl.BlockSpec(memory_space=pltpu.VMEM)
    smem = pl.BlockSpec(memory_space=pltpu.SMEM)
    hbm = pl.BlockSpec(memory_space=pltpu.HBM)
    dma = pltpu.SemaphoreType.DMA
    return pl.pallas_call(
        lanczos_kernel,
        out_shape=(jax.ShapeDtypeStruct((LANCZOS_STEPS, BOND, BOND), f32), jax.ShapeDtypeStruct((1, 8), f32), jax.ShapeDtypeStruct((1, 8), f32)),
        in_specs=[hbm, vmem, vmem, hbm],
        out_specs=(hbm, smem, smem),
        scratch_shapes=[
            pltpu.VMEM((CHUNKS, 8, 2, 2, 2, 2, 80, LANES), bf),
            pltpu.VMEM((TERMS, BOND, BOND), bf),
            pltpu.VMEM((PAIR, TERMS * SLAB, LANES), bf),
            pltpu.VMEM((2, BOND, 256), bf),
            pltpu.VMEM((BOND, BOND), f32),
            pltpu.VMEM((BOND, BOND), f32),
            pltpu.VMEM((BOND, BOND), f32),
            pltpu.VMEM((2, DEVS, 8, 128), f32),
            dma((2,)), dma, dma((CHUNKS, 3, 3)), dma((CHUNKS, 3, 3)), dma((CHUNKS, 10)), dma((CHUNKS, 10)),
            dma((2, DEVS)), dma((2, DEVS)),
        ],
        compiler_params=pltpu.CompilerParams(collective_id=0, has_side_effects=True, vmem_limit_bytes=67043328),
    )(psi_slab, rc, wi, left_all)


def slab_rows(arr):
    lead = arr.shape[:-3]
    parts = []
    for lo, hi in ((0, 16), (16, 32), (32, 40)):
        parts.append(arr[..., :, lo:hi, :].reshape(lead + (PAIR * (hi - lo), arr.shape[-1])))
    return jnp.concatenate(parts, axis=-2)


def slab_unrows(arr):
    lead = arr.shape[:-2]
    last = arr.shape[-1]
    parts = []
    for row, size in ((0, 16), (256, 16), (512, 8)):
        parts.append(arr[..., row:row + PAIR * size, :].reshape(lead + (PAIR, size, last)))
    return jnp.concatenate(parts, axis=-2)


def solution(mesh):
    def device_body(wavefunction, left_loc, pair_loc, right_loc, flag_loc):
        me = lax.axis_index(AXIS_NAME)
        left_all = lax.all_gather(left_loc, AXIS_NAME, axis=0, tiled=True)
        pair_all = lax.all_gather(pair_loc, AXIS_NAME, axis=0, tiled=True)
        flags = lax.all_gather(flag_loc, AXIS_NAME, axis=0, tiled=True)
        right_slab = lax.all_to_all(right_loc, AXIS_NAME, split_axis=1, concat_axis=0, tiled=True)
        cols = me * SLAB + jnp.arange(SLAB)
        ident = (cols[:, None] == jnp.arange(BOND)[None, :]).astype(bf)
        right_slab = jnp.where(flags[:, None, None] == 1, right_slab, ident[None])
        by_src = right_slab.reshape(TERMS, SLAB, DEVS, SLAB)
        main = by_src[..., :32].reshape(TERMS, SLAB, 512)
        tail = by_src[..., 32:]
        zero = jnp.zeros_like(tail)
        even = jnp.concatenate([tail, zero], axis=-1).reshape(TERMS, SLAB, 256)
        odd = jnp.concatenate([zero, tail], axis=-1).reshape(TERMS, SLAB, 256)
        cat = jnp.concatenate([main, even, odd], axis=-1).reshape(TERMS // 2, 2, SLAB, 1024)
        rc = jnp.concatenate([cat[:, 0], cat[:, 1, 32:], cat[:, 1, :32]], axis=1).reshape(TERMS * SLAB, 1024)
        eye = jnp.eye(16, dtype=bf)
        expand = (pair_all[:, :, None, :, None] * eye[None, None, :, None, :]).reshape(TERMS // 2, 2, 256, 256)
        low = (jnp.arange(256) % 16 < 8)[None, :, None]
        wi = jnp.stack([expand[:, 0], jnp.where(low, expand[:, 0], expand[:, 1]), expand[:, 1]], axis=1)
        psi_slab = lax.dynamic_slice_in_dim(wavefunction, me * SLAB, SLAB, axis=2)
        psi_slab = slab_rows(psi_slab.transpose(1, 2, 0))
        vecs, alphas, betas = run_lanczos(psi_slab, rc, wi, left_all)
        norm = betas[0, LANCZOS_STEPS]
        first = lax.dynamic_slice_in_dim(wavefunction, me * SLAB, SLAB, axis=0) / norm
        vecs = slab_unrows(vecs)
        vecs = lax.all_to_all(vecs, AXIS_NAME, split_axis=3, concat_axis=2, tiled=True)
        vecs = vecs.transpose(0, 3, 1, 2)
        krylov = jnp.concatenate([first[None], vecs], axis=0)
        return krylov, alphas[0, :LANCZOS_STEPS], betas[0, :LANCZOS_STEPS]

    return jax.shard_map(device_body, mesh=mesh, in_specs=(P(), P(AXIS_NAME), P(AXIS_NAME), P(AXIS_NAME), P(AXIS_NAME)), out_specs=(P(None, AXIS_NAME), P(), P()), check_vma=False)
```

```python
import functools
import jax
import jax.numpy as jnp
from jax import lax
from jax.experimental import pallas as pl
from jax.sharding import PartitionSpec as P
from jax.experimental.pallas import tpu as pltpu

LANCZOS_STEPS = 6
AXIS_NAME = 'terms'
BOND = 640
PAIR = 16
TERMS = 32
DEVS = 16
SLAB = BOND // DEVS
CHUNKS = 5
LANES = 128
VEC_SIZE = BOND * PAIR * BOND
bf = jnp.bfloat16
f32 = jnp.float32
MESH = pl.DeviceIdType.MESH
PART_PAIRS = ((0, 3), (3, 6), (6, 8))
LEFT_ROWS = (((0, 48), (48, 96), (96, 128)), ((0, 32), (32, 80), (80, 128)), ((0, 48), (48, 80), (80, 128)))
D2D_FLIPS = ((0,), (1,), (2,), (0, 1), (0, 2), (1, 2), (0, 1, 2), ())
PART_AXES = ((0, 1, 2), (1, 2, 0), (2, 0, 1))


def lanczos_kernel(flags, psi, psi_rows, left_hbm, pair_hbm, right_hbm, gathered, alphas, betas,
                   u, lft, y, acc, cur, prev, ar, rc, wi, ops,
                   load_sem, stage_sem, own_sem, ici_send, ici_recv, d2d_send, d2d_recv, ar_send, ar_recv, out_send, out_recv, op_send, op_recv):
    me = lax.axis_index(AXIS_NAME)
    core = lax.rem(me, 2)
    place = (lax.rem(me // 2, 2), lax.rem(me // 4, 2), me // 8)
    across = tuple(me + (2 << n) * (1 - 2 * place[n]) for n in range(3))
    partner = me + 1 - 2 * core

    def slots(flips):
        return tuple(1 - place[n] if n in flips else place[n] for n in (2, 1, 0)) + (core,)

    def vec_view(ch, part, flips):
        pairs = PART_PAIRS[part] if part < 3 else (0, 8)
        return u.at[(ch, slice(pairs[0], pairs[1])) + slots(flips)]

    def left_view(ch, part, flips):
        lo, hi = LEFT_ROWS[ch % 3][part] if part < 3 else (0, 128)
        return lft.at[slots(flips) + (slice(None), slice(128 * ch + lo, 128 * ch + hi), slice(128 * ch, BOND))]

    def remote(ref, dst_ref, send, recv, dev):
        return pltpu.make_async_remote_copy(src_ref=ref, dst_ref=dst_ref, send_sem=send, recv_sem=recv, device_id=(dev,), device_id_type=MESH)

    def unit(view, ch, part, n, arriving=False):
        first, second, third = PART_AXES[part]
        flips, axis = (((), first), ((), second), ((), third), ((first,), second), ((first,), third), ((second,), third), ((first, second), third))[n]
        ref = view(ch, part, flips + (axis,) if arriving else flips)
        return remote(ref, ref, ici_send.at[ch, part, n], ici_recv.at[ch, part, n], across[axis])

    def start_units(view, ch, *which):
        for n in which:
            for part in range(3):
                unit(view, ch, part, n).start()

    def wait_units(view, ch, *which):
        for n in which:
            for part in range(3):
                unit(view, ch, part, n, True).wait_recv()

    def d2d(view, ch, n):
        ref = view(ch, 3, D2D_FLIPS[n])
        return remote(ref, ref, d2d_send.at[ch, n], d2d_recv.at[ch, n], partner)

    def own_out(view, ch):
        start_units(view, ch, 0, 1, 2)
        d2d(view, ch, 7).start()

    def relay_first(view, ch):
        for part in range(3):
            unit(view, ch, part, 0, True).wait_recv()
            unit(view, ch, part, 3).start()
        start_units(view, ch, 4)

    def relay_second(view, ch):
        for part in range(3):
            unit(view, ch, part, 1, True).wait_recv()
            unit(view, ch, part, 5).start()

    def relay_third(view, ch):
        wait_units(view, ch, 2)
        for n in (0, 1, 2):
            d2d(view, ch, n).start()

    def relay_last(view, ch):
        for part in range(3):
            unit(view, ch, part, 3, True).wait_recv()
            unit(view, ch, part, 6).start()

    def take_pairs(view, ch):
        wait_units(view, ch, 4, 5)
        for n in (3, 4, 5):
            d2d(view, ch, n).start()

    def take_last(view, ch):
        wait_units(view, ch, 6)
        d2d(view, ch, 6).start()

    def chunk_ready(view, ch):
        for n in range(8):
            d2d(view, ch, n).wait_recv()

    def drain_sends(view, ch):
        for n in range(8):
            d2d(view, ch, n).wait_send()
        for n in range(7):
            for part in range(3):
                unit(view, ch, part, n).wait_send()

    def for_left(ch, what):
        for c in range(CHUNKS):
            @pl.when(ch == c)
            def _():
                what(left_view, c)

    def send_partial(which, partial):
        ar[which, me] = partial
        for off in range(1, DEVS):
            dev = lax.rem(me + off, DEVS)
            ref = ar.at[which, me]
            remote(ref, ref, ar_send.at[which, off], ar_recv.at[which, me], dev).start()

    def total_of(which):
        for off in range(1, DEVS):
            dev = lax.rem(me + off, DEVS)
            ref = ar.at[which, dev]
            remote(ref, ref, ar_send.at[which, off], ar_recv.at[which, dev], dev).wait_recv()
        total = jnp.sum(jnp.sum(ar[which], axis=0))
        for off in range(1, DEVS):
            dev = lax.rem(me + off, DEVS)
            ref = ar.at[which, me]
            remote(ref, ref, ar_send.at[which, off], ar_recv.at[which, me], dev).wait_send()
        return total

    def all_sum(which, partial):
        send_partial(which, partial)
        return total_of(which)

    def dot_rows(fn):
        def body(g, tot):
            rows = pl.ds(pl.multiple_of(g * 16, 16), 16)
            val = fn(rows)
            for r in range(2):
                for c in range(5):
                    tot = tot + val[8 * r:8 * r + 8, 128 * c:128 * c + 128]
            return tot
        return lax.fori_loop(0, 40, body, jnp.zeros((8, 128), f32))

    def write_u():
        for ch in range(CHUNKS):
            lanes = slice(128 * ch, 128 * ch + 128)
            for i in range(8):
                dst = u.at[ch, i, place[2], place[1], place[0], core]
                dst[0:16] = cur[32 * i:32 * i + 16, lanes].astype(bf)
                dst[16:32] = cur[256 + 32 * i:256 + 32 * i + 16, lanes].astype(bf)
                dst[32:48] = cur[32 * i + 16:32 * i + 32, lanes].astype(bf)
                dst[48:64] = cur[256 + 32 * i + 16:256 + 32 * i + 32, lanes].astype(bf)
                dst[64:80] = cur[512 + 16 * i:512 + 16 * i + 16, lanes].astype(bf)

    def right_phase(ch, middle):
        for par in range(2):
            if par == 1:
                middle()
            rhs = []
            for i in range(8):
                main = u[ch, i, :, :, :, :, 32 * par:32 * par + 32, :].reshape(512, 128)
                tail = u[ch, i, :, :, :, :, 64:80, :].reshape(256, 128)
                rhs.append(jnp.concatenate([main, tail], axis=0))
            rhs = jnp.concatenate(rhs, axis=1)
            lhs = jnp.concatenate([rc[:, 0:512], rc[:, 512 + 256 * par:768 + 256 * par]], axis=1)
            val = jnp.dot(lhs, rhs, preferred_element_type=f32).astype(bf)
            for i in range(8):
                y[2 * i + par] = val[:, 128 * i:128 * i + 128]

    def pair_left_phase(ch, zb, half_done):
        low_rows = (iota((256, 256), 0) & 15) < 8

        @pl.loop(0, 2)
        def _(g):
            for s in range(8):
                k = g * 8 + s
                row = pl.multiple_of(k * 80, 16)
                tile = [y[:, pl.ds(row + 16 * t, 16), :].reshape(256, 128) for t in range(5)]
                z01 = jnp.dot(wi[k, 0], jnp.concatenate([tile[0], tile[1]], axis=1), preferred_element_type=f32).astype(bf)
                mixed = jnp.where(low_rows, wi[k, 0], wi[k, 1])
                z2 = jnp.dot(mixed, tile[2], preferred_element_type=f32).reshape(16, 2, 8, 128)
                z34 = jnp.dot(wi[k, 1], jnp.concatenate([tile[3], tile[4]], axis=1), preferred_element_type=f32).astype(bf)
                zb[s, 0:256, 0:128] = z01[:, 0:128]
                zb[s, 256:512, 0:128] = z01[:, 128:256]
                zb[s, 512:640, 0:128] = z2[:, 0].reshape(128, 128).astype(bf)
                zb[s, 0:256, 128:256] = z34[:, 0:128]
                zb[s, 256:512, 128:256] = z34[:, 128:256]
                zb[s, 512:640, 128:256] = z2[:, 1].reshape(128, 128).astype(bf)
            lhs = jnp.concatenate([zb[s] for s in range(8)], axis=1)
            rows = pl.ds(pl.multiple_of(ch * 128, 128), 128)
            rhs = jnp.concatenate([lft[g, s // 4, s // 2 % 2, s % 2, t, rows, :] for s in range(8) for t in range(2)], axis=0)
            acc[...] += jnp.dot(lhs, rhs, preferred_element_type=f32)

            @pl.when(g == 0)
            def _():
                half_done()

    def turn(turned):
        for lt in range(5):
            rows = []
            for n in range(16 * lt, 16 * lt + 16):
                q, part = n // 5, n % 5
                start = 512 + 8 * q if part == 4 else 256 * (part // 2) + 16 * q + 8 * (part % 2)
                rows.append(cur[start:start + 8, :])
            turned[:, 128 * lt:128 * lt + 128] = jnp.concatenate(rows, axis=0).T

    def flipped(mask):
        dev = me
        for n, bit in enumerate((core,) + place):
            if mask >> n & 1:
                dev = dev + (1 << n) * (1 - 2 * bit)
        return dev

    def out_copy(turned, vec, mask, arriving=False):
        dev = flipped(mask)
        src = dev if arriving else me
        rows = pl.ds(pl.multiple_of(dev * SLAB, 8), SLAB)
        return remote(turned.at[rows], gathered.at[vec, src], out_send.at[mask], out_recv.at[mask], dev)

    def own_copy(turned, vec):
        rows = pl.ds(pl.multiple_of(me * SLAB, 8), SLAB)
        return pltpu.make_async_copy(turned.at[rows], gathered.at[vec, me], own_sem)

    def send_out(turned, vec, masks):
        for mask in masks:
            out_copy(turned, vec, mask).start()

    def finish_out(turned, vec):
        own_copy(turned, vec).wait()
        for mask in range(1, DEVS):
            out_copy(turned, vec, mask, True).wait_recv()
        for mask in range(1, DEVS):
            out_copy(turned, vec, mask).wait_send()

    def iota(shape, dim):
        return lax.broadcasted_iota(jnp.int32, shape, dim)

    def op_copy(which, src_ref, dst_ref, off, dev, src):
        return remote(src_ref, dst_ref, op_send.at[which, off], op_recv.at[which, src], dev)

    def pair_copy(off, dev, src):
        return op_copy(0, ops.at[src], ops.at[src], off, dev, src)

    def right_copy(off, dev, src):
        rows = pl.ds(pl.multiple_of(dev * 80, 16), 80)
        into = pl.ds(pl.multiple_of(src * 80, 16), 80)
        return op_copy(1, y.at[5:10, rows], y.at[10:15, into], off, dev, src)

    def spread_right():
        col = iota((BOND, 128), 0)
        source = (col * 1639) >> 16
        within = col - source * SLAB
        target = jnp.where(within < 32, source * 32 + within, 480 + source * 8 + within)
        for t in range(5):
            perm = (target == iota((BOND, 128), 1) + 128 * t).astype(f32)
            for k in range(2):
                rows = jnp.concatenate([y[n, BOND * k:BOND * k + BOND, :] for n in range(5)], axis=1)
                val = jnp.dot(rows, perm.astype(bf), preferred_element_type=f32)
                val = jnp.where(flags[k] == 1, val, perm)
                val = val.reshape(DEVS, SLAB, 128)
                if k == 0:
                    first = val
            both_terms = jnp.concatenate([first, val[:, 32:], val[:, :32]], axis=1)
            y[5 + t] = both_terms.reshape(2 * BOND, 128).astype(bf)

    def build_right():
        rc[:, 0:512] = jnp.concatenate([y[10 + n] for n in range(4)], axis=1)
        src = iota((128, 256), 0)
        spot = 16 * (src >> 3) + (src & 7)
        for par in range(2):
            widen = (spot + 8 * par == iota((128, 256), 1)).astype(bf)
            rc[:, 512 + 256 * par:768 + 256 * par] = jnp.dot(y[14], widen, preferred_element_type=f32).astype(bf)

    def build_pairs():
        widen = ((iota((128, 256), 1) >> 4) == iota((128, 256), 0)).astype(bf)
        same = (iota((256, 256), 0) & 15) == (iota((256, 256), 1) & 15)

        @pl.loop(0, DEVS)
        def _(k):
            wide = []
            for t in range(2):
                tall = jnp.broadcast_to(ops[k, t].astype(f32)[:, None, :], (16, 16, 128)).reshape(256, 128).astype(bf)
                wide.append(jnp.where(same, jnp.dot(tall, widen, preferred_element_type=f32), 0.0))
            wi[k, 0] = wide[0].astype(bf)
            wi[k, 1] = wide[1].astype(bf)

    def tile_load(stage, t, ch, half):
        rows, qs = pl.ds(pl.multiple_of(128 * ch, 128), 128), pl.ds(pl.multiple_of(8 * half, 8), 8)
        return pltpu.make_async_copy(psi.at[rows, qs, 128 * t:128 * t + 128], stage.at[t], stage_sem.at[t])

    def start_vector(norm, stage, flip):
        base = (me * SLAB) // 128
        skip = pl.multiple_of(me * SLAB - base * 128, 8)
        for t in range(5):
            tile_load(stage, t, 0, 0).start()

        @pl.loop(0, 2 * CHUNKS)
        def _(it):
            ch, half = it // 2, lax.rem(it, 2)
            for t in range(5):
                tile_load(stage, t, ch, half).wait()
            lanes = pl.ds(pl.multiple_of(128 * ch, 128), 128)

            @pl.when(it == 4)
            def _():
                relay_first(left_view, 0)
                relay_second(left_view, 0)
                relay_third(left_view, 0)

            for q in range(8):
                for t in range(2):
                    flip[q, 128 * t:128 * t + 128, :] = stage[jnp.minimum(base + t, 4), :, q, :].T
                val = flip[q, pl.ds(skip, SLAB), :] / norm
                row = 128 * half + 16 * q
                for start, piece, size in ((row, 0, 16), (256 + row, 16, 16), (512 + 64 * half + 8 * q, 32, 8)):
                    cur[pl.ds(pl.multiple_of(start, 8), size), lanes] = val[piece:piece + size, :]
            for t in range(5):
                for q in range(8):
                    val = (stage[t, :, q, :].T / norm).astype(bf)
                    for m in range(16):
                        src, piece = (16 * t + m) // 5, (16 * t + m) % 5
                        row = 64 + 8 * (q % 2) if piece == 4 else 32 * (q % 2) + 8 * piece
                        u[ch, 4 * half + q // 2, src // 8, src // 4 % 2, src // 2 % 2, src % 2, row:row + 8, :] = val[8 * m:8 * m + 8, :]

                @pl.when(it + 1 < 2 * CHUNKS)
                def _():
                    tile_load(stage, t, (it + 1) // 2, lax.rem(it + 1, 2)).start()

    def mirror_left(ch):
        @pl.loop(0, 8)
        def _(g):
            for n in range(4):
                at = (g // 4, lax.rem(g // 2, 2), lax.rem(g, 2), n // 2, n % 2)
                for other in range(ch + 1, CHUNKS):
                    block = lft[at + (slice(128 * ch, 128 * ch + 128), slice(128 * other, 128 * other + 128))]
                    lft[at + (slice(128 * other, 128 * other + 128), slice(128 * ch, 128 * ch + 128))] = block.T

    left_load = pltpu.make_async_copy(left_hbm, lft.at[place[2], place[1], place[0], core], load_sem.at[0])
    slab_load = pltpu.make_async_copy(psi_rows.at[pl.ds(pl.multiple_of(me * BOND, 8), BOND)], cur, load_sem.at[1])
    pair_load = pltpu.make_async_copy(pair_hbm, ops.at[me], load_sem.at[2])
    right_load = [pltpu.make_async_copy(right_hbm.at[:, 128 * n:128 * n + 128], y.at[n], load_sem.at[3 + n]) for n in range(5)]
    pair_load.start()
    slab_load.start()
    for load in right_load:
        load.start()
    left_load.start()
    barrier = pltpu.get_barrier_semaphore()
    for off in range(1, DEVS):
        pl.semaphore_signal(barrier, inc=1, device_id=(lax.rem(me + off, DEVS),), device_id_type=MESH)
    pl.semaphore_wait(barrier, DEVS - 1)
    pair_load.wait()
    for off in range(1, DEVS):
        pair_copy(off, lax.rem(me + off, DEVS), me).start()
    slab_load.wait()
    send_partial(1, dot_rows(lambda rows: cur[rows, :] * cur[rows, :]))
    for load in right_load:
        load.wait()
    spread_right()
    left_load.wait()
    own_out(left_view, 0)
    for off in range(1, DEVS):
        right_copy(off, lax.rem(me + off, DEVS), me).start()
    own = pl.ds(pl.multiple_of(me * 80, 16), 80)
    y[10:15, own] = y[5:10, own]
    norm = jnp.sqrt(total_of(1) / VEC_SIZE)
    betas[0, LANCZOS_STEPS] = norm
    pl.run_scoped(functools.partial(start_vector, norm), pltpu.VMEM((5, 128, 8, LANES), f32), pltpu.VMEM((8, 256, LANES), f32))
    for off in range(1, DEVS):
        dev = lax.rem(me + off, DEVS)
        pair_copy(off, dev, dev).wait_recv()
    build_pairs()
    for off in range(1, DEVS):
        dev = lax.rem(me + off, DEVS)
        rows = pl.ds(pl.multiple_of(dev * 80, 16), 80)
        op_copy(1, y.at[5:10, rows], y.at[10:15, rows], off, dev, dev).wait_recv()
    build_right()
    relay_last(left_view, 0)
    own_out(left_view, 1)
    for off in range(1, DEVS):
        dev = lax.rem(me + off, DEVS)
        pair_copy(off, dev, me).wait_send()
        right_copy(off, dev, me).wait_send()
    prev[...] = jnp.zeros_like(prev)

    def step(zb, turned, j, beta_prev):
        acc[...] = jnp.zeros_like(acc)

        later = j > 0

        @pl.when(later)
        def _():
            own_out(vec_view, 0)
            turn(turned)
            own_copy(turned, j - 1).start()
            relay_first(vec_view, 0)
            relay_second(vec_view, 0)
            relay_last(vec_view, 0)
            own_out(vec_view, 1)
            relay_third(vec_view, 0)
            take_pairs(vec_view, 0)
            take_last(vec_view, 0)
            chunk_ready(vec_view, 0)

        @pl.loop(0, CHUNKS)
        def _(ch):
            @pl.when(later & (ch + 1 < CHUNKS))
            def _():
                relay_first(vec_view, ch + 1)

            def middle():
                @pl.when(later & (ch + 1 < CHUNKS))
                def _():
                    relay_second(vec_view, ch + 1)

            right_phase(ch, middle)

            @pl.when(later & (ch + 1 < CHUNKS))
            def _():
                relay_third(vec_view, ch + 1)
                relay_last(vec_view, ch + 1)

                @pl.when(ch + 2 < CHUNKS)
                def _():
                    own_out(vec_view, ch + 2)

                @pl.when(ch == 3)
                def _():
                    send_out(turned, j - 1, (1, 3, 5, 9, 14, 15))

            @pl.when(later & (ch == 4))
            def _():
                send_out(turned, j - 1, (7, 13, 11))

            @pl.when(j == 0)
            def _():
                def left_ready(view, c):
                    take_pairs(view, c)
                    take_last(view, c)
                    chunk_ready(view, c)
                    mirror_left(c)

                for_left(ch, left_ready)
                for_left(ch + 1, relay_first)

            def half_done():
                @pl.when(later & (ch + 1 < CHUNKS))
                def _():
                    take_pairs(vec_view, ch + 1)
                    take_last(vec_view, ch + 1)

                    @pl.when(ch == 2)
                    def _():
                        send_out(turned, j - 1, (2, 4, 8))

                    @pl.when(ch == 3)
                    def _():
                        send_out(turned, j - 1, (6, 12, 10))

                @pl.when(j == 0)
                def _():
                    for_left(ch + 1, relay_second)

            pair_left_phase(ch, zb, half_done)

            @pl.when(later & (ch + 1 < CHUNKS))
            def _():
                chunk_ready(vec_view, ch + 1)

            @pl.when(j == 0)
            def _():
                def advance(view, c):
                    relay_third(view, c)
                    relay_last(view, c)

                for_left(ch + 1, advance)
                for_left(ch + 2, own_out)

        @pl.loop(0, CHUNKS)
        def _(ch):
            @pl.when(j == 0)
            def _():
                for_left(ch, drain_sends)

            @pl.when(later)
            def _():
                drain_sends(vec_view, ch)

        @pl.when(later)
        def _():
            finish_out(turned, j - 1)

        alpha = all_sum(0, dot_rows(lambda rows: acc[rows, :] * cur[rows, :])) / VEC_SIZE

        def residual(rows):
            w = acc[rows, :] - alpha * cur[rows, :] - beta_prev * prev[rows, :]
            acc[rows, :] = w
            return w * w

        beta = jnp.sqrt(all_sum(1, dot_rows(residual)) / VEC_SIZE)
        alphas[0, j] = alpha
        betas[0, j] = beta

        @pl.loop(0, 40)
        def _(g):
            rows = pl.ds(pl.multiple_of(g * 16, 16), 16)
            prev[rows, :] = cur[rows, :]
            cur[rows, :] = acc[rows, :] / beta

        @pl.when(j + 1 < LANCZOS_STEPS)
        def _():
            write_u()

        return beta

    def all_steps(zb, turned):
        lax.fori_loop(0, LANCZOS_STEPS, functools.partial(step, zb, turned), jnp.zeros((), f32))
        turn(turned)
        own_copy(turned, LANCZOS_STEPS - 1).start()
        send_out(turned, LANCZOS_STEPS - 1, (14, 15, 6, 12, 10, 7, 13, 11, 2, 4, 8, 3, 5, 9, 1))
        finish_out(turned, LANCZOS_STEPS - 1)

    pl.run_scoped(all_steps, pltpu.VMEM((8, BOND, 256), bf), pltpu.VMEM((BOND, BOND), f32))


def run_lanczos(flags, psi, left_loc, pair_loc, right_loc):
    smem = pl.BlockSpec(memory_space=pltpu.SMEM)
    hbm = pl.BlockSpec(memory_space=pltpu.HBM)
    dma = pltpu.SemaphoreType.DMA
    return pl.pallas_call(
        lanczos_kernel,
        out_shape=(jax.ShapeDtypeStruct((LANCZOS_STEPS, DEVS, SLAB, BOND), f32), jax.ShapeDtypeStruct((1, 8), f32), jax.ShapeDtypeStruct((1, 8), f32)),
        in_specs=[smem, hbm, hbm, hbm, hbm, hbm],
        out_specs=(hbm, smem, smem),
        scratch_shapes=[
            pltpu.VMEM((CHUNKS, 8, 2, 2, 2, 2, 80, LANES), bf),
            pltpu.VMEM((2, 2, 2, 2, 2, BOND, BOND), bf),
            pltpu.VMEM((PAIR, TERMS * SLAB, LANES), bf),
            pltpu.VMEM((BOND, BOND), f32),
            pltpu.VMEM((BOND, BOND), f32),
            pltpu.VMEM((BOND, BOND), f32),
            pltpu.VMEM((2, DEVS, 8, 128), f32),
            pltpu.VMEM((TERMS * SLAB, 1024), bf),
            pltpu.VMEM((DEVS, 2, 256, 256), bf),
            pltpu.VMEM((DEVS, 2, PAIR, LANES), bf),
            dma((8,)), dma((5,)), dma, dma((CHUNKS, 3, 7)), dma((CHUNKS, 3, 7)), dma((CHUNKS, 8)), dma((CHUNKS, 8)),
            dma((2, DEVS)), dma((2, DEVS)), dma((DEVS,)), dma((DEVS,)), dma((2, DEVS)), dma((2, DEVS)),
        ],
        compiler_params=pltpu.CompilerParams(collective_id=0, has_side_effects=True, vmem_limit_bytes=67043328),
    )(flags, psi, psi.reshape(BOND * PAIR, BOND), left_loc, pair_loc, right_loc.reshape(2 * BOND, BOND))


def place_kernel(first_block, norm, psi, gathered, out):
    vec = pl.program_id(0)

    @pl.when(vec == 0)
    def _():
        out[0] = psi[...] / norm[0, LANCZOS_STEPS]

    @pl.when(vec > 0)
    def _():
        for r in range(0, SLAB, 8):
            for q in range(PAIR):
                out[0, r:r + 8, q, :] = jnp.concatenate([gathered[0, src, r:r + 8, SLAB * q:SLAB * q + SLAB] for src in range(DEVS)], axis=1)


def place_outputs(first_block, norm, wavefunction, gathered):
    return pl.pallas_call(
        place_kernel,
        out_shape=jax.ShapeDtypeStruct((LANCZOS_STEPS + 1, SLAB, PAIR, BOND), f32),
        grid_spec=pltpu.PrefetchScalarGridSpec(
            num_scalar_prefetch=1,
            grid=(LANCZOS_STEPS + 1,),
            in_specs=[
                pl.BlockSpec(memory_space=pltpu.SMEM),
                pl.BlockSpec((SLAB, PAIR, BOND), lambda v, first: (first[0], 0, 0)),
                pl.BlockSpec((1, DEVS, SLAB, BOND), lambda v, first: (jnp.maximum(v - 1, 0), 0, 0, 0)),
            ],
            out_specs=pl.BlockSpec((1, SLAB, PAIR, BOND), lambda v, first: (v, 0, 0, 0)),
        ),
    )(first_block, norm, wavefunction, gathered)


def solution(mesh):
    def device_body(wavefunction, left_loc, pair_loc, right_loc, flag_loc):
        me = lax.axis_index(AXIS_NAME)
        pair_pad = jnp.pad(pair_loc, ((0, 0), (0, 0), (0, LANES - PAIR)))
        vecs, alphas, betas = run_lanczos(flag_loc, wavefunction, left_loc, pair_pad, right_loc)
        krylov = place_outputs(me.reshape(1), betas, wavefunction, vecs)
        return krylov, alphas[0, :LANCZOS_STEPS], betas[0, :LANCZOS_STEPS]

    return jax.shard_map(device_body, mesh=mesh, in_specs=(P(), P(AXIS_NAME), P(AXIS_NAME), P(AXIS_NAME), P(AXIS_NAME)), out_specs=(P(None, AXIS_NAME), P(), P()), check_vma=False)
```

```python
import functools
import jax
import jax.numpy as jnp
from jax import lax
from jax.experimental import pallas as pl
from jax.sharding import PartitionSpec as P
from jax.experimental.pallas import tpu as pltpu

LANCZOS_STEPS = 6
AXIS_NAME = 'terms'
BOND = 640
PAIR = 16
TERMS = 32
DEVS = 16
SLAB = BOND // DEVS
CHUNKS = 5
FEW = 20
LANES = 128
VEC_SIZE = BOND * PAIR * BOND
bf = jnp.bfloat16
f32 = jnp.float32
MESH = pl.DeviceIdType.MESH
PART_PAIRS = ((0, 3), (3, 6), (6, 8))
LEFT_ROWS = ((0, 48), (48, 96), (96, 128))
AXES = ((1, 0, 0), (0, 1, 0), (0, 0, 1))
D2D_FLIPS = ((0,), (1,), (2,), (0, 1), (0, 2), (1, 2), (0, 1, 2), ())


def entry_barrier(me):
    barrier = pltpu.get_barrier_semaphore()
    for off in range(1, DEVS):
        pl.semaphore_signal(barrier, inc=1, device_id=(lax.rem(me + off, DEVS),), device_id_type=MESH)
    pl.semaphore_wait(barrier, DEVS - 1)


def iota(shape, dim):
    return lax.broadcasted_iota(jnp.int32, shape, dim)


def remote(ref, dst_ref, send, recv, dev):
    return pltpu.make_async_remote_copy(src_ref=ref, dst_ref=dst_ref, send_sem=send, recv_sem=recv, device_id=(dev,), device_id_type=MESH)


class Spot:
    def __init__(self, net, ch):
        self.ch = ch
        self.hits, self.across = [], []
        for n in range(3):
            axis = (n + ch) % 3 if isinstance(ch, int) else lax.rem(n + ch, 3)
            one = axis * (2 - axis)
            two = axis * (axis - 1) // 2 if isinstance(ch, int) else lax.div(axis * (axis - 1), 2)
            hit = (1 - one - two, one, two)
            self.hits.append(hit)
            self.across.append(net.me + hit[0] * net.step[0] + hit[1] * net.step[1] + hit[2] * net.step[2])


class Gather:
    def __init__(self, me, ici_send, ici_recv, d2d_send, d2d_recv):
        self.me, self.sems = me, (ici_send, ici_recv, d2d_send, d2d_recv)
        self.core = lax.rem(me, 2)
        self.place = (lax.rem(lax.div(me, 2), 2), lax.rem(lax.div(me, 4), 2), lax.div(me, 8))
        self.turn = tuple(1 - 2 * at for at in self.place)
        self.step = tuple((2 << n) * turn for n, turn in enumerate(self.turn))
        self.partner = me + 1 - 2 * self.core

    def at(self, ch):
        return Spot(self, ch)

    def slots(self, hits):
        idx = []
        for n in (2, 1, 0):
            moved = self.place[n]
            for hit in hits:
                if not isinstance(hit[n], int) or hit[n]:
                    moved = moved + hit[n] * self.turn[n]
            idx.append(moved)
        return tuple(idx) + (self.core,)

    def unit(self, view, spot, part, n, arriving=False):
        flips, axis = (((), 0), ((), 1), ((), 2), ((0,), 1), ((0,), 2), ((1,), 2), ((0, 1), 2))[n]
        hits = [spot.hits[(part + m) % 3] for m in (flips + (axis,) if arriving else flips)]
        ref = view(spot.ch, part, hits)
        return remote(ref, ref, self.sems[0].at[spot.ch, part, n], self.sems[1].at[spot.ch, part, n], spot.across[(part + axis) % 3])

    def start_units(self, view, spot, *which):
        for n in which:
            for part in range(3):
                self.unit(view, spot, part, n).start()

    def wait_units(self, view, spot, *which):
        for n in which:
            for part in range(3):
                self.unit(view, spot, part, n, True).wait_recv()

    def d2d(self, view, spot, n):
        ref = view(spot.ch, 3, [AXES[m] for m in D2D_FLIPS[n]])
        return remote(ref, ref, self.sems[2].at[spot.ch, n], self.sems[3].at[spot.ch, n], self.partner)

    def own_out(self, view, spot):
        self.start_units(view, spot, 0, 1, 2)
        self.d2d(view, spot, 7).start()

    def relay_first(self, view, spot):
        for part in range(3):
            self.unit(view, spot, part, 0, True).wait_recv()
            self.unit(view, spot, part, 3).start()
        self.start_units(view, spot, 4)

    def relay_second(self, view, spot):
        for part in range(3):
            self.unit(view, spot, part, 1, True).wait_recv()
            self.unit(view, spot, part, 5).start()

    def relay_third(self, view, spot):
        self.wait_units(view, spot, 2)
        for n in (0, 1, 2):
            self.d2d(view, spot, n).start()

    def relay_last(self, view, spot):
        for part in range(3):
            self.unit(view, spot, part, 3, True).wait_recv()
            self.unit(view, spot, part, 6).start()

    def take_pairs(self, view, spot):
        self.wait_units(view, spot, 4, 5)
        for n in (3, 4, 5):
            self.d2d(view, spot, n).start()

    def take_last(self, view, spot):
        self.wait_units(view, spot, 6)
        self.d2d(view, spot, 6).start()

    def chunk_ready(self, view, spot):
        for n in range(8):
            self.d2d(view, spot, n).wait_recv()

    def drain_sends(self, view, spot):
        for n in range(8):
            self.d2d(view, spot, n).wait_send()
        for n in range(7):
            for part in range(3):
                self.unit(view, spot, part, n).wait_send()


def prep_kernel(flags, psi, psi_rows, pair_loc, right_hbm, left_hbm, table, few, norm_out, u_hbm, slab_hbm, wi_hbm, right_out, left_out,
                u, y, moved, cur, seen, ops, wi, left, load_sem, stage_sem, out_sem, seen_send, seen_recv, op_send, op_recv, ici_send, ici_recv, d2d_send, d2d_recv):
    me = lax.axis_index(AXIS_NAME)
    net = Gather(me, ici_send, ici_recv, d2d_send, d2d_recv)

    def left_view(ch, part, flips):
        lo, hi = LEFT_ROWS[part] if part < 3 else (0, 128)
        return left.at[net.slots(flips) + (slice(None), slice(lo, hi))]

    def dots(fn, count):
        def body(g, tots):
            rows = pl.ds(pl.multiple_of(g * 16, 16), 16)
            out = []
            for tot, val in zip(tots, fn(rows)):
                for r in range(2):
                    for c in range(5):
                        tot = tot + val[8 * r:8 * r + 8, 128 * c:128 * c + 128]
                out.append(tot)
            return tuple(out)
        return lax.fori_loop(0, 40, body, (jnp.zeros((8, LANES), f32),) * count)

    def spread_right():
        col = iota((BOND, 128), 0)
        source = (col * 1639) >> 16
        within = col - source * SLAB
        target = jnp.where(within < 32, source * 32 + within, 480 + source * 8 + within)
        for t in range(5):
            perm = (target == iota((BOND, 128), 1) + 128 * t).astype(f32).astype(bf)
            for k in range(2):
                rows = jnp.concatenate([y[n, BOND * k:BOND * k + BOND, :] for n in range(5)], axis=1)
                val = jnp.dot(rows, perm, preferred_element_type=f32).reshape(DEVS, SLAB, 128)
                if k == 0:
                    first = val
            moved[t] = jnp.concatenate([first[:, None], val[:, None]], axis=1).reshape(TERMS, SLAB, 128).astype(bf)

    def build_pairs():
        widen = ((iota((128, 256), 1) >> 4) == iota((128, 256), 0)).astype(bf)
        same = (iota((256, 256), 0) & 15) == (iota((256, 256), 1) & 15)

        @pl.loop(0, DEVS)
        def _(k):
            wide = []
            for t in range(2):
                tall = jnp.broadcast_to(ops[k, t].astype(f32)[:, None, :], (16, 16, 128)).reshape(256, 128).astype(bf)
                wide.append(jnp.where(same, jnp.dot(tall, widen, preferred_element_type=f32), 0.0))
            wi[k, 0] = wide[0].astype(bf)
            wi[k, 1] = wide[1].astype(bf)

    def tile_load(stage, t, ch, half):
        rows, qs = pl.ds(pl.multiple_of(128 * ch, 128), 128), pl.ds(pl.multiple_of(8 * half, 8), 8)
        return pltpu.make_async_copy(psi.at[rows, qs, 128 * t:128 * t + 128], stage.at[t], stage_sem.at[t])

    def vector_out(ch):
        return pltpu.make_async_copy(u.at[ch], u_hbm.at[ch], out_sem.at[ch])

    def start_vector(norm, stage, flip):
        base = (me * SLAB) // 128
        skip = pl.multiple_of(me * SLAB - base * 128, 8)
        for t in range(5):
            tile_load(stage, t, 0, 0).start()

        @pl.loop(0, 2 * CHUNKS)
        def _(it):
            ch, half = it // 2, lax.rem(it, 2)
            @pl.when(it == 3)
            def _():
                net.relay_first(left_view, net.at(0))

            @pl.when(it == 4)
            def _():
                net.relay_second(left_view, net.at(0))
                send_right(5, 10)

            @pl.when(it == 6)
            def _():
                net.relay_third(left_view, net.at(0))

            @pl.when(it == 8)
            def _():
                net.relay_last(left_view, net.at(0))
                send_right(10, 15)

            for t in range(5):
                tile_load(stage, t, ch, half).wait()

                @pl.when((base == t) | (base + 1 == t))
                def _():
                    rows = pl.ds(pl.multiple_of(128 * (t - base), 128), 128)
                    for q in range(8):
                        flip[q, rows, :] = stage[t, :, q, :].T

                for q in range(8):
                    val = (stage[t, :, q, :].T / norm).astype(bf)
                    for m in range(16):
                        src, piece = (16 * t + m) // 5, (16 * t + m) % 5
                        row = 64 + 8 * (q % 2) if piece == 4 else 32 * (q % 2) + 8 * piece
                        u[ch, 4 * half + q // 2, src // 8, src // 4 % 2, src // 2 % 2, src % 2, row:row + 8, :] = val[8 * m:8 * m + 8, :]

                @pl.when(it + 1 < 2 * CHUNKS)
                def _():
                    tile_load(stage, t, (it + 1) // 2, lax.rem(it + 1, 2)).start()

            lanes = pl.ds(pl.multiple_of(128 * ch, 128), 128)
            for q in range(8):
                val = flip[q, pl.ds(skip, SLAB), :] / norm
                row = 128 * half + 16 * q
                for start, piece, size in ((row, 0, 16), (256 + row, 16, 16), (512 + 64 * half + 8 * q, 32, 8)):
                    cur[pl.ds(pl.multiple_of(start, 8), size), lanes] = val[piece:piece + size, :]

            @pl.when(half == 1)
            def _():
                vector_out(ch).start()

    def seen_copy(off, dev, src):
        return remote(seen.at[src], seen.at[src], seen_send.at[off], seen_recv.at[src], dev)

    def pair_copy(off, dev, src):
        return remote(ops.at[src], ops.at[src], op_send.at[0, off], op_recv.at[0, src], dev)

    def right_copy(off, dev, src):
        return remote(moved.at[:, pl.ds(2 * dev, 2)], right_out.at[:, pl.ds(2 * src, 2)], op_send.at[1, off], op_recv.at[1, src], dev)

    def others():
        return [(off, lax.rem(me + off, DEVS)) for off in range(1, DEVS)]

    def send_right(first, last):
        for n in range(first, last):
            off = 3 * (n % 5) + n // 5 + 1
            right_copy(off, lax.rem(me + off, DEVS), me).start()

    slab_load = pltpu.make_async_copy(psi_rows.at[pl.ds(pl.multiple_of(me * BOND, 8), BOND)], cur, load_sem.at[0])
    left_load = pltpu.make_async_copy(left_hbm.at[:, 0:128], left.at[net.slots(())], load_sem.at[1])
    right_load = [pltpu.make_async_copy(right_hbm.at[:, 128 * n:128 * n + 128], y.at[n], load_sem.at[2 + n]) for n in range(5)]
    slab_load.start()
    left_load.start()
    for load in right_load:
        load.start()
    for t in range(2):
        ops[me, t] = jnp.concatenate([pair_loc[t].astype(f32), jnp.zeros((PAIR, LANES - PAIR), f32)], axis=1).astype(bf)
    entry_barrier(me)
    slab_load.wait()
    square, = dots(lambda rows: (cur[rows, :] * cur[rows, :],), 1)
    row = iota((8, LANES), 0)
    full = jnp.where(row == 1, flags[0], flags[1]).astype(f32)
    seen[me] = jnp.where(row == 0, jnp.sum(square, axis=0, keepdims=True), full)
    for off, dev in others():
        seen_copy(off, dev, me).start()
    for off, dev in others():
        pair_copy(off, dev, me).start()
    left_load.wait()
    net.own_out(left_view, net.at(0))
    for load in right_load:
        load.wait()
    spread_right()
    send_right(0, 5)
    own = pl.ds(2 * me, 2)
    right_own = pltpu.make_async_copy(moved.at[:, own], right_out.at[:, own], load_sem.at[0])
    right_own.start()
    for off, dev in others():
        seen_copy(off, dev, dev).wait_recv()
    norm = jnp.sqrt(jnp.sum(jnp.sum(seen[:, 0:1, :], axis=0)) / VEC_SIZE)
    norm_out[0] = norm
    term, lane = iota((TERMS, LANES), 0), iota((TERMS, LANES), 1)
    full = jnp.concatenate([seen[src, 1:3, :] for src in range(DEVS)], axis=0)
    in_lanes = jnp.sum(jnp.where(term == lane, full, 0.0), axis=0, keepdims=True)
    rank = jnp.sum(jnp.where(term < lane, full, 0.0), axis=0, keepdims=True)
    rank_down = jnp.sum(jnp.where(lane < term, in_lanes, 0.0), axis=1, keepdims=True)
    holder = jnp.sum(jnp.where(rank_down == lane.astype(f32), full * term.astype(f32), 0.0), axis=0, keepdims=True)
    table[...] = jnp.where(row == 1, holder, jnp.where(in_lanes > 0.5, rank, jnp.where(row == 0, FEW, TERMS).astype(f32))).astype(jnp.int32)
    few[0] = jnp.where(jnp.sum(in_lanes) < FEW + 0.5, 1, 0)
    pl.run_scoped(functools.partial(start_vector, norm), pltpu.VMEM((5, 128, 8, LANES), f32), pltpu.VMEM((8, 256, LANES), f32))
    slab_out = pltpu.make_async_copy(cur, slab_hbm, load_sem.at[1])
    slab_out.start()
    for off, dev in others():
        pair_copy(off, dev, dev).wait_recv()
    build_pairs()
    wi_out = pltpu.make_async_copy(wi, wi_hbm, load_sem.at[2])
    wi_out.start()
    net.take_pairs(left_view, net.at(0))
    net.take_last(left_view, net.at(0))
    net.chunk_ready(left_view, net.at(0))
    all_left = pltpu.make_async_copy(left, left_out, load_sem.at[3])
    all_left.start()
    net.drain_sends(left_view, net.at(0))
    for off, dev in others():
        right_copy(off, dev, dev).wait_recv()
    for off, dev in others():
        seen_copy(off, dev, me).wait_send()
        pair_copy(off, dev, me).wait_send()
        right_copy(off, dev, me).wait_send()
    right_own.wait()
    slab_out.wait()
    wi_out.wait()
    all_left.wait()
    for ch in range(CHUNKS):
        vector_out(ch).wait()


VECTOR_SHAPE = (CHUNKS, 8, 2, 2, 2, 2, 80, LANES)


def prepare(flags, psi, pair_loc, right_loc, left_loc):
    smem = pl.BlockSpec(memory_space=pltpu.SMEM)
    vmem = pl.BlockSpec(memory_space=pltpu.VMEM)
    hbm = pl.BlockSpec(memory_space=pltpu.HBM)
    dma = pltpu.SemaphoreType.DMA
    return pl.pallas_call(
        prep_kernel,
        out_shape=(
            jax.ShapeDtypeStruct((8, LANES), jnp.int32), jax.ShapeDtypeStruct((1,), jnp.int32), jax.ShapeDtypeStruct((1,), f32),
            jax.ShapeDtypeStruct(VECTOR_SHAPE, bf), jax.ShapeDtypeStruct((BOND, BOND), f32),
            jax.ShapeDtypeStruct((DEVS, 2, 256, 256), bf), jax.ShapeDtypeStruct((5, TERMS, SLAB, LANES), bf), jax.ShapeDtypeStruct((2, 2, 2, 2, 2, 128, BOND), bf),
        ),
        in_specs=[smem, hbm, hbm, vmem, hbm, hbm],
        out_specs=(vmem, smem, smem, hbm, hbm, hbm, hbm, hbm),
        scratch_shapes=[
            pltpu.VMEM(VECTOR_SHAPE, bf),
            pltpu.VMEM((5, 2 * BOND, LANES), bf),
            pltpu.VMEM((5, TERMS, SLAB, LANES), bf),
            pltpu.VMEM((BOND, BOND), f32),
            pltpu.VMEM((DEVS, 8, LANES), f32),
            pltpu.VMEM((DEVS, 2, PAIR, LANES), bf),
            pltpu.VMEM((DEVS, 2, 256, 256), bf),
            pltpu.VMEM((2, 2, 2, 2, 2, 128, BOND), bf),
            dma((8,)), dma((5,)), dma((CHUNKS,)), dma((DEVS,)), dma((DEVS,)), dma((2, DEVS)), dma((2, DEVS)),
            dma((1, 3, 7)), dma((1, 3, 7)), dma((1, 8)), dma((1, 8)),
        ],
        compiler_params=pltpu.CompilerParams(collective_id=0, has_side_effects=True, vmem_limit_bytes=67043328),
    )(flags, psi, psi.reshape(BOND * PAIR, BOND), pair_loc, right_loc.reshape(2 * BOND, BOND), left_loc)


def lanczos_kernel(most, table, u_hbm, slab_hbm, wi_hbm, right_hbm, first_left, left_hbm, gathered, alphas, betas,
                   u, lft, y, acc, cur, prev, ar, rc, wi,
                   load_sem, own_sem, ici_send, ici_recv, d2d_send, d2d_recv, ar_send, ar_recv, out_send, out_recv):
    me = lax.axis_index(AXIS_NAME)
    net = Gather(me, ici_send, ici_recv, d2d_send, d2d_recv)
    core, place = net.core, net.place

    def vec_view(ch, part, flips):
        pairs = PART_PAIRS[part] if part < 3 else (0, 8)
        return u.at[(ch, slice(pairs[0], pairs[1])) + net.slots(flips)]

    def left_view(ch, part, flips):
        lo, hi = LEFT_ROWS[part] if part < 3 else (0, 128)
        return lft.at[net.slots(flips) + (slice(None), slice(128 * ch + lo, 128 * ch + hi), slice(128 * ch, BOND))]

    def for_left(ch, what):
        for c in range(CHUNKS):
            @pl.when(ch == c)
            def _():
                what(left_view, net.at(c))

    def send_partial(which, partials):
        row = iota((8, LANES), 0)
        tile = jnp.zeros((8, LANES), f32)
        for n, partial in enumerate(partials):
            tile = jnp.where(row == n, jnp.sum(partial, axis=0, keepdims=True), tile)
        ar[which, me] = tile
        for off in range(1, DEVS):
            dev = lax.rem(me + off, DEVS)
            ref = ar.at[which, me]
            remote(ref, ref, ar_send.at[which, off], ar_recv.at[which, me], dev).start()

    def total_of(which, count):
        for off in range(1, DEVS):
            dev = lax.rem(me + off, DEVS)
            ref = ar.at[which, dev]
            remote(ref, ref, ar_send.at[which, off], ar_recv.at[which, dev], dev).wait_recv()
        total = jnp.sum(ar[which], axis=0)
        sums = [jnp.sum(total[n:n + 1]) / VEC_SIZE for n in range(count)]
        for off in range(1, DEVS):
            dev = lax.rem(me + off, DEVS)
            ref = ar.at[which, me]
            remote(ref, ref, ar_send.at[which, off], ar_recv.at[which, me], dev).wait_send()
        return sums

    def dots(fn, count):
        def body(g, tots):
            rows = pl.ds(pl.multiple_of(g * 16, 16), 16)
            out = []
            for tot, val in zip(tots, fn(rows)):
                for r in range(2):
                    for c in range(5):
                        tot = tot + val[8 * r:8 * r + 8, 128 * c:128 * c + 128]
                out.append(tot)
            return tuple(out)
        return lax.fori_loop(0, 40, body, (jnp.zeros((8, LANES), f32),) * count)

    def write_u():
        for ch in range(CHUNKS):
            lanes = slice(128 * ch, 128 * ch + 128)
            for i in range(8):
                dst = u.at[ch, i, place[2], place[1], place[0], core]
                dst[0:16] = cur[32 * i:32 * i + 16, lanes].astype(bf)
                dst[16:32] = cur[256 + 32 * i:256 + 32 * i + 16, lanes].astype(bf)
                dst[32:48] = cur[32 * i + 16:32 * i + 32, lanes].astype(bf)
                dst[48:64] = cur[256 + 32 * i + 16:256 + 32 * i + 32, lanes].astype(bf)
                dst[64:80] = cur[512 + 16 * i:512 + 16 * i + 16, lanes].astype(bf)

    def right_phase(ch, middle):
        for par in range(2):
            if par == 1:
                middle()
            rhs = []
            for i in range(8):
                main = u[ch, i, :, :, :, :, 32 * par:32 * par + 32, :].reshape(512, 128)
                tail = u[ch, i, :, :, :, :, 64:80, :].reshape(256, 128)
                rhs.append(jnp.concatenate([main, tail], axis=0))
            rhs = jnp.concatenate(rhs, axis=1)
            lhs = jnp.concatenate([rc[:, 0:512], rc[:, 512 + 256 * par:768 + 256 * par]], axis=1)
            val = jnp.dot(lhs, rhs, preferred_element_type=f32)
            for i in range(8):
                y[2 * i + par, 0:most] = val[:, 128 * i:128 * i + 128].reshape(most, SLAB, 128).astype(bf)
                own = u.at[ch, i, place[2], place[1], place[0], core]
                y[2 * i + par, most, 0:32] = own[32 * par:32 * par + 32, :]
                y[2 * i + par, most, 32:40] = own[64 + 8 * par:72 + 8 * par, :]

    def pair_left_phase(ch, zb, half_done):
        low_rows = (iota((256, 256), 0) & 15) < 8

        @pl.loop(0, 2)
        def _(g):
            for s in range(8):
                k = g * 8 + s
                first, second = [table[0 if most == FEW else 2, 2 * k + t] for t in range(2)]

                def tile(at, row):
                    return y[:, at, row:row + 16, :].reshape(256, 128)

                z01 = jnp.dot(wi[k, 0], jnp.concatenate([tile(first, 0), tile(first, 16)], axis=1), preferred_element_type=f32).astype(bf)
                mixed = jnp.where(low_rows, wi[k, 0], wi[k, 1])
                ends = jnp.concatenate([y[:, at, 32:40, :] for at in (first, second)], axis=1).reshape(256, 128)
                z2 = jnp.dot(mixed, ends, preferred_element_type=f32).reshape(16, 2, 8, 128)
                z34 = jnp.dot(wi[k, 1], jnp.concatenate([tile(second, 0), tile(second, 16)], axis=1), preferred_element_type=f32).astype(bf)
                zb[s, 0:256, 0:128] = z01[:, 0:128]
                zb[s, 256:512, 0:128] = z01[:, 128:256]
                zb[s, 512:640, 0:128] = z2[:, 0].reshape(128, 128).astype(bf)
                zb[s, 0:256, 128:256] = z34[:, 0:128]
                zb[s, 256:512, 128:256] = z34[:, 128:256]
                zb[s, 512:640, 128:256] = z2[:, 1].reshape(128, 128).astype(bf)
            lhs = jnp.concatenate([zb[s] for s in range(8)], axis=1)
            rows = pl.ds(pl.multiple_of(ch * 128, 128), 128)
            rhs = jnp.concatenate([lft[g, s // 4, s // 2 % 2, s % 2, t, rows, :] for s in range(8) for t in range(2)], axis=0)
            acc[...] += jnp.dot(lhs, rhs, preferred_element_type=f32)

            @pl.when(g == 0)
            def _():
                half_done()

    def turn(vec, turned):
        shifted = [lax.rem(q + DEVS - me, DEVS) for q in range(PAIR)]
        for lt in range(5):
            rows = []
            for n in range(16 * lt, 16 * lt + 16):
                q, part = shifted[n // 5], n % 5
                start = 512 + 8 * q if part == 4 else 256 * (part // 2) + 16 * q + 8 * (part % 2)
                rows.append(vec[pl.ds(pl.multiple_of(start, 8), 8), :])
            turned[:, 128 * lt:128 * lt + 128] = jnp.concatenate(rows, axis=0).T

    def flipped(mask):
        dev = me
        for n, bit in enumerate((core,) + place):
            if mask >> n & 1:
                dev = dev + (1 << n) * (1 - 2 * bit)
        return dev

    def out_copy(turned, vec, mask, final, arriving=False):
        dev = flipped(mask)
        src = dev if arriving else me
        rows = pl.ds(pl.multiple_of(dev * SLAB, 8), SLAB)
        return remote(turned.at[rows], gathered.at[vec, src], out_send.at[mask], out_recv.at[final, mask], dev)

    def own_copy(turned, vec):
        rows = pl.ds(pl.multiple_of(me * SLAB, 8), SLAB)
        return pltpu.make_async_copy(turned.at[rows], gathered.at[vec, me], own_sem)

    def send_out(turned, vec, masks, final=0):
        for mask in masks:
            out_copy(turned, vec, mask, final).start()

    def finish_out(turned, vec, final=0):
        own_copy(turned, vec).wait()
        for mask in range(1, DEVS):
            out_copy(turned, vec, mask, final, True).wait_recv()
        for mask in range(1, DEVS):
            out_copy(turned, vec, mask, final).wait_send()

    def build_right():
        for n in range(most):
            for t in range(5):
                rc[SLAB * n:SLAB * n + SLAB, 128 * t:128 * t + 128] = y[t, table[1, n]]
        tails = rc[:, 512:640]
        src = iota((128, 256), 0)
        spot = 16 * (src >> 3) + (src & 7)
        for par in range(2):
            widen = (spot + 8 * par == iota((128, 256), 1)).astype(bf)
            rc[:, 512 + 256 * par:768 + 256 * par] = jnp.dot(tails, widen, preferred_element_type=f32).astype(bf)

    def mirror_left(ch):
        @pl.loop(0, 8)
        def _(g):
            for n in range(4):
                at = (g // 4, lax.rem(g // 2, 2), lax.rem(g, 2), n // 2, n % 2)
                for other in range(ch + 1, CHUNKS):
                    block = lft[at + (slice(128 * ch, 128 * ch + 128), slice(128 * other, 128 * other + 128))]
                    lft[at + (slice(128 * other, 128 * other + 128), slice(128 * ch, 128 * ch + 128))] = block.T

    left_load = pltpu.make_async_copy(left_hbm.at[:, 128:BOND], lft.at[net.slots(()) + (slice(None), slice(128, BOND))], load_sem.at[0])
    right_load = pltpu.make_async_copy(right_hbm, y.at[0:5, 0:TERMS], load_sem.at[1])
    wi_load = pltpu.make_async_copy(wi_hbm, wi, load_sem.at[2])
    slab_load = pltpu.make_async_copy(slab_hbm, cur, load_sem.at[3])
    first_load = pltpu.make_async_copy(first_left, lft.at[:, :, :, :, :, 0:128], load_sem.at[4])

    def vector_load(ch):
        return pltpu.make_async_copy(u_hbm.at[ch], u.at[ch], load_sem.at[5 + ch])

    left_load.start()
    right_load.start()
    vector_load(0).start()
    wi_load.start()
    first_load.start()
    for ch in range(1, CHUNKS):
        vector_load(ch).start()
    slab_load.start()
    entry_barrier(me)
    left_load.wait()
    net.own_out(left_view, net.at(1))
    right_load.wait()
    build_right()
    prev[...] = jnp.zeros_like(prev)

    def step(zb, turned, j, beta_prev):
        acc[...] = jnp.zeros_like(acc)

        later = j > 0

        @pl.when(later)
        def _():
            zero, one = net.at(0), net.at(1)
            net.own_out(vec_view, zero)
            turn(cur, turned)
            own_copy(turned, j - 1).start()
            net.relay_first(vec_view, zero)
            net.relay_second(vec_view, zero)
            net.relay_last(vec_view, zero)
            net.own_out(vec_view, one)
            net.relay_third(vec_view, zero)
            net.take_pairs(vec_view, zero)
            net.take_last(vec_view, zero)
            net.chunk_ready(vec_view, zero)

        @pl.loop(0, CHUNKS)
        def _(ch):
            next_spot, after_spot = net.at(ch + 1), net.at(ch + 2)

            @pl.when(later & (ch + 1 < CHUNKS))
            def _():
                net.relay_first(vec_view, next_spot)

            @pl.when(later & (ch == 4))
            def _():
                send_out(turned, j - 1, (7, 13, 11))

            def middle():
                @pl.when(later & (ch + 1 < CHUNKS))
                def _():
                    net.relay_second(vec_view, next_spot)

            @pl.when(j == 0)
            def _():
                vector_load(ch).wait()

            right_phase(ch, middle)

            @pl.when(later & (ch + 1 < CHUNKS))
            def _():
                net.relay_third(vec_view, next_spot)
                net.relay_last(vec_view, next_spot)

                @pl.when(ch + 2 < CHUNKS)
                def _():
                    net.own_out(vec_view, after_spot)

                @pl.when(ch == 3)
                def _():
                    send_out(turned, j - 1, (1, 3, 5, 9, 14, 15))

            @pl.when(j == 0)
            def _():
                @pl.when(ch == 0)
                def _():
                    wi_load.wait()
                    first_load.wait()

                def left_ready(view, spot):
                    if spot.ch > 0:
                        mirror_left(spot.ch - 1)
                        net.take_pairs(view, spot)
                        net.take_last(view, spot)
                        net.chunk_ready(view, spot)

                for_left(ch, left_ready)
                for_left(ch + 1, net.relay_first)

            def half_done():
                @pl.when(later & (ch + 1 < CHUNKS))
                def _():
                    net.take_pairs(vec_view, next_spot)
                    net.take_last(vec_view, next_spot)

                    @pl.when(ch == 2)
                    def _():
                        send_out(turned, j - 1, (2, 4, 8))

                    @pl.when(ch == 3)
                    def _():
                        send_out(turned, j - 1, (6, 12, 10))

                @pl.when(j == 0)
                def _():
                    for_left(ch + 1, net.relay_second)

            pair_left_phase(ch, zb, half_done)

            @pl.when(later & (ch + 1 < CHUNKS))
            def _():
                net.chunk_ready(vec_view, next_spot)

            @pl.when(j == 0)
            def _():
                def advance(view, spot):
                    net.relay_third(view, spot)
                    net.relay_last(view, spot)

                for_left(ch + 1, advance)
                for_left(ch + 2, net.own_out)

        @pl.loop(0, CHUNKS)
        def _(ch):
            @pl.when((j == 0) & (ch > 0))
            def _():
                for_left(ch, net.drain_sends)

            @pl.when(later)
            def _():
                net.drain_sends(vec_view, net.at(ch))

        @pl.when(later)
        def _():
            finish_out(turned, j - 1)

        @pl.when(j == 0)
        def _():
            slab_load.wait()

        @pl.when(j == 0)
        def _():
            send_partial(0, dots(lambda rows: (acc[rows, :] * cur[rows, :],), 1))
            betas[0, LANCZOS_STEPS + 1] = total_of(0, 1)[0]

        shift = betas[0, LANCZOS_STEPS + 1]

        def products(rows):
            v, v_prev = cur[rows, :], prev[rows, :]
            w = acc[rows, :] - shift * v - beta_prev * v_prev
            acc[rows, :] = w
            return w * w, w * v, v * v, v * v_prev

        send_partial(1, dots(products, 4))

        @pl.when(j + 1 == LANCZOS_STEPS)
        def _():
            turn(acc, turned)
            own_copy(turned, j).start()
            send_out(turned, j, (14, 15, 6, 12, 10, 7, 13, 11, 2, 4, 8, 3, 5, 9, 1), 1)

        ww, wv, vv, vp = total_of(1, 4)
        alpha = wv + shift * vv + beta_prev * vp
        extra = alpha - shift
        beta = jnp.sqrt(ww - 2.0 * extra * wv + extra * extra * vv)
        alphas[0, j] = alpha
        betas[0, j] = beta
        betas[0, LANCZOS_STEPS] = extra
        betas[0, LANCZOS_STEPS + 1] = alpha

        @pl.when(j + 1 < LANCZOS_STEPS)
        def _():
            @pl.loop(0, 40)
            def _(g):
                rows = pl.ds(pl.multiple_of(g * 16, 16), 16)
                v = cur[rows, :]
                prev[rows, :] = v
                cur[rows, :] = (acc[rows, :] - extra * v) / beta

            write_u()

        return beta

    def all_steps(zb, turned):
        lax.fori_loop(0, LANCZOS_STEPS, functools.partial(step, zb, turned), jnp.zeros((), f32))
        finish_out(turned, LANCZOS_STEPS - 1, 1)

    pl.run_scoped(all_steps, pltpu.VMEM((8, BOND, 256), bf), pltpu.VMEM((BOND, BOND), f32))


def run_lanczos(most, table, u_hbm, slab_hbm, wi_hbm, right_hbm, first_left, left_loc):
    smem = pl.BlockSpec(memory_space=pltpu.SMEM)
    hbm = pl.BlockSpec(memory_space=pltpu.HBM)
    dma = pltpu.SemaphoreType.DMA
    return pl.pallas_call(
        functools.partial(lanczos_kernel, most),
        out_shape=(jax.ShapeDtypeStruct((LANCZOS_STEPS, DEVS, SLAB, BOND), f32), jax.ShapeDtypeStruct((1, 8), f32), jax.ShapeDtypeStruct((1, 8), f32)),
        in_specs=[smem] + [hbm] * 6,
        out_specs=(hbm, smem, smem),
        scratch_shapes=[
            pltpu.VMEM(VECTOR_SHAPE, bf),
            pltpu.VMEM((2, 2, 2, 2, 2, BOND, BOND), bf),
            pltpu.VMEM((PAIR, TERMS + 1, SLAB, LANES), bf),
            pltpu.VMEM((BOND, BOND), f32),
            pltpu.VMEM((BOND, BOND), f32),
            pltpu.VMEM((BOND, BOND), f32),
            pltpu.VMEM((2, DEVS, 8, LANES), f32),
            pltpu.VMEM((most * SLAB, 1024), bf),
            pltpu.VMEM((DEVS, 2, 256, 256), bf),
            dma((5 + CHUNKS,)), dma, dma((CHUNKS, 3, 7)), dma((CHUNKS, 3, 7)), dma((CHUNKS, 8)), dma((CHUNKS, 8)),
            dma((2, DEVS)), dma((2, DEVS)), dma((DEVS,)), dma((2, DEVS)),
        ],
        compiler_params=pltpu.CompilerParams(collective_id=most, has_side_effects=True, vmem_limit_bytes=67043328),
    )(table, u_hbm, slab_hbm, wi_hbm, right_hbm, first_left, left_loc)


def place_kernel(norm, alphas, betas, psi, gathered, krylov, alpha_out, beta_out, rows, src, dst, load_sem, store_sem):
    me = lax.axis_index(AXIS_NAME)

    def load(vec):
        return pltpu.make_async_copy(gathered.at[vec], src.at[vec], load_sem.at[vec])

    def store(vec):
        return pltpu.make_async_copy(dst.at[vec], krylov.at[vec], store_sem.at[vec])

    def placed(vec, r, q):
        lane = iota((8, LANES), 1)
        tiles = []
        for t in range(5):
            tile = None
            for m in range(128 * t // SLAB, min(DEVS, (128 * t + 127) // SLAB + 1)):
                val = src[vec, (m - q) % DEVS, pl.ds(r, 8), 128 * t:128 * t + 128]
                tile = val if tile is None else jnp.where(lane >= SLAB * m - 128 * t, val, tile)
            tiles.append(tile)
        skip, rest = SLAB * q // 128, SLAB * q % 128
        if rest:
            tiles = [pltpu.roll(tile, 128 - rest, 1) for tile in tiles]
        tiles = [tiles[(t + skip) % 5] if not rest else jnp.where(lane < 128 - rest, tiles[(t + skip) % 5], tiles[(t + skip + 1) % 5]) for t in range(5)]
        return jnp.concatenate(tiles, axis=1)

    rows_load = pltpu.make_async_copy(psi.at[pl.ds(me * SLAB, SLAB)], rows, load_sem.at[LANCZOS_STEPS])
    rows_load.start()
    for vec in range(LANCZOS_STEPS):
        load(vec).start()
    for n in range(LANCZOS_STEPS):
        alpha_out[n] = alphas[0, n]
        beta_out[n] = betas[0, n]
    rows_load.wait()
    dst[0] = rows[...] / norm[0]
    store(0).start()

    @pl.loop(0, LANCZOS_STEPS - 1)
    def _(vec):
        load(vec).wait()
        for r in range(0, SLAB, 8):
            for q in range(PAIR):
                dst[vec + 1, r:r + 8, q, :] = placed(vec, r, q)
        store(vec + 1).start()

    load(LANCZOS_STEPS - 1).wait()
    for r in range(0, SLAB, 8):
        for q in range(PAIR):
            before = dst[LANCZOS_STEPS - 1, r:r + 8, q, :]
            dst[LANCZOS_STEPS, r:r + 8, q, :] = (placed(LANCZOS_STEPS - 1, r, q) - betas[0, LANCZOS_STEPS] * before) / betas[0, LANCZOS_STEPS - 1]
    store(LANCZOS_STEPS).start()
    for vec in range(LANCZOS_STEPS + 1):
        store(vec).wait()


def place_outputs(norm, alphas, betas, wavefunction, gathered):
    smem = pl.BlockSpec(memory_space=pltpu.SMEM)
    hbm = pl.BlockSpec(memory_space=pltpu.HBM)
    dma = pltpu.SemaphoreType.DMA
    return pl.pallas_call(
        place_kernel,
        out_shape=(jax.ShapeDtypeStruct((LANCZOS_STEPS + 1, SLAB, PAIR, BOND), f32), jax.ShapeDtypeStruct((LANCZOS_STEPS,), f32), jax.ShapeDtypeStruct((LANCZOS_STEPS,), f32)),
        in_specs=[smem, smem, smem, hbm, hbm],
        out_specs=(hbm, smem, smem),
        scratch_shapes=[
            pltpu.VMEM((SLAB, PAIR, BOND), f32),
            pltpu.VMEM((LANCZOS_STEPS, DEVS, SLAB, BOND), f32),
            pltpu.VMEM((LANCZOS_STEPS + 1, SLAB, PAIR, BOND), f32),
            dma((LANCZOS_STEPS + 1,)), dma((LANCZOS_STEPS + 1,)),
        ],
        compiler_params=pltpu.CompilerParams(vmem_limit_bytes=40 * 1024 * 1024),
    )(norm, alphas, betas, wavefunction, gathered)


def solution(mesh):
    def device_body(wavefunction, left_loc, pair_loc, right_loc, flag_loc):
        table, few, norm, *operands = prepare(flag_loc, wavefunction, pair_loc, right_loc, left_loc)
        few_full, all_full = functools.partial(run_lanczos, FEW), functools.partial(run_lanczos, TERMS)
        vecs, alphas, betas = lax.cond(few[0] == 1, few_full, all_full, table, *operands, left_loc)
        return place_outputs(norm, alphas, betas, wavefunction, vecs)

    return jax.shard_map(device_body, mesh=mesh, in_specs=(P(), P(AXIS_NAME), P(AXIS_NAME), P(AXIS_NAME), P(AXIS_NAME)), out_specs=(P(None, AXIS_NAME), P(), P()), check_vma=False)
```

```python
import functools
import jax
import jax.numpy as jnp
from jax import lax
from jax.experimental import pallas as pl
from jax.sharding import PartitionSpec as P
from jax.experimental.pallas import tpu as pltpu

LANCZOS_STEPS = 6
AXIS_NAME = 'terms'
BOND = 640
PAIR = 16
TERMS = 32
DEVS = 16
SLAB = BOND // DEVS
CHUNKS = 5
FEW = 20
LANES = 128
VEC_SIZE = BOND * PAIR * BOND
bf = jnp.bfloat16
f32 = jnp.float32
MESH = pl.DeviceIdType.MESH
PART_PAIRS = ((0, 3), (3, 6), (6, 8))
LEFT_ROWS = ((0, 48), (48, 96), (96, 128))
AXES = ((1, 0, 0), (0, 1, 0), (0, 0, 1))
D2D_FLIPS = ((0,), (1,), (2,), (0, 1), (0, 2), (1, 2), (0, 1, 2), ())


def entry_barrier(me):
    barrier = pltpu.get_barrier_semaphore()
    for off in range(1, DEVS):
        pl.semaphore_signal(barrier, inc=1, device_id=(lax.rem(me + off, DEVS),), device_id_type=MESH)
    pl.semaphore_wait(barrier, DEVS - 1)


def iota(shape, dim):
    return lax.broadcasted_iota(jnp.int32, shape, dim)


def remote(ref, dst_ref, send, recv, dev):
    return pltpu.make_async_remote_copy(src_ref=ref, dst_ref=dst_ref, send_sem=send, recv_sem=recv, device_id=(dev,), device_id_type=MESH)


class Spot:
    def __init__(self, net, ch):
        self.ch = ch
        self.hits, self.across = [], []
        for n in range(3):
            axis = (n + ch) % 3 if isinstance(ch, int) else lax.rem(n + ch, 3)
            one = axis * (2 - axis)
            two = axis * (axis - 1) // 2 if isinstance(ch, int) else lax.div(axis * (axis - 1), 2)
            hit = (1 - one - two, one, two)
            self.hits.append(hit)
            self.across.append(net.me + hit[0] * net.step[0] + hit[1] * net.step[1] + hit[2] * net.step[2])


class Gather:
    def __init__(self, me, ici_send, ici_recv, d2d_send, d2d_recv):
        self.me, self.sems = me, (ici_send, ici_recv, d2d_send, d2d_recv)
        self.core = lax.rem(me, 2)
        self.place = (lax.rem(lax.div(me, 2), 2), lax.rem(lax.div(me, 4), 2), lax.div(me, 8))
        self.turn = tuple(1 - 2 * at for at in self.place)
        self.step = tuple((2 << n) * turn for n, turn in enumerate(self.turn))
        self.partner = me + 1 - 2 * self.core

    def at(self, ch):
        return Spot(self, ch)

    def slots(self, hits):
        idx = []
        for n in (2, 1, 0):
            moved = self.place[n]
            for hit in hits:
                if not isinstance(hit[n], int) or hit[n]:
                    moved = moved + hit[n] * self.turn[n]
            idx.append(moved)
        return tuple(idx) + (self.core,)

    def unit(self, view, spot, part, n, arriving=False):
        flips, axis = (((), 0), ((), 1), ((), 2), ((0,), 1), ((0,), 2), ((1,), 2), ((0, 1), 2))[n]
        hits = [spot.hits[(part + m) % 3] for m in (flips + (axis,) if arriving else flips)]
        ref = view(spot.ch, part, hits)
        return remote(ref, ref, self.sems[0].at[spot.ch, part, n], self.sems[1].at[spot.ch, part, n], spot.across[(part + axis) % 3])

    def start_units(self, view, spot, *which):
        for n in which:
            for part in range(3):
                self.unit(view, spot, part, n).start()

    def wait_units(self, view, spot, *which):
        for n in which:
            for part in range(3):
                self.unit(view, spot, part, n, True).wait_recv()

    def d2d(self, view, spot, n):
        ref = view(spot.ch, 3, [AXES[m] for m in D2D_FLIPS[n]])
        return remote(ref, ref, self.sems[2].at[spot.ch, n], self.sems[3].at[spot.ch, n], self.partner)

    def own_out(self, view, spot):
        self.start_units(view, spot, 0, 1, 2)
        self.d2d(view, spot, 7).start()

    def relay_first(self, view, spot):
        for part in range(3):
            self.unit(view, spot, part, 0, True).wait_recv()
            self.unit(view, spot, part, 3).start()
        self.start_units(view, spot, 4)

    def relay_second(self, view, spot):
        for part in range(3):
            self.unit(view, spot, part, 1, True).wait_recv()
            self.unit(view, spot, part, 5).start()

    def relay_third(self, view, spot):
        self.wait_units(view, spot, 2)
        for n in (0, 1, 2):
            self.d2d(view, spot, n).start()

    def relay_last(self, view, spot):
        for part in range(3):
            self.unit(view, spot, part, 3, True).wait_recv()
            self.unit(view, spot, part, 6).start()

    def take_pairs(self, view, spot):
        self.wait_units(view, spot, 4, 5)
        for n in (3, 4, 5):
            self.d2d(view, spot, n).start()

    def take_last(self, view, spot):
        self.wait_units(view, spot, 6)
        self.d2d(view, spot, 6).start()

    def chunk_ready(self, view, spot):
        for n in range(8):
            self.d2d(view, spot, n).wait_recv()

    def drain_sends(self, view, spot):
        for n in range(8):
            self.d2d(view, spot, n).wait_send()
        for n in range(7):
            for part in range(3):
                self.unit(view, spot, part, n).wait_send()


def prep_kernel(flags, psi, psi_rows, pair_loc, right_hbm, left_hbm, table, few, norm_out, u_hbm, slab_hbm, wi_hbm, right_out, left_out,
                u, y, moved, cur, seen, ops, wi, left, load_sem, stage_sem, out_sem, seen_send, seen_recv, op_send, op_recv, ici_send, ici_recv, d2d_send, d2d_recv):
    me = lax.axis_index(AXIS_NAME)
    net = Gather(me, ici_send, ici_recv, d2d_send, d2d_recv)

    def left_view(ch, part, flips):
        lo, hi = LEFT_ROWS[part] if part < 3 else (0, 128)
        return left.at[net.slots(flips) + (slice(None), slice(lo, hi))]

    def dots(fn, count):
        def body(g, tots):
            rows = pl.ds(pl.multiple_of(g * 16, 16), 16)
            out = []
            for tot, val in zip(tots, fn(rows)):
                for r in range(2):
                    for c in range(5):
                        tot = tot + val[8 * r:8 * r + 8, 128 * c:128 * c + 128]
                out.append(tot)
            return tuple(out)
        return lax.fori_loop(0, 40, body, (jnp.zeros((8, LANES), f32),) * count)

    def spread_right():
        col = iota((BOND, 128), 0)
        source = (col * 1639) >> 16
        within = col - source * SLAB
        target = jnp.where(within < 32, source * 32 + within, 480 + source * 8 + within)
        for t in range(5):
            perm = (target == iota((BOND, 128), 1) + 128 * t).astype(f32).astype(bf)
            for k in range(2):
                rows = jnp.concatenate([y[n, BOND * k:BOND * k + BOND, :] for n in range(5)], axis=1)
                val = jnp.dot(rows, perm, preferred_element_type=f32).reshape(DEVS, SLAB, 128)
                if k == 0:
                    first = val
            moved[t] = jnp.concatenate([first[:, None], val[:, None]], axis=1).reshape(TERMS, SLAB, 128).astype(bf)

    def build_pairs():
        widen = ((iota((128, 256), 1) >> 4) == iota((128, 256), 0)).astype(bf)
        same = (iota((256, 256), 0) & 15) == (iota((256, 256), 1) & 15)

        @pl.loop(0, DEVS)
        def _(k):
            wide = []
            for t in range(2):
                tall = jnp.broadcast_to(ops[k, t].astype(f32)[:, None, :], (16, 16, 128)).reshape(256, 128).astype(bf)
                wide.append(jnp.where(same, jnp.dot(tall, widen, preferred_element_type=f32), 0.0))
            wi[k, 0] = wide[0].astype(bf)
            wi[k, 1] = wide[1].astype(bf)

    def tile_load(stage, t, ch, half):
        rows, qs = pl.ds(pl.multiple_of(128 * ch, 128), 128), pl.ds(pl.multiple_of(8 * half, 8), 8)
        return pltpu.make_async_copy(psi.at[rows, qs, 128 * t:128 * t + 128], stage.at[t], stage_sem.at[t])

    def vector_out(ch):
        return pltpu.make_async_copy(u.at[ch], u_hbm.at[ch], out_sem.at[ch])

    def start_vector(norm, stage, flip):
        base = (me * SLAB) // 128
        skip = pl.multiple_of(me * SLAB - base * 128, 8)
        for t in range(5):
            tile_load(stage, t, 0, 0).start()

        @pl.loop(0, 2 * CHUNKS)
        def _(it):
            ch, half = it // 2, lax.rem(it, 2)
            @pl.when(it == 3)
            def _():
                net.relay_first(left_view, net.at(0))

            @pl.when(it == 4)
            def _():
                net.relay_second(left_view, net.at(0))
                send_right(5, 10)

            @pl.when(it == 6)
            def _():
                net.relay_third(left_view, net.at(0))

            @pl.when(it == 8)
            def _():
                net.relay_last(left_view, net.at(0))
                send_right(10, 15)

            for t in range(5):
                tile_load(stage, t, ch, half).wait()

                @pl.when((base == t) | (base + 1 == t))
                def _():
                    rows = pl.ds(pl.multiple_of(128 * (t - base), 128), 128)
                    for q in range(8):
                        flip[q, rows, :] = stage[t, :, q, :].T

                for q in range(8):
                    val = (stage[t, :, q, :].T / norm).astype(bf)
                    for m in range(16):
                        src, piece = (16 * t + m) // 5, (16 * t + m) % 5
                        row = 64 + 8 * (q % 2) if piece == 4 else 32 * (q % 2) + 8 * piece
                        u[ch, 4 * half + q // 2, src // 8, src // 4 % 2, src // 2 % 2, src % 2, row:row + 8, :] = val[8 * m:8 * m + 8, :]

                @pl.when(it + 1 < 2 * CHUNKS)
                def _():
                    tile_load(stage, t, (it + 1) // 2, lax.rem(it + 1, 2)).start()

            lanes = pl.ds(pl.multiple_of(128 * ch, 128), 128)
            for q in range(8):
                val = flip[q, pl.ds(skip, SLAB), :] / norm
                row = 128 * half + 16 * q
                for start, piece, size in ((row, 0, 16), (256 + row, 16, 16), (512 + 64 * half + 8 * q, 32, 8)):
                    cur[pl.ds(pl.multiple_of(start, 8), size), lanes] = val[piece:piece + size, :]

            @pl.when(half == 1)
            def _():
                vector_out(ch).start()

    def seen_copy(off, dev, src):
        return remote(seen.at[src], seen.at[src], seen_send.at[off], seen_recv.at[src], dev)

    def pair_copy(off, dev, src):
        return remote(ops.at[src], ops.at[src], op_send.at[0, off], op_recv.at[0, src], dev)

    def right_copy(off, dev, src):
        return remote(moved.at[:, pl.ds(2 * dev, 2)], right_out.at[:, pl.ds(2 * src, 2)], op_send.at[1, off], op_recv.at[1, src], dev)

    def others():
        return [(off, lax.rem(me + off, DEVS)) for off in range(1, DEVS)]

    def send_right(first, last):
        for n in range(first, last):
            off = 3 * (n % 5) + n // 5 + 1
            right_copy(off, lax.rem(me + off, DEVS), me).start()

    slab_load = pltpu.make_async_copy(psi_rows.at[pl.ds(pl.multiple_of(me * BOND, 8), BOND)], cur, load_sem.at[0])
    left_load = pltpu.make_async_copy(left_hbm.at[:, 0:128], left.at[net.slots(())], load_sem.at[1])
    right_load = [pltpu.make_async_copy(right_hbm.at[:, 128 * n:128 * n + 128], y.at[n], load_sem.at[2 + n]) for n in range(5)]
    slab_load.start()
    left_load.start()
    for load in right_load:
        load.start()
    for t in range(2):
        ops[me, t] = jnp.concatenate([pair_loc[t].astype(f32), jnp.zeros((PAIR, LANES - PAIR), f32)], axis=1).astype(bf)
    entry_barrier(me)
    slab_load.wait()
    square, = dots(lambda rows: (cur[rows, :] * cur[rows, :],), 1)
    row = iota((8, LANES), 0)
    full = jnp.where(row == 1, flags[0], flags[1]).astype(f32)
    seen[me] = jnp.where(row == 0, jnp.sum(square, axis=0, keepdims=True), full)
    for off, dev in others():
        seen_copy(off, dev, me).start()
    for off, dev in others():
        pair_copy(off, dev, me).start()
    left_load.wait()
    net.own_out(left_view, net.at(0))
    for load in right_load:
        load.wait()
    spread_right()
    send_right(0, 5)
    own = pl.ds(2 * me, 2)
    right_own = pltpu.make_async_copy(moved.at[:, own], right_out.at[:, own], load_sem.at[0])
    right_own.start()
    for off, dev in others():
        seen_copy(off, dev, dev).wait_recv()
    norm = jnp.sqrt(jnp.sum(jnp.sum(seen[:, 0:1, :], axis=0)) / VEC_SIZE)
    norm_out[0] = norm
    term, lane = iota((TERMS, LANES), 0), iota((TERMS, LANES), 1)
    full = jnp.concatenate([seen[src, 1:3, :] for src in range(DEVS)], axis=0)
    in_lanes = jnp.sum(jnp.where(term == lane, full, 0.0), axis=0, keepdims=True)
    rank = jnp.sum(jnp.where(term < lane, full, 0.0), axis=0, keepdims=True)
    rank_down = jnp.sum(jnp.where(lane < term, in_lanes, 0.0), axis=1, keepdims=True)
    holder = jnp.sum(jnp.where(rank_down == lane.astype(f32), full * term.astype(f32), 0.0), axis=0, keepdims=True)
    table[...] = jnp.where(row == 1, holder, jnp.where(in_lanes > 0.5, rank, jnp.where(row == 0, FEW, TERMS).astype(f32))).astype(jnp.int32)
    few[0] = jnp.where(jnp.sum(in_lanes) < FEW + 0.5, 1, 0)
    pl.run_scoped(functools.partial(start_vector, norm), pltpu.VMEM((5, 128, 8, LANES), f32), pltpu.VMEM((8, 256, LANES), f32))
    slab_out = pltpu.make_async_copy(cur, slab_hbm, load_sem.at[1])
    slab_out.start()
    for off, dev in others():
        pair_copy(off, dev, dev).wait_recv()
    build_pairs()
    wi_out = pltpu.make_async_copy(wi, wi_hbm, load_sem.at[2])
    wi_out.start()
    net.take_pairs(left_view, net.at(0))
    net.take_last(left_view, net.at(0))
    net.chunk_ready(left_view, net.at(0))
    all_left = pltpu.make_async_copy(left, left_out, load_sem.at[3])
    all_left.start()
    net.drain_sends(left_view, net.at(0))
    for off, dev in others():
        right_copy(off, dev, dev).wait_recv()
    for off, dev in others():
        seen_copy(off, dev, me).wait_send()
        pair_copy(off, dev, me).wait_send()
        right_copy(off, dev, me).wait_send()
    right_own.wait()
    slab_out.wait()
    wi_out.wait()
    all_left.wait()
    for ch in range(CHUNKS):
        vector_out(ch).wait()


VECTOR_SHAPE = (CHUNKS, 8, 2, 2, 2, 2, 80, LANES)


def prepare(flags, psi, pair_loc, right_loc, left_loc):
    smem = pl.BlockSpec(memory_space=pltpu.SMEM)
    vmem = pl.BlockSpec(memory_space=pltpu.VMEM)
    hbm = pl.BlockSpec(memory_space=pltpu.HBM)
    dma = pltpu.SemaphoreType.DMA
    return pl.pallas_call(
        prep_kernel,
        out_shape=(
            jax.ShapeDtypeStruct((8, LANES), jnp.int32), jax.ShapeDtypeStruct((1,), jnp.int32), jax.ShapeDtypeStruct((1,), f32),
            jax.ShapeDtypeStruct(VECTOR_SHAPE, bf), jax.ShapeDtypeStruct((BOND, BOND), f32),
            jax.ShapeDtypeStruct((DEVS, 2, 256, 256), bf), jax.ShapeDtypeStruct((5, TERMS, SLAB, LANES), bf), jax.ShapeDtypeStruct((2, 2, 2, 2, 2, 128, BOND), bf),
        ),
        in_specs=[smem, hbm, hbm, vmem, hbm, hbm],
        out_specs=(vmem, smem, smem, hbm, hbm, hbm, hbm, hbm),
        scratch_shapes=[
            pltpu.VMEM(VECTOR_SHAPE, bf),
            pltpu.VMEM((5, 2 * BOND, LANES), bf),
            pltpu.VMEM((5, TERMS, SLAB, LANES), bf),
            pltpu.VMEM((BOND, BOND), f32),
            pltpu.VMEM((DEVS, 8, LANES), f32),
            pltpu.VMEM((DEVS, 2, PAIR, LANES), bf),
            pltpu.VMEM((DEVS, 2, 256, 256), bf),
            pltpu.VMEM((2, 2, 2, 2, 2, 128, BOND), bf),
            dma((8,)), dma((5,)), dma((CHUNKS,)), dma((DEVS,)), dma((DEVS,)), dma((2, DEVS)), dma((2, DEVS)),
            dma((1, 3, 7)), dma((1, 3, 7)), dma((1, 8)), dma((1, 8)),
        ],
        compiler_params=pltpu.CompilerParams(collective_id=0, has_side_effects=True, vmem_limit_bytes=67043328),
    )(flags, psi, psi.reshape(BOND * PAIR, BOND), pair_loc, right_loc.reshape(2 * BOND, BOND), left_loc)


def lanczos_kernel(most, table, u_hbm, slab_hbm, wi_hbm, right_hbm, first_left, left_hbm, gathered, alphas, betas,
                   u, lft, y, acc, cur, prev, ar, rc, wi,
                   load_sem, own_sem, ici_send, ici_recv, d2d_send, d2d_recv, ar_send, ar_recv, out_send, out_recv):
    me = lax.axis_index(AXIS_NAME)
    net = Gather(me, ici_send, ici_recv, d2d_send, d2d_recv)
    core, place = net.core, net.place

    def vec_view(ch, part, flips):
        pairs = PART_PAIRS[part] if part < 3 else (0, 8)
        return u.at[(ch, slice(pairs[0], pairs[1])) + net.slots(flips)]

    def left_view(ch, part, flips):
        lo, hi = LEFT_ROWS[part] if part < 3 else (0, 128)
        return lft.at[net.slots(flips) + (slice(None), slice(128 * ch + lo, 128 * ch + hi), slice(128 * ch, BOND))]

    def for_left(ch, what):
        for c in range(CHUNKS):
            @pl.when(ch == c)
            def _():
                what(left_view, net.at(c))

    def send_partial(which, partials):
        row = iota((8, LANES), 0)
        tile = jnp.zeros((8, LANES), f32)
        for n, partial in enumerate(partials):
            tile = jnp.where(row == n, jnp.sum(partial, axis=0, keepdims=True), tile)
        ar[which, me] = tile
        for off in range(1, DEVS):
            dev = lax.rem(me + off, DEVS)
            ref = ar.at[which, me]
            remote(ref, ref, ar_send.at[which, off], ar_recv.at[which, me], dev).start()

    def total_of(which, count):
        for off in range(1, DEVS):
            dev = lax.rem(me + off, DEVS)
            ref = ar.at[which, dev]
            remote(ref, ref, ar_send.at[which, off], ar_recv.at[which, dev], dev).wait_recv()
        total = jnp.sum(ar[which], axis=0)
        sums = [jnp.sum(total[n:n + 1]) / VEC_SIZE for n in range(count)]
        for off in range(1, DEVS):
            dev = lax.rem(me + off, DEVS)
            ref = ar.at[which, me]
            remote(ref, ref, ar_send.at[which, off], ar_recv.at[which, me], dev).wait_send()
        return sums

    def dots(fn, count):
        def body(g, tots):
            rows = pl.ds(pl.multiple_of(g * 16, 16), 16)
            out = []
            for tot, val in zip(tots, fn(rows)):
                for r in range(2):
                    for c in range(5):
                        tot = tot + val[8 * r:8 * r + 8, 128 * c:128 * c + 128]
                out.append(tot)
            return tuple(out)
        return lax.fori_loop(0, 40, body, (jnp.zeros((8, LANES), f32),) * count)

    def write_u():
        for ch in range(CHUNKS):
            lanes = slice(128 * ch, 128 * ch + 128)
            for i in range(8):
                dst = u.at[ch, i, place[2], place[1], place[0], core]
                dst[0:16] = cur[32 * i:32 * i + 16, lanes].astype(bf)
                dst[16:32] = cur[256 + 32 * i:256 + 32 * i + 16, lanes].astype(bf)
                dst[32:48] = cur[32 * i + 16:32 * i + 32, lanes].astype(bf)
                dst[48:64] = cur[256 + 32 * i + 16:256 + 32 * i + 32, lanes].astype(bf)
                dst[64:80] = cur[512 + 16 * i:512 + 16 * i + 16, lanes].astype(bf)

    def right_phase(ch, middle):
        for par in range(2):
            if par == 1:
                middle()
            rhs = []
            for i in range(8):
                main = u[ch, i, :, :, :, :, 32 * par:32 * par + 32, :].reshape(512, 128)
                tail = u[ch, i, :, :, :, :, 64:80, :].reshape(256, 128)
                rhs.append(jnp.concatenate([main, tail], axis=0))
            rhs = jnp.concatenate(rhs, axis=1)
            lhs = jnp.concatenate([rc[:, 0:512], rc[:, 512 + 256 * par:768 + 256 * par]], axis=1)
            val = jnp.dot(lhs, rhs, preferred_element_type=f32)
            for i in range(8):
                y[2 * i + par, 0:most] = val[:, 128 * i:128 * i + 128].reshape(most, SLAB, 128).astype(bf)
                own = u.at[ch, i, place[2], place[1], place[0], core]
                y[2 * i + par, most, 0:32] = own[32 * par:32 * par + 32, :]
                y[2 * i + par, most, 32:40] = own[64 + 8 * par:72 + 8 * par, :]

    def pair_left_phase(ch, zb, half_done):
        low_rows = (iota((256, 256), 0) & 15) < 8

        @pl.loop(0, 2)
        def _(g):
            for s in range(8):
                k = g * 8 + s
                first, second = [table[0 if most == FEW else 2, 2 * k + t] for t in range(2)]

                def tile(at, row):
                    return y[:, at, row:row + 16, :].reshape(256, 128)

                z01 = jnp.dot(wi[k, 0], jnp.concatenate([tile(first, 0), tile(first, 16)], axis=1), preferred_element_type=f32).astype(bf)
                mixed = jnp.where(low_rows, wi[k, 0], wi[k, 1])
                ends = jnp.concatenate([y[:, at, 32:40, :] for at in (first, second)], axis=1).reshape(256, 128)
                z2 = jnp.dot(mixed, ends, preferred_element_type=f32).reshape(16, 2, 8, 128)
                z34 = jnp.dot(wi[k, 1], jnp.concatenate([tile(second, 0), tile(second, 16)], axis=1), preferred_element_type=f32).astype(bf)
                zb[s, 0:256, 0:128] = z01[:, 0:128]
                zb[s, 256:512, 0:128] = z01[:, 128:256]
                zb[s, 512:640, 0:128] = z2[:, 0].reshape(128, 128).astype(bf)
                zb[s, 0:256, 128:256] = z34[:, 0:128]
                zb[s, 256:512, 128:256] = z34[:, 128:256]
                zb[s, 512:640, 128:256] = z2[:, 1].reshape(128, 128).astype(bf)
            lhs = jnp.concatenate([zb[s] for s in range(8)], axis=1)
            rows = pl.ds(pl.multiple_of(ch * 128, 128), 128)
            rhs = jnp.concatenate([lft[g, s // 4, s // 2 % 2, s % 2, t, rows, :] for s in range(8) for t in range(2)], axis=0)
            acc[...] += jnp.dot(lhs, rhs, preferred_element_type=f32)

            @pl.when(g == 0)
            def _():
                half_done()

    def turn(vec, turned):
        shifted = [lax.rem(q + DEVS - me, DEVS) for q in range(PAIR)]
        for lt in range(5):
            rows = []
            for n in range(16 * lt, 16 * lt + 16):
                q, part = shifted[n // 5], n % 5
                start = 512 + 8 * q if part == 4 else 256 * (part // 2) + 16 * q + 8 * (part % 2)
                rows.append(vec[pl.ds(pl.multiple_of(start, 8), 8), :])
            turned[:, 128 * lt:128 * lt + 128] = jnp.concatenate(rows, axis=0).T

    def flipped(mask):
        dev = me
        for n, bit in enumerate((core,) + place):
            if mask >> n & 1:
                dev = dev + (1 << n) * (1 - 2 * bit)
        return dev

    def out_copy(turned, vec, mask, final, arriving=False):
        dev = flipped(mask)
        src = dev if arriving else me
        rows = pl.ds(pl.multiple_of(dev * SLAB, 8), SLAB)
        return remote(turned.at[rows], gathered.at[vec, src], out_send.at[mask], out_recv.at[final, mask], dev)

    def own_copy(turned, vec):
        rows = pl.ds(pl.multiple_of(me * SLAB, 8), SLAB)
        return pltpu.make_async_copy(turned.at[rows], gathered.at[vec, me], own_sem)

    def send_out(turned, vec, masks, final=0):
        for mask in masks:
            out_copy(turned, vec, mask, final).start()

    def finish_out(turned, vec, final=0):
        own_copy(turned, vec).wait()
        for mask in range(1, DEVS):
            out_copy(turned, vec, mask, final, True).wait_recv()
        for mask in range(1, DEVS):
            out_copy(turned, vec, mask, final).wait_send()

    def build_right():
        for n in range(most):
            for t in range(5):
                rc[SLAB * n:SLAB * n + SLAB, 128 * t:128 * t + 128] = y[t, table[1, n]]
        tails = rc[:, 512:640]
        src = iota((128, 256), 0)
        spot = 16 * (src >> 3) + (src & 7)
        for par in range(2):
            widen = (spot + 8 * par == iota((128, 256), 1)).astype(bf)
            rc[:, 512 + 256 * par:768 + 256 * par] = jnp.dot(tails, widen, preferred_element_type=f32).astype(bf)

    def mirror_left(ch):
        @pl.loop(0, 8)
        def _(g):
            for n in range(4):
                at = (g // 4, lax.rem(g // 2, 2), lax.rem(g, 2), n // 2, n % 2)
                for other in range(ch + 1, CHUNKS):
                    block = lft[at + (slice(128 * ch, 128 * ch + 128), slice(128 * other, 128 * other + 128))]
                    lft[at + (slice(128 * other, 128 * other + 128), slice(128 * ch, 128 * ch + 128))] = block.T

    left_load = pltpu.make_async_copy(left_hbm.at[:, 128:BOND], lft.at[net.slots(()) + (slice(None), slice(128, BOND))], load_sem.at[0])
    right_load = pltpu.make_async_copy(right_hbm, y.at[0:5, 0:TERMS], load_sem.at[1])
    wi_load = pltpu.make_async_copy(wi_hbm, wi, load_sem.at[2])
    slab_load = pltpu.make_async_copy(slab_hbm, cur, load_sem.at[3])
    first_load = pltpu.make_async_copy(first_left, lft.at[:, :, :, :, :, 0:128], load_sem.at[4])

    def vector_load(ch):
        return pltpu.make_async_copy(u_hbm.at[ch], u.at[ch], load_sem.at[5 + ch])

    left_load.start()
    right_load.start()
    vector_load(0).start()
    wi_load.start()
    first_load.start()
    for ch in range(1, CHUNKS):
        vector_load(ch).start()
    slab_load.start()
    entry_barrier(me)
    left_load.wait()
    net.own_out(left_view, net.at(1))
    right_load.wait()
    build_right()
    prev[...] = jnp.zeros_like(prev)

    def step(zb, turned, j, beta_prev):
        later = j > 0

        @pl.when(later)
        def _():
            zero, one = net.at(0), net.at(1)
            net.own_out(vec_view, zero)
            turn(cur, turned)
            own_copy(turned, j - 1).start()
            net.relay_first(vec_view, zero)
            net.relay_second(vec_view, zero)
            net.relay_last(vec_view, zero)
            net.own_out(vec_view, one)
            net.relay_third(vec_view, zero)
            net.take_pairs(vec_view, zero)
            net.take_last(vec_view, zero)
            net.relay_first(vec_view, one)
            net.chunk_ready(vec_view, zero)

        acc[...] = jnp.zeros_like(acc)

        @pl.loop(0, CHUNKS)
        def _(ch):
            next_spot, after_spot = net.at(ch + 1), net.at(ch + 2)

            @pl.when(later & (ch + 1 < CHUNKS))
            def _():
                net.relay_second(vec_view, next_spot)

            @pl.when(later & (ch == 4))
            def _():
                send_out(turned, j - 1, (7, 13, 11))

            @pl.when(j == 0)
            def _():
                vector_load(ch).wait()

            def middle():
                @pl.when(later & (ch + 1 < CHUNKS))
                def _():
                    net.relay_third(vec_view, next_spot)
                    net.relay_last(vec_view, next_spot)

                    @pl.when(ch + 2 < CHUNKS)
                    def _():
                        net.own_out(vec_view, after_spot)

                    @pl.when(ch == 3)
                    def _():
                        send_out(turned, j - 1, (1, 3, 5, 9, 14, 15))

                @pl.when((j == 0) & (ch > 0))
                def _():
                    def take(view, spot):
                        net.take_pairs(view, spot)
                        net.take_last(view, spot)

                    for_left(ch, take)

            right_phase(ch, middle)

            @pl.when(j == 0)
            def _():
                @pl.when(ch == 0)
                def _():
                    wi_load.wait()
                    first_load.wait()

                def left_ready(view, spot):
                    if spot.ch > 0:
                        mirror_left(spot.ch - 1)
                        net.chunk_ready(view, spot)

                for_left(ch, left_ready)
                for_left(ch + 1, net.relay_first)

            def half_done():
                @pl.when(later & (ch + 1 < CHUNKS))
                def _():
                    net.take_pairs(vec_view, next_spot)
                    net.take_last(vec_view, next_spot)

                    @pl.when(ch + 2 < CHUNKS)
                    def _():
                        net.relay_first(vec_view, after_spot)

                    @pl.when(ch == 2)
                    def _():
                        send_out(turned, j - 1, (2, 4, 8))

                    @pl.when(ch == 3)
                    def _():
                        send_out(turned, j - 1, (6, 12, 10))

                @pl.when(j == 0)
                def _():
                    for_left(ch + 1, net.relay_second)

            pair_left_phase(ch, zb, half_done)

            @pl.when(later & (ch + 1 < CHUNKS))
            def _():
                net.chunk_ready(vec_view, next_spot)

            @pl.when(j == 0)
            def _():
                def advance(view, spot):
                    net.relay_third(view, spot)
                    net.relay_last(view, spot)

                for_left(ch + 1, advance)
                for_left(ch + 2, net.own_out)

        @pl.loop(0, CHUNKS)
        def _(ch):
            @pl.when((j == 0) & (ch > 0))
            def _():
                for_left(ch, net.drain_sends)

            @pl.when(later)
            def _():
                net.drain_sends(vec_view, net.at(ch))

        @pl.when(j == 0)
        def _():
            slab_load.wait()

        @pl.when(j == 0)
        def _():
            send_partial(0, dots(lambda rows: (acc[rows, :] * cur[rows, :],), 1))
            betas[0, LANCZOS_STEPS + 1] = total_of(0, 1)[0]

        shift = betas[0, LANCZOS_STEPS + 1]

        def products(rows):
            v, v_prev = cur[rows, :], prev[rows, :]
            w = acc[rows, :] - shift * v - beta_prev * v_prev
            acc[rows, :] = w
            return w * w, w * v, v * v, v * v_prev

        send_partial(1, dots(products, 4))

        @pl.when(later)
        def _():
            finish_out(turned, j - 1)

        @pl.when(j + 1 == LANCZOS_STEPS)
        def _():
            turn(acc, turned)
            own_copy(turned, j).start()
            send_out(turned, j, (14, 15, 6, 12, 10, 7, 13, 11, 2, 4, 8, 3, 5, 9, 1), 1)

        ww, wv, vv, vp = total_of(1, 4)
        alpha = wv + shift * vv + beta_prev * vp
        extra = alpha - shift
        beta = jnp.sqrt(ww - 2.0 * extra * wv + extra * extra * vv)
        alphas[0, j] = alpha
        betas[0, j] = beta
        betas[0, LANCZOS_STEPS] = extra
        betas[0, LANCZOS_STEPS + 1] = alpha

        @pl.when(j + 1 < LANCZOS_STEPS)
        def _():
            @pl.loop(0, 40)
            def _(g):
                rows = pl.ds(pl.multiple_of(g * 16, 16), 16)
                v = cur[rows, :]
                prev[rows, :] = v
                cur[rows, :] = (acc[rows, :] - extra * v) / beta

            write_u()

        return beta

    def all_steps(zb, turned):
        lax.fori_loop(0, LANCZOS_STEPS, functools.partial(step, zb, turned), jnp.zeros((), f32))
        finish_out(turned, LANCZOS_STEPS - 1, 1)

    pl.run_scoped(all_steps, pltpu.VMEM((8, BOND, 256), bf), pltpu.VMEM((BOND, BOND), f32))


def run_lanczos(most, table, u_hbm, slab_hbm, wi_hbm, right_hbm, first_left, left_loc):
    smem = pl.BlockSpec(memory_space=pltpu.SMEM)
    hbm = pl.BlockSpec(memory_space=pltpu.HBM)
    dma = pltpu.SemaphoreType.DMA
    return pl.pallas_call(
        functools.partial(lanczos_kernel, most),
        out_shape=(jax.ShapeDtypeStruct((LANCZOS_STEPS, DEVS, SLAB, BOND), f32), jax.ShapeDtypeStruct((1, 8), f32), jax.ShapeDtypeStruct((1, 8), f32)),
        in_specs=[smem] + [hbm] * 6,
        out_specs=(hbm, smem, smem),
        scratch_shapes=[
            pltpu.VMEM(VECTOR_SHAPE, bf),
            pltpu.VMEM((2, 2, 2, 2, 2, BOND, BOND), bf),
            pltpu.VMEM((PAIR, TERMS + 1, SLAB, LANES), bf),
            pltpu.VMEM((BOND, BOND), f32),
            pltpu.VMEM((BOND, BOND), f32),
            pltpu.VMEM((BOND, BOND), f32),
            pltpu.VMEM((2, DEVS, 8, LANES), f32),
            pltpu.VMEM((most * SLAB, 1024), bf),
            pltpu.VMEM((DEVS, 2, 256, 256), bf),
            dma((5 + CHUNKS,)), dma, dma((CHUNKS, 3, 7)), dma((CHUNKS, 3, 7)), dma((CHUNKS, 8)), dma((CHUNKS, 8)),
            dma((2, DEVS)), dma((2, DEVS)), dma((DEVS,)), dma((2, DEVS)),
        ],
        compiler_params=pltpu.CompilerParams(collective_id=most, has_side_effects=True, vmem_limit_bytes=67043328),
    )(table, u_hbm, slab_hbm, wi_hbm, right_hbm, first_left, left_loc)


def place_kernel(norm, alphas, betas, psi, gathered, krylov, alpha_out, beta_out, rows, src, dst, load_sem, store_sem):
    me = lax.axis_index(AXIS_NAME)

    def load(vec):
        return pltpu.make_async_copy(gathered.at[vec], src.at[vec], load_sem.at[vec])

    def store(vec):
        return pltpu.make_async_copy(dst.at[vec], krylov.at[vec], store_sem.at[vec])

    def placed(vec, r, q):
        lane = iota((8, LANES), 1)
        tiles = []
        for t in range(5):
            tile = None
            for m in range(128 * t // SLAB, min(DEVS, (128 * t + 127) // SLAB + 1)):
                val = src[vec, (m - q) % DEVS, pl.ds(r, 8), 128 * t:128 * t + 128]
                tile = val if tile is None else jnp.where(lane >= SLAB * m - 128 * t, val, tile)
            tiles.append(tile)
        skip, rest = SLAB * q // 128, SLAB * q % 128
        if rest:
            tiles = [pltpu.roll(tile, 128 - rest, 1) for tile in tiles]
        tiles = [tiles[(t + skip) % 5] if not rest else jnp.where(lane < 128 - rest, tiles[(t + skip) % 5], tiles[(t + skip + 1) % 5]) for t in range(5)]
        return jnp.concatenate(tiles, axis=1)

    rows_load = pltpu.make_async_copy(psi.at[pl.ds(me * SLAB, SLAB)], rows, load_sem.at[LANCZOS_STEPS])
    rows_load.start()
    for vec in range(LANCZOS_STEPS):
        load(vec).start()
    for n in range(LANCZOS_STEPS):
        alpha_out[n] = alphas[0, n]
        beta_out[n] = betas[0, n]
    rows_load.wait()
    dst[0] = rows[...] / norm[0]
    store(0).start()

    @pl.loop(0, LANCZOS_STEPS - 1)
    def _(vec):
        load(vec).wait()
        for r in range(0, SLAB, 8):
            for q in range(PAIR):
                dst[vec + 1, r:r + 8, q, :] = placed(vec, r, q)
        store(vec + 1).start()

    load(LANCZOS_STEPS - 1).wait()
    for r in range(0, SLAB, 8):
        for q in range(PAIR):
            before = dst[LANCZOS_STEPS - 1, r:r + 8, q, :]
            dst[LANCZOS_STEPS, r:r + 8, q, :] = (placed(LANCZOS_STEPS - 1, r, q) - betas[0, LANCZOS_STEPS] * before) / betas[0, LANCZOS_STEPS - 1]
    store(LANCZOS_STEPS).start()
    for vec in range(LANCZOS_STEPS + 1):
        store(vec).wait()


def place_outputs(norm, alphas, betas, wavefunction, gathered):
    smem = pl.BlockSpec(memory_space=pltpu.SMEM)
    hbm = pl.BlockSpec(memory_space=pltpu.HBM)
    dma = pltpu.SemaphoreType.DMA
    return pl.pallas_call(
        place_kernel,
        out_shape=(jax.ShapeDtypeStruct((LANCZOS_STEPS + 1, SLAB, PAIR, BOND), f32), jax.ShapeDtypeStruct((LANCZOS_STEPS,), f32), jax.ShapeDtypeStruct((LANCZOS_STEPS,), f32)),
        in_specs=[smem, smem, smem, hbm, hbm],
        out_specs=(hbm, smem, smem),
        scratch_shapes=[
            pltpu.VMEM((SLAB, PAIR, BOND), f32),
            pltpu.VMEM((LANCZOS_STEPS, DEVS, SLAB, BOND), f32),
            pltpu.VMEM((LANCZOS_STEPS + 1, SLAB, PAIR, BOND), f32),
            dma((LANCZOS_STEPS + 1,)), dma((LANCZOS_STEPS + 1,)),
        ],
        compiler_params=pltpu.CompilerParams(vmem_limit_bytes=40 * 1024 * 1024),
    )(norm, alphas, betas, wavefunction, gathered)


def solution(mesh):
    def device_body(wavefunction, left_loc, pair_loc, right_loc, flag_loc):
        table, few, norm, *operands = prepare(flag_loc, wavefunction, pair_loc, right_loc, left_loc)
        few_full, all_full = functools.partial(run_lanczos, FEW), functools.partial(run_lanczos, TERMS)
        vecs, alphas, betas = lax.cond(few[0] == 1, few_full, all_full, table, *operands, left_loc)
        return place_outputs(norm, alphas, betas, wavefunction, vecs)

    return jax.shard_map(device_body, mesh=mesh, in_specs=(P(), P(AXIS_NAME), P(AXIS_NAME), P(AXIS_NAME), P(AXIS_NAME)), out_specs=(P(None, AXIS_NAME), P(), P()), check_vma=False)
```

```python
import functools
import jax
import jax.numpy as jnp
from jax import lax
from jax.experimental import pallas as pl
from jax.sharding import PartitionSpec as P
from jax.experimental.pallas import tpu as pltpu

LANCZOS_STEPS = 6
AXIS_NAME = 'terms'
BOND = 640
PAIR = 16
TERMS = 32
DEVS = 16
SLAB = BOND // DEVS
CHUNKS = 5
FEWER, FEW = 16, 20
TABLE_ROW = {16: 0, 20: 2, 32: 3}
LANES = 128
VEC_SIZE = BOND * PAIR * BOND
bf = jnp.bfloat16
f32 = jnp.float32
MESH = pl.DeviceIdType.MESH
PART_PAIRS = ((0, 3), (3, 6), (6, 8))
LEFT_ROWS = ((0, 48), (48, 96), (96, 128))
AXES = ((1, 0, 0), (0, 1, 0), (0, 0, 1))
D2D_FLIPS = ((0,), (1,), (2,), (0, 1), (0, 2), (1, 2), (0, 1, 2), ())


def entry_barrier(me):
    barrier = pltpu.get_barrier_semaphore()
    for off in range(1, DEVS):
        pl.semaphore_signal(barrier, inc=1, device_id=(lax.rem(me + off, DEVS),), device_id_type=MESH)
    pl.semaphore_wait(barrier, DEVS - 1)


def iota(shape, dim):
    return lax.broadcasted_iota(jnp.int32, shape, dim)


def remote(ref, dst_ref, send, recv, dev):
    return pltpu.make_async_remote_copy(src_ref=ref, dst_ref=dst_ref, send_sem=send, recv_sem=recv, device_id=(dev,), device_id_type=MESH)


class Spot:
    def __init__(self, net, ch):
        self.ch = ch
        self.hits, self.across = [], []
        for n in range(3):
            axis = (n + ch) % 3 if isinstance(ch, int) else lax.rem(n + ch, 3)
            one = axis * (2 - axis)
            two = axis * (axis - 1) // 2 if isinstance(ch, int) else lax.div(axis * (axis - 1), 2)
            hit = (1 - one - two, one, two)
            self.hits.append(hit)
            self.across.append(net.me + hit[0] * net.step[0] + hit[1] * net.step[1] + hit[2] * net.step[2])


class Gather:
    def __init__(self, me, ici_send, ici_recv, d2d_send, d2d_recv):
        self.me, self.sems = me, (ici_send, ici_recv, d2d_send, d2d_recv)
        self.core = lax.rem(me, 2)
        self.place = (lax.rem(lax.div(me, 2), 2), lax.rem(lax.div(me, 4), 2), lax.div(me, 8))
        self.turn = tuple(1 - 2 * at for at in self.place)
        self.step = tuple((2 << n) * turn for n, turn in enumerate(self.turn))
        self.partner = me + 1 - 2 * self.core

    def at(self, ch):
        return Spot(self, ch)

    def slots(self, hits):
        idx = []
        for n in (2, 1, 0):
            moved = self.place[n]
            for hit in hits:
                if not isinstance(hit[n], int) or hit[n]:
                    moved = moved + hit[n] * self.turn[n]
            idx.append(moved)
        return tuple(idx) + (self.core,)

    def unit(self, view, spot, part, n, arriving=False):
        flips, axis = (((), 0), ((), 1), ((), 2), ((0,), 1), ((0,), 2), ((1,), 2), ((0, 1), 2))[n]
        hits = [spot.hits[(part + m) % 3] for m in (flips + (axis,) if arriving else flips)]
        ref = view(spot.ch, part, hits)
        return remote(ref, ref, self.sems[0].at[spot.ch, part, n], self.sems[1].at[spot.ch, part, n], spot.across[(part + axis) % 3])

    def start_units(self, view, spot, *which):
        for n in which:
            for part in range(3):
                self.unit(view, spot, part, n).start()

    def wait_units(self, view, spot, *which):
        for n in which:
            for part in range(3):
                self.unit(view, spot, part, n, True).wait_recv()

    def d2d(self, view, spot, n):
        ref = view(spot.ch, 3, [AXES[m] for m in D2D_FLIPS[n]])
        return remote(ref, ref, self.sems[2].at[spot.ch, n], self.sems[3].at[spot.ch, n], self.partner)

    def own_out(self, view, spot):
        self.start_units(view, spot, 0, 1, 2)
        self.d2d(view, spot, 7).start()

    def relay_first(self, view, spot):
        for part in range(3):
            self.unit(view, spot, part, 0, True).wait_recv()
            self.unit(view, spot, part, 3).start()
        self.start_units(view, spot, 4)

    def relay_second(self, view, spot):
        for part in range(3):
            self.unit(view, spot, part, 1, True).wait_recv()
            self.unit(view, spot, part, 5).start()

    def relay_third(self, view, spot):
        self.wait_units(view, spot, 2)
        for n in (0, 1, 2):
            self.d2d(view, spot, n).start()

    def relay_last(self, view, spot):
        for part in range(3):
            self.unit(view, spot, part, 3, True).wait_recv()
            self.unit(view, spot, part, 6).start()

    def take_pairs(self, view, spot):
        self.wait_units(view, spot, 4, 5)
        for n in (3, 4, 5):
            self.d2d(view, spot, n).start()

    def take_last(self, view, spot):
        self.wait_units(view, spot, 6)
        self.d2d(view, spot, 6).start()

    def wait_d2d(self, view, spot, *which):
        for n in which:
            self.d2d(view, spot, n).wait_recv()

    def chunk_ready(self, view, spot):
        self.wait_d2d(view, spot, *range(8))

    def drain_sends(self, view, spot):
        for n in range(8):
            self.d2d(view, spot, n).wait_send()
        for n in range(7):
            for part in range(3):
                self.unit(view, spot, part, n).wait_send()


def prep_kernel(flags, psi, psi_rows, pair_loc, right_hbm, left_hbm, table, few, norm_out, u_hbm, slab_hbm, wi_hbm, right_out, left_out,
                u, y, moved, cur, seen, ops, wi, left, load_sem, stage_sem, out_sem, seen_send, seen_recv, op_send, op_recv, ici_send, ici_recv, d2d_send, d2d_recv, left_sem, small_i, small_f):
    me = lax.axis_index(AXIS_NAME)
    net = Gather(me, ici_send, ici_recv, d2d_send, d2d_recv)

    def left_view(ch, part, flips):
        lo, hi = LEFT_ROWS[part] if part < 3 else (0, 128)
        return left.at[net.slots(flips) + (slice(None), slice(lo, hi))]

    def dots(fn, count):
        def body(g, tots):
            vals = fn(pl.ds(pl.multiple_of(g * 32, 32), 32))
            out = []
            for n, val in enumerate(vals):
                two = [tots[2 * n], tots[2 * n + 1]]
                for r in range(4):
                    for c in range(5):
                        two[r % 2] = two[r % 2] + val[8 * r:8 * r + 8, 128 * c:128 * c + 128]
                out += two
            return tuple(out)
        tots = lax.fori_loop(0, 20, body, (jnp.zeros((8, LANES), f32),) * (2 * count))
        return [tots[2 * n] + tots[2 * n + 1] for n in range(count)]

    def spread_right():
        col = iota((BOND, 128), 0)
        source = (col * 1639) >> 16
        within = col - source * SLAB
        target = jnp.where(within < 32, source * 32 + within, 480 + source * 8 + within)
        for t in range(5):
            perm = (target == iota((BOND, 128), 1) + 128 * t).astype(f32).astype(bf)
            for k in range(2):
                rows = jnp.concatenate([y[n, BOND * k:BOND * k + BOND, :] for n in range(5)], axis=1)
                val = jnp.dot(rows, perm, preferred_element_type=f32).reshape(DEVS, SLAB, 128)
                if k == 0:
                    first = val
            moved[t] = jnp.concatenate([first[:, None], val[:, None]], axis=1).reshape(TERMS, SLAB, 128).astype(bf)

    def build_pairs():
        widen = ((iota((128, 256), 1) >> 4) == iota((128, 256), 0)).astype(bf)
        same = (iota((256, 256), 0) & 15) == (iota((256, 256), 1) & 15)

        @pl.loop(0, DEVS)
        def _(k):
            wide = []
            for t in range(2):
                tall = jnp.broadcast_to(ops[k, t].astype(f32)[:, None, :], (16, 16, 128)).reshape(256, 128).astype(bf)
                wide.append(jnp.where(same, jnp.dot(tall, widen, preferred_element_type=f32), 0.0))
            wi[k, 0] = wide[0].astype(bf)
            wi[k, 1] = wide[1].astype(bf)

    def tile_load(stage, t, ch, half):
        rows, qs = pl.ds(pl.multiple_of(128 * ch, 128), 128), pl.ds(pl.multiple_of(8 * half, 8), 8)
        return pltpu.make_async_copy(psi.at[rows, qs, 128 * t:128 * t + 128], stage.at[t], stage_sem.at[t])

    def vector_out(ch):
        return pltpu.make_async_copy(u.at[ch], u_hbm.at[ch], out_sem.at[ch])

    def start_vector(norm, stage, flip):
        base = (me * SLAB) // 128
        skip = pl.multiple_of(me * SLAB - base * 128, 8)
        for t in range(5):
            tile_load(stage, t, 0, 0).start()

        @pl.loop(0, 2 * CHUNKS)
        def _(it):
            ch, half = it // 2, lax.rem(it, 2)
            @pl.when(it == 3)
            def _():
                net.relay_first(left_view, net.at(0))

            @pl.when(it == 4)
            def _():
                net.relay_second(left_view, net.at(0))
                send_right(5, 10)

            @pl.when(it == 6)
            def _():
                net.relay_third(left_view, net.at(0))
                for n in (7, 0, 1, 2):
                    left_store(n).start()

            @pl.when(it == 8)
            def _():
                net.relay_last(left_view, net.at(0))
                send_right(10, 15)

            for t in range(5):
                tile_load(stage, t, ch, half).wait()

                @pl.when((base == t) | (base + 1 == t))
                def _():
                    rows = pl.ds(pl.multiple_of(128 * (t - base), 128), 128)
                    for q in range(8):
                        flip[q, rows, :] = stage[t, :, q, :].T

                for q in range(8):
                    val = (stage[t, :, q, :].T / norm).astype(bf)
                    for m in range(16):
                        src, piece = (16 * t + m) // 5, (16 * t + m) % 5
                        row = 64 + 8 * (q % 2) if piece == 4 else 32 * (q % 2) + 8 * piece
                        u[ch, 4 * half + q // 2, src // 8, src // 4 % 2, src // 2 % 2, src % 2, row:row + 8, :] = val[8 * m:8 * m + 8, :]

                @pl.when(it + 1 < 2 * CHUNKS)
                def _():
                    tile_load(stage, t, (it + 1) // 2, lax.rem(it + 1, 2)).start()

            lanes = pl.ds(pl.multiple_of(128 * ch, 128), 128)
            for q in range(8):
                val = flip[q, pl.ds(skip, SLAB), :] / norm
                row = 128 * half + 16 * q
                for start, piece, size in ((row, 0, 16), (256 + row, 16, 16), (512 + 64 * half + 8 * q, 32, 8)):
                    cur[pl.ds(pl.multiple_of(start, 8), size), lanes] = val[piece:piece + size, :]

            @pl.when(half == 1)
            def _():
                vector_out(ch).start()

    def left_store(n, other=False):
        at = net.slots([AXES[m] for m in D2D_FLIPS[n]])
        at = at[:3] + ((1 - net.core,) if other else at[3:])
        return pltpu.make_async_copy(left.at[at], left_out.at[at], left_sem.at[int(other), n])

    def seen_copy(off, dev, src):
        return remote(seen.at[src], seen.at[src], seen_send.at[off], seen_recv.at[src], dev)

    def pair_copy(off, dev, src):
        return remote(ops.at[src], ops.at[src], op_send.at[0, off], op_recv.at[0, src], dev)

    def right_copy(off, dev, src):
        return remote(moved.at[:, pl.ds(2 * dev, 2)], right_out.at[:, pl.ds(2 * src, 2)], op_send.at[1, off], op_recv.at[1, src], dev)

    def others():
        return [(off, lax.rem(me + off, DEVS)) for off in range(1, DEVS)]

    def send_right(first, last):
        for n in range(first, last):
            off = 3 * (n % 5) + n // 5 + 1
            right_copy(off, lax.rem(me + off, DEVS), me).start()

    slab_load = pltpu.make_async_copy(psi_rows.at[pl.ds(pl.multiple_of(me * BOND, 8), BOND)], cur, load_sem.at[0])
    left_load = pltpu.make_async_copy(left_hbm.at[:, 0:128], left.at[net.slots(())], load_sem.at[1])
    right_load = [pltpu.make_async_copy(right_hbm.at[:, 128 * n:128 * n + 128], y.at[n], load_sem.at[2 + n]) for n in range(5)]
    slab_load.start()
    left_load.start()
    for load in right_load:
        load.start()
    for t in range(2):
        ops[me, t] = jnp.concatenate([pair_loc[t].astype(f32), jnp.zeros((PAIR, LANES - PAIR), f32)], axis=1).astype(bf)
    entry_barrier(me)
    slab_load.wait()
    square, = dots(lambda rows: (cur[rows, :] * cur[rows, :],), 1)
    row = iota((8, LANES), 0)
    full = jnp.where(row == 1, flags[0], flags[1]).astype(f32)
    seen[me] = jnp.where(row == 0, jnp.sum(square, axis=0, keepdims=True), full)
    for off, dev in others():
        seen_copy(off, dev, me).start()
    for off, dev in others():
        pair_copy(off, dev, me).start()
    left_load.wait()
    net.own_out(left_view, net.at(0))
    for load in right_load:
        load.wait()
    spread_right()
    send_right(0, 5)
    own = pl.ds(2 * me, 2)
    right_own = pltpu.make_async_copy(moved.at[:, own], right_out.at[:, own], load_sem.at[0])
    right_own.start()
    for off, dev in others():
        seen_copy(off, dev, dev).wait_recv()
    norm = jnp.sqrt(jnp.sum(jnp.sum(seen[:, 0:1, :], axis=0)) / VEC_SIZE)
    small_f[...] = jnp.zeros((8, LANES), f32) + norm
    norm_store = pltpu.make_async_copy(small_f, norm_out, load_sem.at[6])
    norm_store.start()
    term, lane = iota((TERMS, LANES), 0), iota((TERMS, LANES), 1)
    full = jnp.concatenate([seen[src, 1:3, :] for src in range(DEVS)], axis=0)
    in_lanes = jnp.sum(jnp.where(term == lane, full, 0.0), axis=0, keepdims=True)
    rank = jnp.sum(jnp.where(term < lane, full, 0.0), axis=0, keepdims=True)
    rank_down = jnp.sum(jnp.where(lane < term, in_lanes, 0.0), axis=1, keepdims=True)
    holder = jnp.sum(jnp.where(rank_down == lane.astype(f32), full * term.astype(f32), 0.0), axis=0, keepdims=True)
    small_i[...] = jnp.where(row == 1, holder, jnp.where(in_lanes > 0.5, rank, jnp.where(row == 0, FEWER, jnp.where(row == 2, FEW, TERMS)).astype(f32))).astype(jnp.int32)
    count = jnp.sum(in_lanes)
    few[0] = jnp.where(count < FEW + 0.5, 0, 1)
    table_store = pltpu.make_async_copy(small_i, table, load_sem.at[7])
    table_store.start()
    pl.run_scoped(functools.partial(start_vector, norm), pltpu.VMEM((5, 128, 8, LANES), f32), pltpu.VMEM((8, 256, LANES), f32))
    slab_out = pltpu.make_async_copy(cur, slab_hbm, load_sem.at[1])
    slab_out.start()
    for off, dev in others():
        pair_copy(off, dev, dev).wait_recv()
    build_pairs()
    wi_out = pltpu.make_async_copy(wi, wi_hbm, load_sem.at[2])
    wi_out.start()
    net.take_pairs(left_view, net.at(0))
    for n in (3, 4, 5):
        left_store(n).start()
    net.wait_d2d(left_view, net.at(0), 7, 0, 1, 2)
    for n in (7, 0, 1, 2):
        left_store(n, True).start()
    net.take_last(left_view, net.at(0))
    left_store(6).start()
    net.wait_d2d(left_view, net.at(0), 3, 4, 5, 6)
    for n in (3, 4, 5, 6):
        left_store(n, True).start()
    net.drain_sends(left_view, net.at(0))
    for off, dev in others():
        right_copy(off, dev, dev).wait_recv()
    for off, dev in others():
        seen_copy(off, dev, me).wait_send()
        pair_copy(off, dev, me).wait_send()
        right_copy(off, dev, me).wait_send()
    right_own.wait()
    slab_out.wait()
    wi_out.wait()
    norm_store.wait()
    table_store.wait()
    for n in range(8):
        left_store(n).wait()
        left_store(n, True).wait()
    for ch in range(CHUNKS):
        vector_out(ch).wait()


VECTOR_SHAPE = (CHUNKS, 8, 2, 2, 2, 2, 80, LANES)


def prepare(flags, psi, pair_loc, right_loc, left_loc):
    smem = pl.BlockSpec(memory_space=pltpu.SMEM)
    vmem = pl.BlockSpec(memory_space=pltpu.VMEM)
    hbm = pl.BlockSpec(memory_space=pltpu.HBM)
    dma = pltpu.SemaphoreType.DMA
    return pl.pallas_call(
        prep_kernel,
        out_shape=(
            jax.ShapeDtypeStruct((8, LANES), jnp.int32), jax.ShapeDtypeStruct((1,), jnp.int32), jax.ShapeDtypeStruct((8, LANES), f32),
            jax.ShapeDtypeStruct(VECTOR_SHAPE, bf), jax.ShapeDtypeStruct((BOND, BOND), f32),
            jax.ShapeDtypeStruct((DEVS, 2, 256, 256), bf), jax.ShapeDtypeStruct((5, TERMS, SLAB, LANES), bf), jax.ShapeDtypeStruct((2, 2, 2, 2, 2, 128, BOND), bf),
        ),
        in_specs=[smem, hbm, hbm, vmem, hbm, hbm],
        out_specs=(hbm, smem, hbm, hbm, hbm, hbm, hbm, hbm),
        scratch_shapes=[
            pltpu.VMEM(VECTOR_SHAPE, bf),
            pltpu.VMEM((5, 2 * BOND, LANES), bf),
            pltpu.VMEM((5, TERMS, SLAB, LANES), bf),
            pltpu.VMEM((BOND, BOND), f32),
            pltpu.VMEM((DEVS, 8, LANES), f32),
            pltpu.VMEM((DEVS, 2, PAIR, LANES), bf),
            pltpu.VMEM((DEVS, 2, 256, 256), bf),
            pltpu.VMEM((2, 2, 2, 2, 2, 128, BOND), bf),
            dma((8,)), dma((5,)), dma((CHUNKS,)), dma((DEVS,)), dma((DEVS,)), dma((2, DEVS)), dma((2, DEVS)),
            dma((1, 3, 7)), dma((1, 3, 7)), dma((1, 8)), dma((1, 8)), dma((2, 8)),
            pltpu.VMEM((8, LANES), jnp.int32), pltpu.VMEM((8, LANES), f32),
        ],
        compiler_params=pltpu.CompilerParams(collective_id=0, has_side_effects=True, vmem_limit_bytes=67043328),
    )(flags, psi, psi.reshape(BOND * PAIR, BOND), pair_loc, right_loc.reshape(2 * BOND, BOND), left_loc)


def lanczos_kernel(most, table, u_hbm, slab_hbm, wi_hbm, right_hbm, first_left, left_hbm, gathered, alphas, betas,
                   u, lft, y, acc, cur, prev, ar, rc, wi,
                   load_sem, own_sem, ici_send, ici_recv, d2d_send, d2d_recv, ar_send, ar_recv, out_send, out_recv):
    me = lax.axis_index(AXIS_NAME)
    net = Gather(me, ici_send, ici_recv, d2d_send, d2d_recv)
    core, place = net.core, net.place

    def vec_view(ch, part, flips):
        pairs = PART_PAIRS[part] if part < 3 else (0, 8)
        return u.at[(ch, slice(pairs[0], pairs[1])) + net.slots(flips)]

    def left_view(ch, part, flips):
        lo, hi = LEFT_ROWS[part] if part < 3 else (0, 128)
        return lft.at[net.slots(flips) + (slice(None), slice(128 * ch + lo, 128 * ch + hi), slice(128 * ch, BOND))]

    def for_left(ch, what):
        for c in range(CHUNKS):
            @pl.when(ch == c)
            def _():
                what(left_view, net.at(c))

    def send_partial(which, partials):
        row = iota((8, LANES), 0)
        tile = jnp.zeros((8, LANES), f32)
        for n, partial in enumerate(partials):
            tile = jnp.where(row == n, jnp.sum(partial, axis=0, keepdims=True), tile)
        ar[which, me] = tile
        for off in range(1, DEVS):
            dev = lax.rem(me + off, DEVS)
            ref = ar.at[which, me]
            remote(ref, ref, ar_send.at[which, off], ar_recv.at[which, me], dev).start()

    def total_of(which, count):
        for off in range(1, DEVS):
            dev = lax.rem(me + off, DEVS)
            ref = ar.at[which, dev]
            remote(ref, ref, ar_send.at[which, off], ar_recv.at[which, dev], dev).wait_recv()
        total = jnp.sum(ar[which], axis=0)
        sums = [jnp.sum(total[n:n + 1]) / VEC_SIZE for n in range(count)]
        for off in range(1, DEVS):
            dev = lax.rem(me + off, DEVS)
            ref = ar.at[which, me]
            remote(ref, ref, ar_send.at[which, off], ar_recv.at[which, me], dev).wait_send()
        return sums

    def dots(fn, count):
        def body(g, tots):
            vals = fn(pl.ds(pl.multiple_of(g * 32, 32), 32))
            out = []
            for n, val in enumerate(vals):
                two = [tots[2 * n], tots[2 * n + 1]]
                for r in range(4):
                    for c in range(5):
                        two[r % 2] = two[r % 2] + val[8 * r:8 * r + 8, 128 * c:128 * c + 128]
                out += two
            return tuple(out)
        tots = lax.fori_loop(0, 20, body, (jnp.zeros((8, LANES), f32),) * (2 * count))
        return [tots[2 * n] + tots[2 * n + 1] for n in range(count)]

    def write_u():
        for ch in range(CHUNKS):
            lanes = slice(128 * ch, 128 * ch + 128)
            for i in range(8):
                dst = u.at[ch, i, place[2], place[1], place[0], core]
                dst[0:16] = cur[32 * i:32 * i + 16, lanes].astype(bf)
                dst[16:32] = cur[256 + 32 * i:256 + 32 * i + 16, lanes].astype(bf)
                dst[32:48] = cur[32 * i + 16:32 * i + 32, lanes].astype(bf)
                dst[48:64] = cur[256 + 32 * i + 16:256 + 32 * i + 32, lanes].astype(bf)
                dst[64:80] = cur[512 + 16 * i:512 + 16 * i + 16, lanes].astype(bf)

    def right_part(ch, par, pairs):
        rhs = []
        for i in pairs:
            main = u[ch, i, :, :, :, :, 32 * par:32 * par + 32, :].reshape(512, 128)
            tail = u[ch, i, :, :, :, :, 64:80, :].reshape(256, 128)
            rhs.append(jnp.concatenate([main, tail], axis=0))
        rhs = jnp.concatenate(rhs, axis=1)
        lhs = jnp.concatenate([rc[:, 0:512], rc[:, 512 + 256 * par:768 + 256 * par]], axis=1)
        val = jnp.dot(lhs, rhs, preferred_element_type=f32)
        for n, i in enumerate(pairs):
            y[2 * i + par, 0:most] = val[:, 128 * n:128 * n + 128].reshape(most, SLAB, 128).astype(bf)
            own = u.at[ch, i, place[2], place[1], place[0], core]
            y[2 * i + par, most, 0:32] = own[32 * par:32 * par + 32, :]
            y[2 * i + par, most, 32:40] = own[64 + 8 * par:72 + 8 * par, :]

    def right_phase(ch, middle):
        for par in range(2):
            if par == 1:
                middle()
            if most < TERMS:
                right_part(ch, par, range(8))
            else:
                @pl.loop(0, 4)
                def _(g):
                    right_part(ch, par, [2 * g, 2 * g + 1])

    def pair_left_phase(ch, zb, half_done):
        low_rows = (iota((256, 256), 0) & 15) < 8
        deep = 8 if most < TERMS else 4

        @pl.loop(0, DEVS // deep)
        def _(g):
            for s in range(deep):
                k = g * deep + s
                first, second = [table[TABLE_ROW[most], 2 * k + t] for t in range(2)]

                def tile(at, row):
                    return y[:, at, row:row + 16, :].reshape(256, 128)

                z01 = jnp.dot(wi[k, 0], jnp.concatenate([tile(first, 0), tile(first, 16)], axis=1), preferred_element_type=f32).astype(bf)
                mixed = jnp.where(low_rows, wi[k, 0], wi[k, 1])
                ends = jnp.concatenate([y[:, at, 32:40, :] for at in (first, second)], axis=1).reshape(256, 128)
                z2 = jnp.dot(mixed, ends, preferred_element_type=f32).reshape(16, 2, 8, 128)
                z34 = jnp.dot(wi[k, 1], jnp.concatenate([tile(second, 0), tile(second, 16)], axis=1), preferred_element_type=f32).astype(bf)
                zb[s, 0:256, 0:128] = z01[:, 0:128]
                zb[s, 256:512, 0:128] = z01[:, 128:256]
                zb[s, 512:640, 0:128] = z2[:, 0].reshape(128, 128).astype(bf)
                zb[s, 0:256, 128:256] = z34[:, 0:128]
                zb[s, 256:512, 128:256] = z34[:, 128:256]
                zb[s, 512:640, 128:256] = z2[:, 1].reshape(128, 128).astype(bf)
            lhs = jnp.concatenate([zb[s] for s in range(deep)], axis=1)
            rows = pl.ds(pl.multiple_of(ch * 128, 128), 128)
            rhs = []
            for s in range(deep):
                for t in range(2):
                    at = (g, s // 4, s // 2 % 2) if deep == 8 else (lax.div(g, 2), lax.rem(g, 2), s // 2)
                    rhs.append(lft[at + (s % 2, t, rows)])
            acc[...] += jnp.dot(lhs, jnp.concatenate(rhs, axis=0), preferred_element_type=f32)

            @pl.when(g == 8 // deep - 1)
            def _():
                half_done()

    def turn(vec, turned):
        shifted = [lax.rem(q + DEVS - me, DEVS) for q in range(PAIR)]
        for lt in range(5):
            rows = []
            for n in range(16 * lt, 16 * lt + 16):
                q, part = shifted[n // 5], n % 5
                start = 512 + 8 * q if part == 4 else 256 * (part // 2) + 16 * q + 8 * (part % 2)
                rows.append(vec[pl.ds(pl.multiple_of(start, 8), 8), :])
            turned[:, 128 * lt:128 * lt + 128] = jnp.concatenate(rows, axis=0).T

    def flipped(mask):
        dev = me
        for n, bit in enumerate((core,) + place):
            if mask >> n & 1:
                dev = dev + (1 << n) * (1 - 2 * bit)
        return dev

    def out_copy(turned, vec, mask, final, arriving=False):
        dev = flipped(mask)
        src = dev if arriving else me
        rows = pl.ds(pl.multiple_of(dev * SLAB, 8), SLAB)
        return remote(turned.at[rows], gathered.at[vec, src], out_send.at[mask], out_recv.at[final, mask], dev)

    def own_copy(turned, vec):
        rows = pl.ds(pl.multiple_of(me * SLAB, 8), SLAB)
        return pltpu.make_async_copy(turned.at[rows], gathered.at[vec, me], own_sem)

    def send_out(turned, vec, masks, final=0):
        for mask in masks:
            out_copy(turned, vec, mask, final).start()

    def finish_out(turned, vec, final=0):
        own_copy(turned, vec).wait()
        for mask in range(1, DEVS):
            out_copy(turned, vec, mask, final, True).wait_recv()
        for mask in range(1, DEVS):
            out_copy(turned, vec, mask, final).wait_send()

    def build_right():
        for n in range(most):
            for t in range(5):
                rc[SLAB * n:SLAB * n + SLAB, 128 * t:128 * t + 128] = y[t, table[1, n]]
        tails = rc[:, 512:640]
        src = iota((128, 256), 0)
        spot = 16 * (src >> 3) + (src & 7)
        for par in range(2):
            widen = (spot + 8 * par == iota((128, 256), 1)).astype(bf)
            rc[:, 512 + 256 * par:768 + 256 * par] = jnp.dot(tails, widen, preferred_element_type=f32).astype(bf)

    def mirror_left(ch):
        @pl.loop(0, 8)
        def _(g):
            for n in range(4):
                at = (g // 4, lax.rem(g // 2, 2), lax.rem(g, 2), n // 2, n % 2)
                for other in range(ch + 1, CHUNKS):
                    block = lft[at + (slice(128 * ch, 128 * ch + 128), slice(128 * other, 128 * other + 128))]
                    lft[at + (slice(128 * other, 128 * other + 128), slice(128 * ch, 128 * ch + 128))] = block.T

    left_load = pltpu.make_async_copy(left_hbm.at[:, 128:BOND], lft.at[net.slots(()) + (slice(None), slice(128, BOND))], load_sem.at[0])
    right_load = pltpu.make_async_copy(right_hbm, y.at[0:5, 0:TERMS], load_sem.at[1])
    wi_load = pltpu.make_async_copy(wi_hbm, wi, load_sem.at[2])
    slab_load = pltpu.make_async_copy(slab_hbm, cur, load_sem.at[3])
    first_load = pltpu.make_async_copy(first_left, lft.at[:, :, :, :, :, 0:128], load_sem.at[4])

    def vector_load(ch):
        return pltpu.make_async_copy(u_hbm.at[ch], u.at[ch], load_sem.at[5 + ch])

    left_load.start()
    right_load.start()
    vector_load(0).start()
    wi_load.start()
    first_load.start()
    for ch in range(1, CHUNKS):
        vector_load(ch).start()
    slab_load.start()
    entry_barrier(me)
    left_load.wait()
    net.own_out(left_view, net.at(1))
    right_load.wait()
    build_right()
    prev[...] = jnp.zeros_like(prev)

    def step(zb, turned, j, beta_prev):
        later = j > 0

        @pl.when(later)
        def _():
            zero, one = net.at(0), net.at(1)
            net.own_out(vec_view, zero)
            turn(cur, turned)
            own_copy(turned, j - 1).start()
            net.relay_first(vec_view, zero)
            net.relay_second(vec_view, zero)
            net.relay_last(vec_view, zero)
            net.own_out(vec_view, one)
            net.relay_third(vec_view, zero)
            net.take_pairs(vec_view, zero)
            net.take_last(vec_view, zero)
            net.relay_first(vec_view, one)
            net.chunk_ready(vec_view, zero)

        acc[...] = jnp.zeros_like(acc)

        @pl.loop(0, CHUNKS)
        def _(ch):
            next_spot, after_spot = net.at(ch + 1), net.at(ch + 2)

            @pl.when(later & (ch + 1 < CHUNKS))
            def _():
                net.relay_second(vec_view, next_spot)

            @pl.when(later & (ch == 4))
            def _():
                send_out(turned, j - 1, (7, 13, 11))

            @pl.when(j == 0)
            def _():
                vector_load(ch).wait()

            def middle():
                @pl.when(later & (ch + 1 < CHUNKS))
                def _():
                    net.relay_third(vec_view, next_spot)
                    net.relay_last(vec_view, next_spot)

                    @pl.when(ch + 2 < CHUNKS)
                    def _():
                        net.own_out(vec_view, after_spot)

                    @pl.when(ch == 3)
                    def _():
                        send_out(turned, j - 1, (1, 3, 5, 9, 14, 15))

                @pl.when((j == 0) & (ch > 0))
                def _():
                    def take(view, spot):
                        if spot.ch > 0:
                            mirror_left(spot.ch - 1)
                        net.take_pairs(view, spot)
                        net.take_last(view, spot)

                    for_left(ch, take)

            right_phase(ch, middle)

            @pl.when(j == 0)
            def _():
                @pl.when(ch == 0)
                def _():
                    wi_load.wait()
                    first_load.wait()

                def left_ready(view, spot):
                    if spot.ch > 0:
                        net.chunk_ready(view, spot)

                for_left(ch, left_ready)
                for_left(ch + 1, net.relay_first)

            def half_done():
                @pl.when(later & (ch + 1 < CHUNKS))
                def _():
                    net.take_pairs(vec_view, next_spot)
                    net.take_last(vec_view, next_spot)

                    @pl.when(ch + 2 < CHUNKS)
                    def _():
                        net.relay_first(vec_view, after_spot)

                    @pl.when(ch == 2)
                    def _():
                        send_out(turned, j - 1, (2, 4, 8))

                    @pl.when(ch == 3)
                    def _():
                        send_out(turned, j - 1, (6, 12, 10))

                @pl.when(j == 0)
                def _():
                    for_left(ch + 1, net.relay_second)

            pair_left_phase(ch, zb, half_done)

            @pl.when(later & (ch + 1 < CHUNKS))
            def _():
                net.chunk_ready(vec_view, next_spot)

            @pl.when(j == 0)
            def _():
                def advance(view, spot):
                    net.relay_third(view, spot)
                    net.relay_last(view, spot)

                for_left(ch + 1, advance)
                for_left(ch + 2, net.own_out)

        @pl.when(j == 0)
        def _():
            for c in range(1, CHUNKS):
                net.drain_sends(left_view, net.at(c))

        @pl.when(later)
        def _():
            @pl.loop(0, CHUNKS)
            def _(ch):
                net.drain_sends(vec_view, net.at(ch))

        @pl.when(j == 0)
        def _():
            slab_load.wait()

        @pl.when(j == 0)
        def _():
            send_partial(0, dots(lambda rows: (acc[rows, :] * cur[rows, :],), 1))
            betas[0, LANCZOS_STEPS + 1] = total_of(0, 1)[0]

        shift = betas[0, LANCZOS_STEPS + 1]

        def products(rows):
            v, v_prev = cur[rows, :], prev[rows, :]
            w = acc[rows, :] - shift * v - beta_prev * v_prev
            acc[rows, :] = w
            return w * w, w * v, v * v, v * v_prev

        send_partial(1, dots(products, 4))

        @pl.when(later)
        def _():
            finish_out(turned, j - 1)

        @pl.when(j + 1 == LANCZOS_STEPS)
        def _():
            turn(acc, turned)
            own_copy(turned, j).start()
            send_out(turned, j, (14, 15, 6, 12, 10, 7, 13, 11, 2, 4, 8, 3, 5, 9, 1), 1)

        ww, wv, vv, vp = total_of(1, 4)
        alpha = wv + shift * vv + beta_prev * vp
        extra = alpha - shift
        beta = jnp.sqrt(ww - 2.0 * extra * wv + extra * extra * vv)
        alphas[0, j] = alpha
        betas[0, j] = beta
        betas[0, LANCZOS_STEPS] = extra
        betas[0, LANCZOS_STEPS + 1] = alpha

        @pl.when(j + 1 < LANCZOS_STEPS)
        def _():
            @pl.loop(0, 20)
            def _(g):
                rows = pl.ds(pl.multiple_of(g * 32, 32), 32)
                v = cur[rows, :]
                prev[rows, :] = v
                cur[rows, :] = (acc[rows, :] - extra * v) / beta

            write_u()

        return beta

    def all_steps(zb, turned):
        lax.fori_loop(0, LANCZOS_STEPS, functools.partial(step, zb, turned), jnp.zeros((), f32))
        finish_out(turned, LANCZOS_STEPS - 1, 1)

    pl.run_scoped(all_steps, pltpu.VMEM((8, BOND, 256), bf), pltpu.VMEM((BOND, BOND), f32))


def run_lanczos(most, table, u_hbm, slab_hbm, wi_hbm, right_hbm, first_left, left_loc):
    smem = pl.BlockSpec(memory_space=pltpu.SMEM)
    hbm = pl.BlockSpec(memory_space=pltpu.HBM)
    dma = pltpu.SemaphoreType.DMA
    return pl.pallas_call(
        functools.partial(lanczos_kernel, most),
        out_shape=(jax.ShapeDtypeStruct((LANCZOS_STEPS, DEVS, SLAB, BOND), f32), jax.ShapeDtypeStruct((1, 8), f32), jax.ShapeDtypeStruct((1, 8), f32)),
        in_specs=[smem] + [hbm] * 6,
        out_specs=(hbm, smem, smem),
        scratch_shapes=[
            pltpu.VMEM(VECTOR_SHAPE, bf),
            pltpu.VMEM((2, 2, 2, 2, 2, BOND, BOND), bf),
            pltpu.VMEM((PAIR, TERMS + 1, SLAB, LANES), bf),
            pltpu.VMEM((BOND, BOND), f32),
            pltpu.VMEM((BOND, BOND), f32),
            pltpu.VMEM((BOND, BOND), f32),
            pltpu.VMEM((2, DEVS, 8, LANES), f32),
            pltpu.VMEM((most * SLAB, 1024), bf),
            pltpu.VMEM((DEVS, 2, 256, 256), bf),
            dma((5 + CHUNKS,)), dma, dma((CHUNKS, 3, 7)), dma((CHUNKS, 3, 7)), dma((CHUNKS, 8)), dma((CHUNKS, 8)),
            dma((2, DEVS)), dma((2, DEVS)), dma((DEVS,)), dma((2, DEVS)),
        ],
        compiler_params=pltpu.CompilerParams(collective_id=most, has_side_effects=True, vmem_limit_bytes=67043328),
    )(table, u_hbm, slab_hbm, wi_hbm, right_hbm, first_left, left_loc)


def place_kernel(norm, alphas, betas, psi, gathered, krylov, alpha_out, beta_out, rows, src, dst, load_sem, store_sem):
    me = lax.axis_index(AXIS_NAME)

    def load(vec):
        return pltpu.make_async_copy(gathered.at[vec], src.at[vec], load_sem.at[vec])

    def store(vec):
        return pltpu.make_async_copy(dst.at[vec], krylov.at[vec], store_sem.at[vec])

    def placed(vec, r, q):
        lane = iota((8, LANES), 1)
        tiles = []
        for t in range(5):
            tile = None
            for m in range(128 * t // SLAB, min(DEVS, (128 * t + 127) // SLAB + 1)):
                val = src[vec, (m - q) % DEVS, pl.ds(r, 8), 128 * t:128 * t + 128]
                tile = val if tile is None else jnp.where(lane >= SLAB * m - 128 * t, val, tile)
            tiles.append(tile)
        skip, rest = SLAB * q // 128, SLAB * q % 128
        if rest:
            tiles = [pltpu.roll(tile, 128 - rest, 1) for tile in tiles]
        tiles = [tiles[(t + skip) % 5] if not rest else jnp.where(lane < 128 - rest, tiles[(t + skip) % 5], tiles[(t + skip + 1) % 5]) for t in range(5)]
        return jnp.concatenate(tiles, axis=1)

    rows_load = pltpu.make_async_copy(psi.at[pl.ds(me * SLAB, SLAB)], rows, load_sem.at[LANCZOS_STEPS])
    rows_load.start()
    for vec in range(LANCZOS_STEPS):
        load(vec).start()
    for n in range(LANCZOS_STEPS):
        alpha_out[n] = alphas[0, n]
        beta_out[n] = betas[0, n]
    rows_load.wait()
    dst[0] = rows[...] / norm[0, 0]
    store(0).start()

    @pl.loop(0, LANCZOS_STEPS - 1)
    def _(vec):
        load(vec).wait()
        for r in range(0, SLAB, 8):
            for q in range(PAIR):
                dst[vec + 1, r:r + 8, q, :] = placed(vec, r, q)
        store(vec + 1).start()

    load(LANCZOS_STEPS - 1).wait()
    for r in range(0, SLAB, 8):
        for q in range(PAIR):
            before = dst[LANCZOS_STEPS - 1, r:r + 8, q, :]
            dst[LANCZOS_STEPS, r:r + 8, q, :] = (placed(LANCZOS_STEPS - 1, r, q) - betas[0, LANCZOS_STEPS] * before) / betas[0, LANCZOS_STEPS - 1]
    store(LANCZOS_STEPS).start()
    for vec in range(LANCZOS_STEPS + 1):
        store(vec).wait()


def place_outputs(norm, alphas, betas, wavefunction, gathered):
    smem = pl.BlockSpec(memory_space=pltpu.SMEM)
    hbm = pl.BlockSpec(memory_space=pltpu.HBM)
    dma = pltpu.SemaphoreType.DMA
    return pl.pallas_call(
        place_kernel,
        out_shape=(jax.ShapeDtypeStruct((LANCZOS_STEPS + 1, SLAB, PAIR, BOND), f32), jax.ShapeDtypeStruct((LANCZOS_STEPS,), f32), jax.ShapeDtypeStruct((LANCZOS_STEPS,), f32)),
        in_specs=[smem, smem, smem, hbm, hbm],
        out_specs=(hbm, smem, smem),
        scratch_shapes=[
            pltpu.VMEM((SLAB, PAIR, BOND), f32),
            pltpu.VMEM((LANCZOS_STEPS, DEVS, SLAB, BOND), f32),
            pltpu.VMEM((LANCZOS_STEPS + 1, SLAB, PAIR, BOND), f32),
            dma((LANCZOS_STEPS + 1,)), dma((LANCZOS_STEPS + 1,)),
        ],
        compiler_params=pltpu.CompilerParams(vmem_limit_bytes=40 * 1024 * 1024),
    )(norm, alphas, betas, wavefunction, gathered)


def solution(mesh):
    def device_body(wavefunction, left_loc, pair_loc, right_loc, flag_loc):
        table, few, norm, *operands = prepare(flag_loc, wavefunction, pair_loc, right_loc, left_loc)
        k16, k20, k32 = [functools.partial(run_lanczos, most) for most in (FEWER, FEW, TERMS)]
        vecs, alphas, betas = lax.switch(few[0], [k20, k32], table, *operands, left_loc)
        return place_outputs(norm, alphas, betas, wavefunction, vecs)

    return jax.shard_map(device_body, mesh=mesh, in_specs=(P(), P(AXIS_NAME), P(AXIS_NAME), P(AXIS_NAME), P(AXIS_NAME)), out_specs=(P(None, AXIS_NAME), P(), P()), check_vma=False)
```

```python
import functools
import jax
import jax.numpy as jnp
from jax import lax
from jax.experimental import pallas as pl
from jax.sharding import PartitionSpec as P
from jax.experimental.pallas import tpu as pltpu

LANCZOS_STEPS = 6
AXIS_NAME = 'terms'
BOND = 640
PAIR = 16
TERMS = 32
DEVS = 16
SLAB = BOND // DEVS
CHUNKS = 5
FEWER, FEW = 16, 20
TABLE_ROW = {16: 0, 20: 2, 32: 3}
LANES = 128
VEC_SIZE = BOND * PAIR * BOND
bf = jnp.bfloat16
f32 = jnp.float32
MESH = pl.DeviceIdType.MESH
PART_PAIRS = ((0, 3), (3, 6), (6, 8))
LEFT_ROWS = ((0, 48), (48, 96), (96, 128))
AXES = ((1, 0, 0), (0, 1, 0), (0, 0, 1))
D2D_FLIPS = ((0,), (1,), (2,), (0, 1), (0, 2), (1, 2), (0, 1, 2), ())


def entry_barrier(me):
    barrier = pltpu.get_barrier_semaphore()
    for off in range(1, DEVS):
        pl.semaphore_signal(barrier, inc=1, device_id=(lax.rem(me + off, DEVS),), device_id_type=MESH)
    pl.semaphore_wait(barrier, DEVS - 1)


def iota(shape, dim):
    return lax.broadcasted_iota(jnp.int32, shape, dim)


def remote(ref, dst_ref, send, recv, dev):
    return pltpu.make_async_remote_copy(src_ref=ref, dst_ref=dst_ref, send_sem=send, recv_sem=recv, device_id=(dev,), device_id_type=MESH)


class Spot:
    def __init__(self, net, ch):
        self.ch = ch
        self.hits, self.across = [], []
        for n in range(3):
            axis = (n + ch) % 3 if isinstance(ch, int) else lax.rem(n + ch, 3)
            one = axis * (2 - axis)
            two = axis * (axis - 1) // 2 if isinstance(ch, int) else lax.div(axis * (axis - 1), 2)
            hit = (1 - one - two, one, two)
            self.hits.append(hit)
            self.across.append(net.me + hit[0] * net.step[0] + hit[1] * net.step[1] + hit[2] * net.step[2])


class Gather:
    def __init__(self, me, ici_send, ici_recv, d2d_send, d2d_recv):
        self.me, self.sems = me, (ici_send, ici_recv, d2d_send, d2d_recv)
        self.core = lax.rem(me, 2)
        self.place = (lax.rem(lax.div(me, 2), 2), lax.rem(lax.div(me, 4), 2), lax.div(me, 8))
        self.turn = tuple(1 - 2 * at for at in self.place)
        self.step = tuple((2 << n) * turn for n, turn in enumerate(self.turn))
        self.partner = me + 1 - 2 * self.core

    def at(self, ch):
        return Spot(self, ch)

    def slots(self, hits):
        idx = []
        for n in (2, 1, 0):
            moved = self.place[n]
            for hit in hits:
                if not isinstance(hit[n], int) or hit[n]:
                    moved = moved + hit[n] * self.turn[n]
            idx.append(moved)
        return tuple(idx) + (self.core,)

    def unit(self, view, spot, part, n, arriving=False):
        flips, axis = (((), 0), ((), 1), ((), 2), ((0,), 1), ((0,), 2), ((1,), 2), ((0, 1), 2))[n]
        hits = [spot.hits[(part + m) % 3] for m in (flips + (axis,) if arriving else flips)]
        ref = view(spot.ch, part, hits)
        return remote(ref, ref, self.sems[0].at[spot.ch, part, n], self.sems[1].at[spot.ch, part, n], spot.across[(part + axis) % 3])

    def start_units(self, view, spot, *which):
        for n in which:
            for part in range(3):
                self.unit(view, spot, part, n).start()

    def wait_units(self, view, spot, *which):
        for n in which:
            for part in range(3):
                self.unit(view, spot, part, n, True).wait_recv()

    def d2d(self, view, spot, n):
        ref = view(spot.ch, 3, [AXES[m] for m in D2D_FLIPS[n]])
        return remote(ref, ref, self.sems[2].at[spot.ch, n], self.sems[3].at[spot.ch, n], self.partner)

    def own_out(self, view, spot):
        self.start_units(view, spot, 0, 1, 2)
        self.d2d(view, spot, 7).start()

    def relay_first(self, view, spot):
        for part in range(3):
            self.unit(view, spot, part, 0, True).wait_recv()
            self.unit(view, spot, part, 3).start()
        self.start_units(view, spot, 4)

    def relay_second(self, view, spot):
        for part in range(3):
            self.unit(view, spot, part, 1, True).wait_recv()
            self.unit(view, spot, part, 5).start()

    def relay_third(self, view, spot):
        self.wait_units(view, spot, 2)
        for n in (0, 1, 2):
            self.d2d(view, spot, n).start()

    def relay_last(self, view, spot):
        for part in range(3):
            self.unit(view, spot, part, 3, True).wait_recv()
            self.unit(view, spot, part, 6).start()

    def take_pairs(self, view, spot):
        self.wait_units(view, spot, 4, 5)
        for n in (3, 4, 5):
            self.d2d(view, spot, n).start()

    def take_last(self, view, spot):
        self.wait_units(view, spot, 6)
        self.d2d(view, spot, 6).start()

    def wait_d2d(self, view, spot, *which):
        for n in which:
            self.d2d(view, spot, n).wait_recv()

    def chunk_ready(self, view, spot):
        self.wait_d2d(view, spot, *range(8))

    def drain_sends(self, view, spot):
        for n in range(8):
            self.d2d(view, spot, n).wait_send()
        for n in range(7):
            for part in range(3):
                self.unit(view, spot, part, n).wait_send()


def prep_kernel(flags, psi, psi_rows, pair_loc, right_hbm, left_hbm, table, few, norm_out, u_hbm, slab_hbm, wi_hbm, right_out, left_out,
                u, y, moved, cur, seen, ops, wi, left, load_sem, stage_sem, out_sem, seen_send, seen_recv, op_send, op_recv, ici_send, ici_recv, d2d_send, d2d_recv, left_sem, small_i, small_f):
    me = lax.axis_index(AXIS_NAME)
    net = Gather(me, ici_send, ici_recv, d2d_send, d2d_recv)

    def left_view(ch, part, flips):
        lo, hi = LEFT_ROWS[part] if part < 3 else (0, 128)
        return left.at[net.slots(flips) + (slice(None), slice(lo, hi))]

    def dots(fn, count):
        def body(g, tots):
            vals = fn(pl.ds(pl.multiple_of(g * 32, 32), 32))
            out = []
            for n, val in enumerate(vals):
                two = [tots[2 * n], tots[2 * n + 1]]
                for r in range(4):
                    for c in range(5):
                        two[r % 2] = two[r % 2] + val[8 * r:8 * r + 8, 128 * c:128 * c + 128]
                out += two
            return tuple(out)
        tots = lax.fori_loop(0, 20, body, (jnp.zeros((8, LANES), f32),) * (2 * count))
        return [tots[2 * n] + tots[2 * n + 1] for n in range(count)]

    def spread_right():
        col = iota((BOND, 128), 0)
        source = (col * 1639) >> 16
        within = col - source * SLAB
        target = jnp.where(within < 32, source * 32 + within, 480 + source * 8 + within)
        for t in range(5):
            perm = (target == iota((BOND, 128), 1) + 128 * t).astype(f32).astype(bf)
            for k in range(2):
                rows = jnp.concatenate([y[n, BOND * k:BOND * k + BOND, :] for n in range(5)], axis=1)
                val = jnp.dot(rows, perm, preferred_element_type=f32).reshape(DEVS, SLAB, 128)
                if k == 0:
                    first = val
            moved[t] = jnp.concatenate([first[:, None], val[:, None]], axis=1).reshape(TERMS, SLAB, 128).astype(bf)

    def build_pairs():
        widen = ((iota((128, 256), 1) >> 4) == iota((128, 256), 0)).astype(bf)
        same = (iota((256, 256), 0) & 15) == (iota((256, 256), 1) & 15)

        @pl.loop(0, DEVS)
        def _(k):
            wide = []
            for t in range(2):
                tall = jnp.broadcast_to(ops[k, t].astype(f32)[:, None, :], (16, 16, 128)).reshape(256, 128).astype(bf)
                wide.append(jnp.where(same, jnp.dot(tall, widen, preferred_element_type=f32), 0.0))
            wi[k, 0] = wide[0].astype(bf)
            wi[k, 1] = wide[1].astype(bf)

    def tile_load(stage, t, ch, half):
        rows, qs = pl.ds(pl.multiple_of(128 * ch, 128), 128), pl.ds(pl.multiple_of(8 * half, 8), 8)
        return pltpu.make_async_copy(psi.at[rows, qs, 128 * t:128 * t + 128], stage.at[t], stage_sem.at[t])

    def vector_out(ch):
        return pltpu.make_async_copy(u.at[ch], u_hbm.at[ch], out_sem.at[ch])

    def start_vector(norm, stage, flip):
        base = (me * SLAB) // 128
        skip = pl.multiple_of(me * SLAB - base * 128, 8)
        for t in range(5):
            tile_load(stage, t, 0, 0).start()

        @pl.loop(0, 2 * CHUNKS)
        def _(it):
            ch, half = it // 2, lax.rem(it, 2)
            @pl.when(it == 3)
            def _():
                net.relay_first(left_view, net.at(0))

            @pl.when(it == 4)
            def _():
                net.relay_second(left_view, net.at(0))
                send_right(5, 10)

            @pl.when(it == 6)
            def _():
                net.relay_third(left_view, net.at(0))
                for n in (7, 0, 1, 2):
                    left_store(n).start()

            @pl.when(it == 8)
            def _():
                net.relay_last(left_view, net.at(0))
                send_right(10, 15)

            for t in range(5):
                tile_load(stage, t, ch, half).wait()

                @pl.when((base == t) | (base + 1 == t))
                def _():
                    rows = pl.ds(pl.multiple_of(128 * (t - base), 128), 128)
                    for q in range(8):
                        flip[q, rows, :] = stage[t, :, q, :].T

                for q in range(8):
                    val = (stage[t, :, q, :].T / norm).astype(bf)
                    for m in range(16):
                        src, piece = (16 * t + m) // 5, (16 * t + m) % 5
                        row = 64 + 8 * (q % 2) if piece == 4 else 32 * (q % 2) + 8 * piece
                        u[ch, 4 * half + q // 2, src // 8, src // 4 % 2, src // 2 % 2, src % 2, row:row + 8, :] = val[8 * m:8 * m + 8, :]

                @pl.when(it + 1 < 2 * CHUNKS)
                def _():
                    tile_load(stage, t, (it + 1) // 2, lax.rem(it + 1, 2)).start()

            lanes = pl.ds(pl.multiple_of(128 * ch, 128), 128)
            for q in range(8):
                val = flip[q, pl.ds(skip, SLAB), :] / norm
                row = 128 * half + 16 * q
                for start, piece, size in ((row, 0, 16), (256 + row, 16, 16), (512 + 64 * half + 8 * q, 32, 8)):
                    cur[pl.ds(pl.multiple_of(start, 8), size), lanes] = val[piece:piece + size, :]

            @pl.when(half == 1)
            def _():
                vector_out(ch).start()

    def left_store(n, other=False):
        at = net.slots([AXES[m] for m in D2D_FLIPS[n]])
        at = at[:3] + ((1 - net.core,) if other else at[3:])
        return pltpu.make_async_copy(left.at[at], left_out.at[at], left_sem.at[int(other), n])

    def seen_copy(off, dev, src):
        return remote(seen.at[src], seen.at[src], seen_send.at[off], seen_recv.at[src], dev)

    def pair_copy(off, dev, src):
        return remote(ops.at[src], ops.at[src], op_send.at[0, off], op_recv.at[0, src], dev)

    def right_copy(off, dev, src):
        return remote(moved.at[:, pl.ds(2 * dev, 2)], right_out.at[:, pl.ds(2 * src, 2)], op_send.at[1, off], op_recv.at[1, src], dev)

    def others():
        return [(off, lax.rem(me + off, DEVS)) for off in range(1, DEVS)]

    def send_right(first, last):
        for n in range(first, last):
            off = 3 * (n % 5) + n // 5 + 1
            right_copy(off, lax.rem(me + off, DEVS), me).start()

    slab_load = pltpu.make_async_copy(psi_rows.at[pl.ds(pl.multiple_of(me * BOND, 8), BOND)], cur, load_sem.at[0])
    left_load = pltpu.make_async_copy(left_hbm.at[:, 0:128], left.at[net.slots(())], load_sem.at[1])
    right_load = [pltpu.make_async_copy(right_hbm.at[:, 128 * n:128 * n + 128], y.at[n], load_sem.at[2 + n]) for n in range(5)]
    slab_load.start()
    left_load.start()
    for load in right_load:
        load.start()
    for t in range(2):
        ops[me, t] = jnp.concatenate([pair_loc[t].astype(f32), jnp.zeros((PAIR, LANES - PAIR), f32)], axis=1).astype(bf)
    entry_barrier(me)
    slab_load.wait()
    square, = dots(lambda rows: (cur[rows, :] * cur[rows, :],), 1)
    row = iota((8, LANES), 0)
    full = jnp.where(row == 1, flags[0], flags[1]).astype(f32)
    seen[me] = jnp.where(row == 0, jnp.sum(square, axis=0, keepdims=True), full)
    for off, dev in others():
        seen_copy(off, dev, me).start()
    for off, dev in others():
        pair_copy(off, dev, me).start()
    left_load.wait()
    net.own_out(left_view, net.at(0))
    for load in right_load:
        load.wait()
    spread_right()
    send_right(0, 5)
    own = pl.ds(2 * me, 2)
    right_own = pltpu.make_async_copy(moved.at[:, own], right_out.at[:, own], load_sem.at[0])
    right_own.start()
    for off, dev in others():
        seen_copy(off, dev, dev).wait_recv()
    norm = jnp.sqrt(jnp.sum(jnp.sum(seen[:, 0:1, :], axis=0)) / VEC_SIZE)
    small_f[...] = jnp.zeros((8, LANES), f32) + norm
    norm_store = pltpu.make_async_copy(small_f, norm_out, load_sem.at[6])
    norm_store.start()
    term, lane = iota((TERMS, LANES), 0), iota((TERMS, LANES), 1)
    full = jnp.concatenate([seen[src, 1:3, :] for src in range(DEVS)], axis=0)
    in_lanes = jnp.sum(jnp.where(term == lane, full, 0.0), axis=0, keepdims=True)
    rank = jnp.sum(jnp.where(term < lane, full, 0.0), axis=0, keepdims=True)
    rank_down = jnp.sum(jnp.where(lane < term, in_lanes, 0.0), axis=1, keepdims=True)
    holder = jnp.sum(jnp.where(rank_down == lane.astype(f32), full * term.astype(f32), 0.0), axis=0, keepdims=True)
    small_i[...] = jnp.where(row == 1, holder, jnp.where(in_lanes > 0.5, rank, jnp.where(row == 0, FEWER, jnp.where(row == 2, FEW, TERMS)).astype(f32))).astype(jnp.int32)
    count = jnp.sum(in_lanes)
    few[0] = jnp.where(count < FEWER + 0.5, 2, jnp.where(count < FEW + 0.5, 1, 0))
    table_store = pltpu.make_async_copy(small_i, table, load_sem.at[7])
    table_store.start()
    pl.run_scoped(functools.partial(start_vector, norm), pltpu.VMEM((5, 128, 8, LANES), f32), pltpu.VMEM((8, 256, LANES), f32))
    slab_out = pltpu.make_async_copy(cur, slab_hbm, load_sem.at[1])
    slab_out.start()
    for off, dev in others():
        pair_copy(off, dev, dev).wait_recv()
    build_pairs()
    wi_out = pltpu.make_async_copy(wi, wi_hbm, load_sem.at[2])
    wi_out.start()
    net.take_pairs(left_view, net.at(0))
    for n in (3, 4, 5):
        left_store(n).start()
    net.wait_d2d(left_view, net.at(0), 7, 0, 1, 2)
    for n in (7, 0, 1, 2):
        left_store(n, True).start()
    net.take_last(left_view, net.at(0))
    left_store(6).start()
    net.wait_d2d(left_view, net.at(0), 3, 4, 5, 6)
    for n in (3, 4, 5, 6):
        left_store(n, True).start()
    net.drain_sends(left_view, net.at(0))
    for off, dev in others():
        right_copy(off, dev, dev).wait_recv()
    for off, dev in others():
        seen_copy(off, dev, me).wait_send()
        pair_copy(off, dev, me).wait_send()
        right_copy(off, dev, me).wait_send()
    right_own.wait()
    slab_out.wait()
    wi_out.wait()
    norm_store.wait()
    table_store.wait()
    for n in range(8):
        left_store(n).wait()
        left_store(n, True).wait()
    for ch in range(CHUNKS):
        vector_out(ch).wait()


VECTOR_SHAPE = (CHUNKS, 8, 2, 2, 2, 2, 80, LANES)


def prepare(flags, psi, pair_loc, right_loc, left_loc):
    smem = pl.BlockSpec(memory_space=pltpu.SMEM)
    vmem = pl.BlockSpec(memory_space=pltpu.VMEM)
    hbm = pl.BlockSpec(memory_space=pltpu.HBM)
    dma = pltpu.SemaphoreType.DMA
    return pl.pallas_call(
        prep_kernel,
        out_shape=(
            jax.ShapeDtypeStruct((8, LANES), jnp.int32), jax.ShapeDtypeStruct((1,), jnp.int32), jax.ShapeDtypeStruct((8, LANES), f32),
            jax.ShapeDtypeStruct(VECTOR_SHAPE, bf), jax.ShapeDtypeStruct((BOND, BOND), f32),
            jax.ShapeDtypeStruct((DEVS, 2, 256, 256), bf), jax.ShapeDtypeStruct((5, TERMS, SLAB, LANES), bf), jax.ShapeDtypeStruct((2, 2, 2, 2, 2, 128, BOND), bf),
        ),
        in_specs=[smem, hbm, hbm, vmem, hbm, hbm],
        out_specs=(hbm, smem, hbm, hbm, hbm, hbm, hbm, hbm),
        scratch_shapes=[
            pltpu.VMEM(VECTOR_SHAPE, bf),
            pltpu.VMEM((5, 2 * BOND, LANES), bf),
            pltpu.VMEM((5, TERMS, SLAB, LANES), bf),
            pltpu.VMEM((BOND, BOND), f32),
            pltpu.VMEM((DEVS, 8, LANES), f32),
            pltpu.VMEM((DEVS, 2, PAIR, LANES), bf),
            pltpu.VMEM((DEVS, 2, 256, 256), bf),
            pltpu.VMEM((2, 2, 2, 2, 2, 128, BOND), bf),
            dma((8,)), dma((5,)), dma((CHUNKS,)), dma((DEVS,)), dma((DEVS,)), dma((2, DEVS)), dma((2, DEVS)),
            dma((1, 3, 7)), dma((1, 3, 7)), dma((1, 8)), dma((1, 8)), dma((2, 8)),
            pltpu.VMEM((8, LANES), jnp.int32), pltpu.VMEM((8, LANES), f32),
        ],
        compiler_params=pltpu.CompilerParams(collective_id=0, has_side_effects=True, vmem_limit_bytes=67043328),
    )(flags, psi, psi.reshape(BOND * PAIR, BOND), pair_loc, right_loc.reshape(2 * BOND, BOND), left_loc)


def lanczos_kernel(most, table, u_hbm, slab_hbm, wi_hbm, right_hbm, first_left, left_hbm, gathered, alphas, betas,
                   u, lft, y, acc, cur, prev, ar, rc, wi,
                   load_sem, own_sem, ici_send, ici_recv, d2d_send, d2d_recv, ar_send, ar_recv, out_send, out_recv):
    me = lax.axis_index(AXIS_NAME)
    net = Gather(me, ici_send, ici_recv, d2d_send, d2d_recv)
    core, place = net.core, net.place

    def vec_view(ch, part, flips):
        pairs = PART_PAIRS[part] if part < 3 else (0, 8)
        return u.at[(ch, slice(pairs[0], pairs[1])) + net.slots(flips)]

    def left_view(ch, part, flips):
        lo, hi = LEFT_ROWS[part] if part < 3 else (0, 128)
        return lft.at[net.slots(flips) + (slice(None), slice(128 * ch + lo, 128 * ch + hi), slice(128 * ch, BOND))]

    def for_left(ch, what):
        for c in range(CHUNKS):
            @pl.when(ch == c)
            def _():
                what(left_view, net.at(c))

    def send_partial(which, partials):
        row = iota((8, LANES), 0)
        tile = jnp.zeros((8, LANES), f32)
        for n, partial in enumerate(partials):
            tile = jnp.where(row == n, jnp.sum(partial, axis=0, keepdims=True), tile)
        ar[which, me] = tile
        for off in range(1, DEVS):
            dev = lax.rem(me + off, DEVS)
            ref = ar.at[which, me]
            remote(ref, ref, ar_send.at[which, off], ar_recv.at[which, me], dev).start()

    def total_of(which, count):
        for off in range(1, DEVS):
            dev = lax.rem(me + off, DEVS)
            ref = ar.at[which, dev]
            remote(ref, ref, ar_send.at[which, off], ar_recv.at[which, dev], dev).wait_recv()
        total = jnp.sum(ar[which], axis=0)
        sums = [jnp.sum(total[n:n + 1]) / VEC_SIZE for n in range(count)]
        for off in range(1, DEVS):
            dev = lax.rem(me + off, DEVS)
            ref = ar.at[which, me]
            remote(ref, ref, ar_send.at[which, off], ar_recv.at[which, me], dev).wait_send()
        return sums

    def dots(fn, count):
        def body(g, tots):
            vals = fn(pl.ds(pl.multiple_of(g * 32, 32), 32))
            out = []
            for n, val in enumerate(vals):
                two = [tots[2 * n], tots[2 * n + 1]]
                for r in range(4):
                    for c in range(5):
                        two[r % 2] = two[r % 2] + val[8 * r:8 * r + 8, 128 * c:128 * c + 128]
                out += two
            return tuple(out)
        tots = lax.fori_loop(0, 20, body, (jnp.zeros((8, LANES), f32),) * (2 * count))
        return [tots[2 * n] + tots[2 * n + 1] for n in range(count)]

    def next_vector(ch, extra, beta):
        lanes = pl.ds(pl.multiple_of(128 * ch, 128), 128)
        for i in range(8):
            dst = u.at[ch, i, place[2], place[1], place[0], core]
            for n, start in enumerate((32 * i, 256 + 32 * i, 32 * i + 16, 256 + 32 * i + 16, 512 + 16 * i)):
                v = cur[start:start + 16, lanes]
                new = (acc[start:start + 16, lanes] - extra * v) / beta
                prev[start:start + 16, lanes] = v
                cur[start:start + 16, lanes] = new
                dst[16 * n:16 * n + 16] = new.astype(bf)

    def right_part(ch, par, pairs):
        rhs = []
        for i in pairs:
            main = u[ch, i, :, :, :, :, 32 * par:32 * par + 32, :].reshape(512, 128)
            tail = u[ch, i, :, :, :, :, 64:80, :].reshape(256, 128)
            rhs.append(jnp.concatenate([main, tail], axis=0))
        rhs = jnp.concatenate(rhs, axis=1)
        lhs = jnp.concatenate([rc[:, 0:512], rc[:, 512 + 256 * par:768 + 256 * par]], axis=1)
        val = jnp.dot(lhs, rhs, preferred_element_type=f32)
        for n, i in enumerate(pairs):
            y[2 * i + par, 0:most] = val[:, 128 * n:128 * n + 128].reshape(most, SLAB, 128).astype(bf)
            own = u.at[ch, i, place[2], place[1], place[0], core]
            y[2 * i + par, most, 0:32] = own[32 * par:32 * par + 32, :]
            y[2 * i + par, most, 32:40] = own[64 + 8 * par:72 + 8 * par, :]

    def right_phase(ch, middle):
        for par in range(2):
            if par == 1:
                middle()
            if most < TERMS:
                right_part(ch, par, range(8))
            else:
                @pl.loop(0, 4)
                def _(g):
                    right_part(ch, par, [2 * g, 2 * g + 1])

    def pair_left_phase(ch, zb, half_done):
        low_rows = (iota((256, 256), 0) & 15) < 8
        deep = 8 if most < TERMS else 4

        @pl.loop(0, DEVS // deep)
        def _(g):
            for s in range(deep):
                k = g * deep + s
                first, second = [table[TABLE_ROW[most], 2 * k + t] for t in range(2)]

                def tile(at, row):
                    return y[:, at, row:row + 16, :].reshape(256, 128)

                z01 = jnp.dot(wi[k, 0], jnp.concatenate([tile(first, 0), tile(first, 16)], axis=1), preferred_element_type=f32).astype(bf)
                mixed = jnp.where(low_rows, wi[k, 0], wi[k, 1])
                ends = jnp.concatenate([y[:, at, 32:40, :] for at in (first, second)], axis=1).reshape(256, 128)
                z2 = jnp.dot(mixed, ends, preferred_element_type=f32).reshape(16, 2, 8, 128)
                z34 = jnp.dot(wi[k, 1], jnp.concatenate([tile(second, 0), tile(second, 16)], axis=1), preferred_element_type=f32).astype(bf)
                zb[s, 0:256, 0:128] = z01[:, 0:128]
                zb[s, 256:512, 0:128] = z01[:, 128:256]
                zb[s, 512:640, 0:128] = z2[:, 0].reshape(128, 128).astype(bf)
                zb[s, 0:256, 128:256] = z34[:, 0:128]
                zb[s, 256:512, 128:256] = z34[:, 128:256]
                zb[s, 512:640, 128:256] = z2[:, 1].reshape(128, 128).astype(bf)
            lhs = jnp.concatenate([zb[s] for s in range(deep)], axis=1)
            rows = pl.ds(pl.multiple_of(ch * 128, 128), 128)
            rhs = []
            for s in range(deep):
                for t in range(2):
                    at = (g, s // 4, s // 2 % 2) if deep == 8 else (lax.div(g, 2), lax.rem(g, 2), s // 2)
                    rhs.append(lft[at + (s % 2, t, rows)])
            acc[...] += jnp.dot(lhs, jnp.concatenate(rhs, axis=0), preferred_element_type=f32)

            @pl.when(g == 8 // deep - 1)
            def _():
                half_done()

    def turn(vec, turned):
        shifted = [lax.rem(q + DEVS - me, DEVS) for q in range(PAIR)]
        for lt in range(5):
            rows = []
            for n in range(16 * lt, 16 * lt + 16):
                q, part = shifted[n // 5], n % 5
                start = 512 + 8 * q if part == 4 else 256 * (part // 2) + 16 * q + 8 * (part % 2)
                rows.append(vec[pl.ds(pl.multiple_of(start, 8), 8), :])
            turned[:, 128 * lt:128 * lt + 128] = jnp.concatenate(rows, axis=0).T

    def flipped(mask):
        dev = me
        for n, bit in enumerate((core,) + place):
            if mask >> n & 1:
                dev = dev + (1 << n) * (1 - 2 * bit)
        return dev

    def out_copy(turned, vec, mask, final, arriving=False):
        dev = flipped(mask)
        src = dev if arriving else me
        rows = pl.ds(pl.multiple_of(dev * SLAB, 8), SLAB)
        return remote(turned.at[rows], gathered.at[vec, src], out_send.at[mask], out_recv.at[final, mask], dev)

    def own_copy(turned, vec):
        rows = pl.ds(pl.multiple_of(me * SLAB, 8), SLAB)
        return pltpu.make_async_copy(turned.at[rows], gathered.at[vec, me], own_sem)

    def send_out(turned, vec, masks, final=0):
        for mask in masks:
            out_copy(turned, vec, mask, final).start()

    def finish_out(turned, vec, final=0):
        own_copy(turned, vec).wait()
        for mask in range(1, DEVS):
            out_copy(turned, vec, mask, final, True).wait_recv()
        for mask in range(1, DEVS):
            out_copy(turned, vec, mask, final).wait_send()

    def build_right():
        for n in range(most):
            for t in range(5):
                rc[SLAB * n:SLAB * n + SLAB, 128 * t:128 * t + 128] = y[t, table[1, n]]
        tails = rc[:, 512:640]
        src = iota((128, 256), 0)
        spot = 16 * (src >> 3) + (src & 7)
        for par in range(2):
            widen = (spot + 8 * par == iota((128, 256), 1)).astype(bf)
            rc[:, 512 + 256 * par:768 + 256 * par] = jnp.dot(tails, widen, preferred_element_type=f32).astype(bf)

    def mirror_left(ch):
        @pl.loop(0, 8)
        def _(g):
            for n in range(4):
                at = (g // 4, lax.rem(g // 2, 2), lax.rem(g, 2), n // 2, n % 2)
                for other in range(ch + 1, CHUNKS):
                    block = lft[at + (slice(128 * ch, 128 * ch + 128), slice(128 * other, 128 * other + 128))]
                    lft[at + (slice(128 * other, 128 * other + 128), slice(128 * ch, 128 * ch + 128))] = block.T

    left_load = pltpu.make_async_copy(left_hbm.at[:, 128:BOND], lft.at[net.slots(()) + (slice(None), slice(128, BOND))], load_sem.at[0])
    right_load = pltpu.make_async_copy(right_hbm, y.at[0:5, 0:TERMS], load_sem.at[1])
    wi_load = pltpu.make_async_copy(wi_hbm, wi, load_sem.at[2])
    slab_load = pltpu.make_async_copy(slab_hbm, cur, load_sem.at[3])
    first_load = pltpu.make_async_copy(first_left, lft.at[:, :, :, :, :, 0:128], load_sem.at[4])

    def vector_load(ch):
        return pltpu.make_async_copy(u_hbm.at[ch], u.at[ch], load_sem.at[5 + ch])

    left_load.start()
    right_load.start()
    vector_load(0).start()
    wi_load.start()
    first_load.start()
    for ch in range(1, CHUNKS):
        vector_load(ch).start()
    slab_load.start()
    entry_barrier(me)
    left_load.wait()
    net.own_out(left_view, net.at(1))
    right_load.wait()
    build_right()
    prev[...] = jnp.zeros_like(prev)

    def step(zb, turned, j, beta_prev):
        later = j > 0

        @pl.when(later)
        def _():
            zero, one = net.at(0), net.at(1)
            turn(cur, turned)
            own_copy(turned, j - 1).start()
            net.relay_first(vec_view, zero)
            net.relay_second(vec_view, zero)
            net.relay_last(vec_view, zero)
            net.own_out(vec_view, one)
            net.relay_third(vec_view, zero)
            net.take_pairs(vec_view, zero)
            net.take_last(vec_view, zero)
            net.relay_first(vec_view, one)
            net.chunk_ready(vec_view, zero)

        acc[...] = jnp.zeros_like(acc)

        @pl.loop(0, CHUNKS)
        def _(ch):
            next_spot, after_spot = net.at(ch + 1), net.at(ch + 2)

            @pl.when(later & (ch + 1 < CHUNKS))
            def _():
                net.relay_second(vec_view, next_spot)

            @pl.when(later & (ch == 4))
            def _():
                send_out(turned, j - 1, (7, 13, 11))

            @pl.when(j == 0)
            def _():
                vector_load(ch).wait()

            def middle():
                @pl.when(later & (ch + 1 < CHUNKS))
                def _():
                    net.relay_third(vec_view, next_spot)
                    net.relay_last(vec_view, next_spot)

                    @pl.when(ch + 2 < CHUNKS)
                    def _():
                        net.own_out(vec_view, after_spot)

                    @pl.when(ch == 3)
                    def _():
                        send_out(turned, j - 1, (1, 3, 5, 9, 14, 15))

                @pl.when((j == 0) & (ch > 0))
                def _():
                    def take(view, spot):
                        if spot.ch > 0:
                            mirror_left(spot.ch - 1)
                        net.take_pairs(view, spot)
                        net.take_last(view, spot)

                    for_left(ch, take)

            right_phase(ch, middle)

            @pl.when(j == 0)
            def _():
                @pl.when(ch == 0)
                def _():
                    wi_load.wait()
                    first_load.wait()

                def left_ready(view, spot):
                    if spot.ch > 0:
                        net.chunk_ready(view, spot)

                for_left(ch, left_ready)
                for_left(ch + 1, net.relay_first)

            def half_done():
                @pl.when(later & (ch + 1 < CHUNKS))
                def _():
                    net.take_pairs(vec_view, next_spot)
                    net.take_last(vec_view, next_spot)

                    @pl.when(ch + 2 < CHUNKS)
                    def _():
                        net.relay_first(vec_view, after_spot)

                    @pl.when(ch == 2)
                    def _():
                        send_out(turned, j - 1, (2, 4, 8))

                    @pl.when(ch == 3)
                    def _():
                        send_out(turned, j - 1, (6, 12, 10))

                @pl.when(j == 0)
                def _():
                    for_left(ch + 1, net.relay_second)

            pair_left_phase(ch, zb, half_done)

            @pl.when(later & (ch + 1 < CHUNKS))
            def _():
                net.chunk_ready(vec_view, next_spot)

            @pl.when(j == 0)
            def _():
                def advance(view, spot):
                    net.relay_third(view, spot)
                    net.relay_last(view, spot)

                for_left(ch + 1, advance)
                for_left(ch + 2, net.own_out)

                @pl.when(ch == CHUNKS - 2)
                def _():
                    slab_load.wait()
                    send_partial(0, dots(lambda rows: (acc[rows, :] * cur[rows, :],), 1))

        @pl.when(j == 0)
        def _():
            for c in range(1, CHUNKS):
                net.drain_sends(left_view, net.at(c))

        @pl.when(later)
        def _():
            @pl.loop(0, CHUNKS)
            def _(ch):
                net.drain_sends(vec_view, net.at(ch))

        @pl.when(j == 0)
        def _():
            betas[0, LANCZOS_STEPS + 1] = total_of(0, 1)[0] * (CHUNKS / (CHUNKS - 1))

        shift = betas[0, LANCZOS_STEPS + 1]

        def products(rows):
            v, v_prev = cur[rows, :], prev[rows, :]
            w = acc[rows, :] - shift * v - beta_prev * v_prev
            acc[rows, :] = w
            return w * w, w * v, v * v, v * v_prev

        send_partial(1, dots(products, 4))

        @pl.when(later)
        def _():
            finish_out(turned, j - 1)

        @pl.when(j + 1 == LANCZOS_STEPS)
        def _():
            turn(acc, turned)
            own_copy(turned, j).start()
            send_out(turned, j, (14, 15, 6, 12, 10, 7, 13, 11, 2, 4, 8, 3, 5, 9, 1), 1)

        ww, wv, vv, vp = total_of(1, 4)
        alpha = wv + shift * vv + beta_prev * vp
        extra = alpha - shift
        beta = jnp.sqrt(ww - 2.0 * extra * wv + extra * extra * vv)
        alphas[0, j] = alpha
        betas[0, j] = beta
        betas[0, LANCZOS_STEPS] = extra
        betas[0, LANCZOS_STEPS + 1] = alpha

        @pl.when(j + 1 < LANCZOS_STEPS)
        def _():
            next_vector(0, extra, beta)
            net.own_out(vec_view, net.at(0))

            @pl.loop(1, CHUNKS)
            def _(ch):
                next_vector(ch, extra, beta)

        return beta

    def all_steps(zb, turned):
        lax.fori_loop(0, LANCZOS_STEPS, functools.partial(step, zb, turned), jnp.zeros((), f32))
        finish_out(turned, LANCZOS_STEPS - 1, 1)

    pl.run_scoped(all_steps, pltpu.VMEM((8, BOND, 256), bf), pltpu.VMEM((BOND, BOND), f32))


def run_lanczos(most, table, u_hbm, slab_hbm, wi_hbm, right_hbm, first_left, left_loc):
    smem = pl.BlockSpec(memory_space=pltpu.SMEM)
    hbm = pl.BlockSpec(memory_space=pltpu.HBM)
    dma = pltpu.SemaphoreType.DMA
    return pl.pallas_call(
        functools.partial(lanczos_kernel, most),
        out_shape=(jax.ShapeDtypeStruct((LANCZOS_STEPS, DEVS, SLAB, BOND), f32), jax.ShapeDtypeStruct((1, 8), f32), jax.ShapeDtypeStruct((1, 8), f32)),
        in_specs=[smem] + [hbm] * 6,
        out_specs=(hbm, smem, smem),
        scratch_shapes=[
            pltpu.VMEM(VECTOR_SHAPE, bf),
            pltpu.VMEM((2, 2, 2, 2, 2, BOND, BOND), bf),
            pltpu.VMEM((PAIR, TERMS + 1, SLAB, LANES), bf),
            pltpu.VMEM((BOND, BOND), f32),
            pltpu.VMEM((BOND, BOND), f32),
            pltpu.VMEM((BOND, BOND), f32),
            pltpu.VMEM((2, DEVS, 8, LANES), f32),
            pltpu.VMEM((most * SLAB, 1024), bf),
            pltpu.VMEM((DEVS, 2, 256, 256), bf),
            dma((5 + CHUNKS,)), dma, dma((CHUNKS, 3, 7)), dma((CHUNKS, 3, 7)), dma((CHUNKS, 8)), dma((CHUNKS, 8)),
            dma((2, DEVS)), dma((2, DEVS)), dma((DEVS,)), dma((2, DEVS)),
        ],
        compiler_params=pltpu.CompilerParams(collective_id=most, has_side_effects=True, vmem_limit_bytes=67043328),
    )(table, u_hbm, slab_hbm, wi_hbm, right_hbm, first_left, left_loc)


def place_kernel(alphas, betas, norm_hbm, psi, gathered, krylov, alpha_out, beta_out, norm, rows, src, dst, load_sem, store_sem):
    me = lax.axis_index(AXIS_NAME)

    def load(vec):
        return pltpu.make_async_copy(gathered.at[vec], src.at[vec], load_sem.at[vec])

    def store(vec):
        return pltpu.make_async_copy(dst.at[vec], krylov.at[vec], store_sem.at[vec])

    def placed(vec, r, q):
        lane = iota((8, LANES), 1)
        tiles = []
        for t in range(5):
            tile = None
            for m in range(128 * t // SLAB, min(DEVS, (128 * t + 127) // SLAB + 1)):
                val = src[vec, (m - q) % DEVS, pl.ds(r, 8), 128 * t:128 * t + 128]
                tile = val if tile is None else jnp.where(lane >= SLAB * m - 128 * t, val, tile)
            tiles.append(tile)
        skip, rest = SLAB * q // 128, SLAB * q % 128
        if rest:
            tiles = [pltpu.roll(tile, 128 - rest, 1) for tile in tiles]
        return [tiles[(t + skip) % 5] if not rest else jnp.where(lane < 128 - rest, tiles[(t + skip) % 5], tiles[(t + skip + 1) % 5]) for t in range(5)]

    def blocks(vec):
        for r in range(0, SLAB, 8):
            for half in range(0, PAIR, 8):
                found = [placed(vec, r, q) for q in range(half, half + 8)]
                for t in range(5):
                    block = jnp.stack([tiles[t] for tiles in found], axis=0).transpose(1, 0, 2)
                    yield (slice(r, r + 8), slice(half, half + 8), slice(128 * t, 128 * t + 128)), block

    rows_load = pltpu.make_async_copy(psi.at[pl.ds(me * SLAB, SLAB)], rows, load_sem.at[LANCZOS_STEPS])
    rows_load.start()
    norm_load = pltpu.make_async_copy(norm_hbm, norm, load_sem.at[LANCZOS_STEPS + 1])
    norm_load.start()
    for vec in range(LANCZOS_STEPS):
        load(vec).start()
    for n in range(LANCZOS_STEPS):
        alpha_out[n] = alphas[0, n]
        beta_out[n] = betas[0, n]
    rows_load.wait()
    norm_load.wait()
    dst[0] = rows[...] / norm[0, 0]
    store(0).start()

    @pl.loop(0, LANCZOS_STEPS - 1)
    def _(vec):
        load(vec).wait()
        for at, block in blocks(vec):
            dst[(vec + 1,) + at] = block
        store(vec + 1).start()

    load(LANCZOS_STEPS - 1).wait()
    for at, block in blocks(LANCZOS_STEPS - 1):
        dst[(LANCZOS_STEPS,) + at] = (block - betas[0, LANCZOS_STEPS] * dst[(LANCZOS_STEPS - 1,) + at]) / betas[0, LANCZOS_STEPS - 1]
    store(LANCZOS_STEPS).start()
    for vec in range(LANCZOS_STEPS + 1):
        store(vec).wait()


def place_outputs(norm, alphas, betas, wavefunction, gathered):
    smem = pl.BlockSpec(memory_space=pltpu.SMEM)
    hbm = pl.BlockSpec(memory_space=pltpu.HBM)
    dma = pltpu.SemaphoreType.DMA
    return pl.pallas_call(
        place_kernel,
        out_shape=(jax.ShapeDtypeStruct((LANCZOS_STEPS + 1, SLAB, PAIR, BOND), f32), jax.ShapeDtypeStruct((LANCZOS_STEPS,), f32), jax.ShapeDtypeStruct((LANCZOS_STEPS,), f32)),
        in_specs=[smem, smem, hbm, hbm, hbm],
        out_specs=(hbm, smem, smem),
        scratch_shapes=[
            pltpu.SMEM((8, LANES), f32),
            pltpu.VMEM((SLAB, PAIR, BOND), f32),
            pltpu.VMEM((LANCZOS_STEPS, DEVS, SLAB, BOND), f32),
            pltpu.VMEM((LANCZOS_STEPS + 1, SLAB, PAIR, BOND), f32),
            dma((LANCZOS_STEPS + 2,)), dma((LANCZOS_STEPS + 1,)),
        ],
        compiler_params=pltpu.CompilerParams(vmem_limit_bytes=67043328),
    )(alphas, betas, norm, wavefunction, gathered)


def solution(mesh):
    def device_body(wavefunction, left_loc, pair_loc, right_loc, flag_loc):
        table, few, norm, *operands = prepare(flag_loc, wavefunction, pair_loc, right_loc, left_loc)
        kernels = [functools.partial(run_lanczos, most) for most in (TERMS, FEW, FEWER)]
        vecs, alphas, betas = lax.switch(few[0], kernels, table, *operands, left_loc)
        return place_outputs(norm, alphas, betas, wavefunction, vecs)

    return jax.shard_map(device_body, mesh=mesh, in_specs=(P(), P(AXIS_NAME), P(AXIS_NAME), P(AXIS_NAME), P(AXIS_NAME)), out_specs=(P(None, AXIS_NAME), P(), P()), check_vma=False)
```

```python
import functools
import jax
import jax.numpy as jnp
from jax import lax
from jax.experimental import pallas as pl
from jax.sharding import PartitionSpec as P
from jax.experimental.pallas import tpu as pltpu

LANCZOS_STEPS = 6
AXIS_NAME = 'terms'
BOND = 640
PAIR = 16
TERMS = 32
DEVS = 16
SLAB = BOND // DEVS
CHUNKS = 5
FEWER, FEW = 20, 24
TABLE_ROW = {20: 0, 24: 2, 32: 3}
LANES = 128
VEC_SIZE = BOND * PAIR * BOND
bf = jnp.bfloat16
f32 = jnp.float32
MESH = pl.DeviceIdType.MESH
PART_PAIRS = ((0, 3), (3, 6), (6, 8))
LEFT_ROWS = ((0, 48), (48, 96), (96, 128))
AXES = ((1, 0, 0), (0, 1, 0), (0, 0, 1))
D2D_FLIPS = ((0,), (1,), (2,), (0, 1), (0, 2), (1, 2), (0, 1, 2), ())


def entry_barrier(me):
    barrier = pltpu.get_barrier_semaphore()
    for off in range(1, DEVS):
        pl.semaphore_signal(barrier, inc=1, device_id=(lax.rem(me + off, DEVS),), device_id_type=MESH)
    pl.semaphore_wait(barrier, DEVS - 1)


def iota(shape, dim):
    return lax.broadcasted_iota(jnp.int32, shape, dim)


def remote(ref, dst_ref, send, recv, dev):
    return pltpu.make_async_remote_copy(src_ref=ref, dst_ref=dst_ref, send_sem=send, recv_sem=recv, device_id=(dev,), device_id_type=MESH)


class Spot:
    def __init__(self, net, ch):
        self.ch = ch
        self.hits, self.across = [], []
        for n in range(3):
            axis = (n + ch) % 3 if isinstance(ch, int) else lax.rem(n + ch, 3)
            one = axis * (2 - axis)
            two = axis * (axis - 1) // 2 if isinstance(ch, int) else lax.div(axis * (axis - 1), 2)
            hit = (1 - one - two, one, two)
            self.hits.append(hit)
            self.across.append(net.me + hit[0] * net.step[0] + hit[1] * net.step[1] + hit[2] * net.step[2])


class Gather:
    def __init__(self, me, ici_send, ici_recv, d2d_send, d2d_recv):
        self.me, self.sems = me, (ici_send, ici_recv, d2d_send, d2d_recv)
        self.core = lax.rem(me, 2)
        self.place = (lax.rem(lax.div(me, 2), 2), lax.rem(lax.div(me, 4), 2), lax.div(me, 8))
        self.turn = tuple(1 - 2 * at for at in self.place)
        self.step = tuple((2 << n) * turn for n, turn in enumerate(self.turn))
        self.partner = me + 1 - 2 * self.core

    def at(self, ch):
        return Spot(self, ch)

    def slots(self, hits):
        idx = []
        for n in (2, 1, 0):
            moved = self.place[n]
            for hit in hits:
                if not isinstance(hit[n], int) or hit[n]:
                    moved = moved + hit[n] * self.turn[n]
            idx.append(moved)
        return tuple(idx) + (self.core,)

    def unit(self, view, spot, part, n, arriving=False):
        flips, axis = (((), 0), ((), 1), ((), 2), ((0,), 1), ((0,), 2), ((1,), 2), ((0, 1), 2))[n]
        hits = [spot.hits[(part + m) % 3] for m in (flips + (axis,) if arriving else flips)]
        ref = view(spot.ch, part, hits)
        return remote(ref, ref, self.sems[0].at[spot.ch, part, n], self.sems[1].at[spot.ch, part, n], spot.across[(part + axis) % 3])

    def start_units(self, view, spot, *which):
        for n in which:
            for part in range(3):
                self.unit(view, spot, part, n).start()

    def wait_units(self, view, spot, *which):
        for n in which:
            for part in range(3):
                self.unit(view, spot, part, n, True).wait_recv()

    def d2d(self, view, spot, n):
        ref = view(spot.ch, 3, [AXES[m] for m in D2D_FLIPS[n]])
        return remote(ref, ref, self.sems[2].at[spot.ch, n], self.sems[3].at[spot.ch, n], self.partner)

    def own_out(self, view, spot):
        self.start_units(view, spot, 0, 1, 2)
        self.d2d(view, spot, 7).start()

    def relay_first(self, view, spot):
        for part in range(3):
            self.unit(view, spot, part, 0, True).wait_recv()
            self.unit(view, spot, part, 3).start()
        self.start_units(view, spot, 4)

    def relay_second(self, view, spot):
        for part in range(3):
            self.unit(view, spot, part, 1, True).wait_recv()
            self.unit(view, spot, part, 5).start()

    def relay_third(self, view, spot):
        self.wait_units(view, spot, 2)
        for n in (0, 1, 2):
            self.d2d(view, spot, n).start()

    def relay_last(self, view, spot):
        for part in range(3):
            self.unit(view, spot, part, 3, True).wait_recv()
            self.unit(view, spot, part, 6).start()

    def take_pairs(self, view, spot):
        self.wait_units(view, spot, 4, 5)
        for n in (3, 4, 5):
            self.d2d(view, spot, n).start()

    def take_last(self, view, spot):
        self.wait_units(view, spot, 6)
        self.d2d(view, spot, 6).start()

    def wait_d2d(self, view, spot, *which):
        for n in which:
            self.d2d(view, spot, n).wait_recv()

    def chunk_ready(self, view, spot):
        self.wait_d2d(view, spot, *range(8))

    def drain_sends(self, view, spot):
        for n in range(8):
            self.d2d(view, spot, n).wait_send()
        for n in range(7):
            for part in range(3):
                self.unit(view, spot, part, n).wait_send()


def prep_kernel(flags, psi, psi_rows, pair_loc, right_hbm, left_hbm, table, few, norm_out, u_hbm, slab_hbm, wi_hbm, right_out, left_out,
                u, y, moved, cur, seen, ops, wi, left, load_sem, stage_sem, out_sem, seen_send, seen_recv, op_send, op_recv, ici_send, ici_recv, d2d_send, d2d_recv, left_sem, small_i, small_f):
    me = lax.axis_index(AXIS_NAME)
    net = Gather(me, ici_send, ici_recv, d2d_send, d2d_recv)

    def left_view(ch, part, flips):
        lo, hi = LEFT_ROWS[part] if part < 3 else (0, 128)
        return left.at[net.slots(flips) + (slice(None), slice(lo, hi))]

    def dots(fn, count):
        def body(g, tots):
            vals = fn(pl.ds(pl.multiple_of(g * 32, 32), 32))
            out = []
            for n, val in enumerate(vals):
                two = [tots[2 * n], tots[2 * n + 1]]
                for r in range(4):
                    for c in range(5):
                        two[r % 2] = two[r % 2] + val[8 * r:8 * r + 8, 128 * c:128 * c + 128]
                out += two
            return tuple(out)
        tots = lax.fori_loop(0, 20, body, (jnp.zeros((8, LANES), f32),) * (2 * count))
        return [tots[2 * n] + tots[2 * n + 1] for n in range(count)]

    def spread_right():
        col = iota((BOND, 128), 0)
        source = (col * 1639) >> 16
        within = col - source * SLAB
        target = jnp.where(within < 32, source * 32 + within, 480 + source * 8 + within)
        for t in range(5):
            perm = (target == iota((BOND, 128), 1) + 128 * t).astype(f32).astype(bf)
            for k in range(2):
                rows = jnp.concatenate([y[n, BOND * k:BOND * k + BOND, :] for n in range(5)], axis=1)
                val = jnp.dot(rows, perm, preferred_element_type=f32).reshape(DEVS, SLAB, 128)
                if k == 0:
                    first = val
            moved[t] = jnp.concatenate([first[:, None], val[:, None]], axis=1).reshape(TERMS, SLAB, 128).astype(bf)

    def build_pairs():
        widen = ((iota((128, 256), 1) >> 4) == iota((128, 256), 0)).astype(bf)
        same = (iota((256, 256), 0) & 15) == (iota((256, 256), 1) & 15)

        @pl.loop(0, DEVS)
        def _(k):
            wide = []
            for t in range(2):
                tall = jnp.broadcast_to(ops[k, t].astype(f32)[:, None, :], (16, 16, 128)).reshape(256, 128).astype(bf)
                wide.append(jnp.where(same, jnp.dot(tall, widen, preferred_element_type=f32), 0.0))
            wi[k, 0] = wide[0].astype(bf)
            wi[k, 1] = wide[1].astype(bf)

    def tile_load(stage, t, ch, half):
        rows, qs = pl.ds(pl.multiple_of(128 * ch, 128), 128), pl.ds(pl.multiple_of(8 * half, 8), 8)
        return pltpu.make_async_copy(psi.at[rows, qs, 128 * t:128 * t + 128], stage.at[t], stage_sem.at[t])

    def vector_out(ch):
        return pltpu.make_async_copy(u.at[ch], u_hbm.at[ch], out_sem.at[ch])

    def start_vector(norm, stage, flip):
        base = (me * SLAB) // 128
        skip = pl.multiple_of(me * SLAB - base * 128, 8)
        for t in range(5):
            tile_load(stage, t, 0, 0).start()

        @pl.loop(0, 2 * CHUNKS)
        def _(it):
            ch, half = it // 2, lax.rem(it, 2)
            @pl.when(it == 3)
            def _():
                net.relay_first(left_view, net.at(0))

            @pl.when(it == 4)
            def _():
                net.relay_second(left_view, net.at(0))
                send_right(5, 10)

            @pl.when(it == 6)
            def _():
                net.relay_third(left_view, net.at(0))
                for n in (7, 0, 1, 2):
                    left_store(n).start()

            @pl.when(it == 8)
            def _():
                net.relay_last(left_view, net.at(0))
                send_right(10, 15)

            for t in range(5):
                tile_load(stage, t, ch, half).wait()

                @pl.when((base == t) | (base + 1 == t))
                def _():
                    rows = pl.ds(pl.multiple_of(128 * (t - base), 128), 128)
                    for q in range(8):
                        flip[q, rows, :] = stage[t, :, q, :].T

                for q in range(8):
                    val = (stage[t, :, q, :].T / norm).astype(bf)
                    for m in range(16):
                        src, piece = (16 * t + m) // 5, (16 * t + m) % 5
                        row = 64 + 8 * (q % 2) if piece == 4 else 32 * (q % 2) + 8 * piece
                        u[ch, 4 * half + q // 2, src // 8, src // 4 % 2, src // 2 % 2, src % 2, row:row + 8, :] = val[8 * m:8 * m + 8, :]

                @pl.when(it + 1 < 2 * CHUNKS)
                def _():
                    tile_load(stage, t, (it + 1) // 2, lax.rem(it + 1, 2)).start()

            lanes = pl.ds(pl.multiple_of(128 * ch, 128), 128)
            for q in range(8):
                val = flip[q, pl.ds(skip, SLAB), :] / norm
                row = 128 * half + 16 * q
                for start, piece, size in ((row, 0, 16), (256 + row, 16, 16), (512 + 64 * half + 8 * q, 32, 8)):
                    cur[pl.ds(pl.multiple_of(start, 8), size), lanes] = val[piece:piece + size, :]

            @pl.when(half == 1)
            def _():
                vector_out(ch).start()

    def left_store(n, other=False):
        at = net.slots([AXES[m] for m in D2D_FLIPS[n]])
        at = at[:3] + ((1 - net.core,) if other else at[3:])
        return pltpu.make_async_copy(left.at[at], left_out.at[at], left_sem.at[int(other), n])

    def seen_copy(off, dev, src):
        return remote(seen.at[src], seen.at[src], seen_send.at[off], seen_recv.at[src], dev)

    def pair_copy(off, dev, src):
        return remote(ops.at[src], ops.at[src], op_send.at[0, off], op_recv.at[0, src], dev)

    def right_copy(off, dev, src):
        return remote(moved.at[:, pl.ds(2 * dev, 2)], right_out.at[:, pl.ds(2 * src, 2)], op_send.at[1, off], op_recv.at[1, src], dev)

    def others():
        return [(off, lax.rem(me + off, DEVS)) for off in range(1, DEVS)]

    def send_right(first, last):
        for n in range(first, last):
            off = 3 * (n % 5) + n // 5 + 1
            right_copy(off, lax.rem(me + off, DEVS), me).start()

    slab_load = pltpu.make_async_copy(psi_rows.at[pl.ds(pl.multiple_of(me * BOND, 8), BOND)], cur, load_sem.at[0])
    left_load = pltpu.make_async_copy(left_hbm.at[:, 0:128], left.at[net.slots(())], load_sem.at[1])
    right_load = [pltpu.make_async_copy(right_hbm.at[:, 128 * n:128 * n + 128], y.at[n], load_sem.at[2 + n]) for n in range(5)]
    slab_load.start()
    left_load.start()
    for load in right_load:
        load.start()
    for t in range(2):
        ops[me, t] = jnp.concatenate([pair_loc[t].astype(f32), jnp.zeros((PAIR, LANES - PAIR), f32)], axis=1).astype(bf)
    entry_barrier(me)
    slab_load.wait()
    square, = dots(lambda rows: (cur[rows, :] * cur[rows, :],), 1)
    row = iota((8, LANES), 0)
    full = jnp.where(row == 1, flags[0], flags[1]).astype(f32)
    seen[me] = jnp.where(row == 0, jnp.sum(square, axis=0, keepdims=True), full)
    for off, dev in others():
        seen_copy(off, dev, me).start()
    for off, dev in others():
        pair_copy(off, dev, me).start()
    left_load.wait()
    net.own_out(left_view, net.at(0))
    for load in right_load:
        load.wait()
    spread_right()
    send_right(0, 5)
    own = pl.ds(2 * me, 2)
    right_own = pltpu.make_async_copy(moved.at[:, own], right_out.at[:, own], load_sem.at[0])
    right_own.start()
    for off, dev in others():
        seen_copy(off, dev, dev).wait_recv()
    norm = jnp.sqrt(jnp.sum(jnp.sum(seen[:, 0:1, :], axis=0)) / VEC_SIZE)
    small_f[...] = jnp.zeros((8, LANES), f32) + norm
    norm_store = pltpu.make_async_copy(small_f, norm_out, load_sem.at[6])
    norm_store.start()
    term, lane = iota((TERMS, LANES), 0), iota((TERMS, LANES), 1)
    full = jnp.concatenate([seen[src, 1:3, :] for src in range(DEVS)], axis=0)
    in_lanes = jnp.sum(jnp.where(term == lane, full, 0.0), axis=0, keepdims=True)
    rank = jnp.sum(jnp.where(term < lane, full, 0.0), axis=0, keepdims=True)
    rank_down = jnp.sum(jnp.where(lane < term, in_lanes, 0.0), axis=1, keepdims=True)
    holder = jnp.sum(jnp.where(rank_down == lane.astype(f32), full * term.astype(f32), 0.0), axis=0, keepdims=True)
    small_i[...] = jnp.where(row == 1, holder, jnp.where(in_lanes > 0.5, rank, jnp.where(row == 0, FEWER, jnp.where(row == 2, FEW, TERMS)).astype(f32))).astype(jnp.int32)
    count = jnp.sum(in_lanes)
    few[0] = jnp.where(count < FEWER + 0.5, 2, jnp.where(count < FEW + 0.5, 1, 0))
    table_store = pltpu.make_async_copy(small_i, table, load_sem.at[7])
    table_store.start()
    pl.run_scoped(functools.partial(start_vector, norm), pltpu.VMEM((5, 128, 8, LANES), f32), pltpu.VMEM((8, 256, LANES), f32))
    slab_out = pltpu.make_async_copy(cur, slab_hbm, load_sem.at[1])
    slab_out.start()
    for off, dev in others():
        pair_copy(off, dev, dev).wait_recv()
    build_pairs()
    wi_out = pltpu.make_async_copy(wi, wi_hbm, load_sem.at[2])
    wi_out.start()
    net.take_pairs(left_view, net.at(0))
    for n in (3, 4, 5):
        left_store(n).start()
    net.wait_d2d(left_view, net.at(0), 7, 0, 1, 2)
    for n in (7, 0, 1, 2):
        left_store(n, True).start()
    net.take_last(left_view, net.at(0))
    left_store(6).start()
    net.wait_d2d(left_view, net.at(0), 3, 4, 5, 6)
    for n in (3, 4, 5, 6):
        left_store(n, True).start()
    net.drain_sends(left_view, net.at(0))
    for off, dev in others():
        right_copy(off, dev, dev).wait_recv()
    for off, dev in others():
        seen_copy(off, dev, me).wait_send()
        pair_copy(off, dev, me).wait_send()
        right_copy(off, dev, me).wait_send()
    right_own.wait()
    slab_out.wait()
    wi_out.wait()
    norm_store.wait()
    table_store.wait()
    for n in range(8):
        left_store(n).wait()
        left_store(n, True).wait()
    for ch in range(CHUNKS):
        vector_out(ch).wait()


VECTOR_SHAPE = (CHUNKS, 8, 2, 2, 2, 2, 80, LANES)


def prepare(flags, psi, pair_loc, right_loc, left_loc):
    smem = pl.BlockSpec(memory_space=pltpu.SMEM)
    vmem = pl.BlockSpec(memory_space=pltpu.VMEM)
    hbm = pl.BlockSpec(memory_space=pltpu.HBM)
    dma = pltpu.SemaphoreType.DMA
    return pl.pallas_call(
        prep_kernel,
        out_shape=(
            jax.ShapeDtypeStruct((8, LANES), jnp.int32), jax.ShapeDtypeStruct((1,), jnp.int32), jax.ShapeDtypeStruct((8, LANES), f32),
            jax.ShapeDtypeStruct(VECTOR_SHAPE, bf), jax.ShapeDtypeStruct((BOND, BOND), f32),
            jax.ShapeDtypeStruct((DEVS, 2, 256, 256), bf), jax.ShapeDtypeStruct((5, TERMS, SLAB, LANES), bf), jax.ShapeDtypeStruct((2, 2, 2, 2, 2, 128, BOND), bf),
        ),
        in_specs=[smem, hbm, hbm, vmem, hbm, hbm],
        out_specs=(hbm, smem, hbm, hbm, hbm, hbm, hbm, hbm),
        scratch_shapes=[
            pltpu.VMEM(VECTOR_SHAPE, bf),
            pltpu.VMEM((5, 2 * BOND, LANES), bf),
            pltpu.VMEM((5, TERMS, SLAB, LANES), bf),
            pltpu.VMEM((BOND, BOND), f32),
            pltpu.VMEM((DEVS, 8, LANES), f32),
            pltpu.VMEM((DEVS, 2, PAIR, LANES), bf),
            pltpu.VMEM((DEVS, 2, 256, 256), bf),
            pltpu.VMEM((2, 2, 2, 2, 2, 128, BOND), bf),
            dma((8,)), dma((5,)), dma((CHUNKS,)), dma((DEVS,)), dma((DEVS,)), dma((2, DEVS)), dma((2, DEVS)),
            dma((1, 3, 7)), dma((1, 3, 7)), dma((1, 8)), dma((1, 8)), dma((2, 8)),
            pltpu.VMEM((8, LANES), jnp.int32), pltpu.VMEM((8, LANES), f32),
        ],
        compiler_params=pltpu.CompilerParams(collective_id=0, has_side_effects=True, vmem_limit_bytes=67043328),
    )(flags, psi, psi.reshape(BOND * PAIR, BOND), pair_loc, right_loc.reshape(2 * BOND, BOND), left_loc)


def lanczos_kernel(most, table, u_hbm, slab_hbm, wi_hbm, right_hbm, first_left, left_hbm, gathered, alphas, betas,
                   u, lft, y, acc, cur, prev, ar, rc, wi,
                   load_sem, own_sem, ici_send, ici_recv, d2d_send, d2d_recv, ar_send, ar_recv, out_send, out_recv):
    me = lax.axis_index(AXIS_NAME)
    net = Gather(me, ici_send, ici_recv, d2d_send, d2d_recv)
    core, place = net.core, net.place

    def vec_view(ch, part, flips):
        pairs = PART_PAIRS[part] if part < 3 else (0, 8)
        return u.at[(ch, slice(pairs[0], pairs[1])) + net.slots(flips)]

    def left_view(ch, part, flips):
        lo, hi = LEFT_ROWS[part] if part < 3 else (0, 128)
        return lft.at[net.slots(flips) + (slice(None), slice(128 * ch + lo, 128 * ch + hi), slice(128 * ch, BOND))]

    def for_left(ch, what):
        for c in range(CHUNKS):
            @pl.when(ch == c)
            def _():
                what(left_view, net.at(c))

    def send_partial(which, partials):
        row = iota((8, LANES), 0)
        tile = jnp.zeros((8, LANES), f32)
        for n, partial in enumerate(partials):
            tile = jnp.where(row == n, jnp.sum(partial, axis=0, keepdims=True), tile)
        ar[which, me] = tile
        for off in range(1, DEVS):
            dev = lax.rem(me + off, DEVS)
            ref = ar.at[which, me]
            remote(ref, ref, ar_send.at[which, off], ar_recv.at[which, me], dev).start()

    def total_of(which, count):
        for off in range(1, DEVS):
            dev = lax.rem(me + off, DEVS)
            ref = ar.at[which, dev]
            remote(ref, ref, ar_send.at[which, off], ar_recv.at[which, dev], dev).wait_recv()
        total = jnp.sum(ar[which], axis=0)
        sums = [jnp.sum(total[n:n + 1]) / VEC_SIZE for n in range(count)]
        for off in range(1, DEVS):
            dev = lax.rem(me + off, DEVS)
            ref = ar.at[which, me]
            remote(ref, ref, ar_send.at[which, off], ar_recv.at[which, me], dev).wait_send()
        return sums

    def dots(fn, count):
        def body(g, tots):
            vals = fn(pl.ds(pl.multiple_of(g * 32, 32), 32))
            out = []
            for n, val in enumerate(vals):
                two = [tots[2 * n], tots[2 * n + 1]]
                for r in range(4):
                    for c in range(5):
                        two[r % 2] = two[r % 2] + val[8 * r:8 * r + 8, 128 * c:128 * c + 128]
                out += two
            return tuple(out)
        tots = lax.fori_loop(0, 20, body, (jnp.zeros((8, LANES), f32),) * (2 * count))
        return [tots[2 * n] + tots[2 * n + 1] for n in range(count)]

    def next_vector(ch, extra, beta):
        lanes = pl.ds(pl.multiple_of(128 * ch, 128), 128)
        for i in range(8):
            dst = u.at[ch, i, place[2], place[1], place[0], core]
            for n, start in enumerate((32 * i, 256 + 32 * i, 32 * i + 16, 256 + 32 * i + 16, 512 + 16 * i)):
                v = cur[start:start + 16, lanes]
                new = (acc[start:start + 16, lanes] - extra * v) / beta
                prev[start:start + 16, lanes] = v
                cur[start:start + 16, lanes] = new
                dst[16 * n:16 * n + 16] = new.astype(bf)

    def right_part(ch, par, pairs):
        rhs = []
        for i in pairs:
            main = u[ch, i, :, :, :, :, 32 * par:32 * par + 32, :].reshape(512, 128)
            tail = u[ch, i, :, :, :, :, 64:80, :].reshape(256, 128)
            rhs.append(jnp.concatenate([main, tail], axis=0))
        rhs = jnp.concatenate(rhs, axis=1)
        lhs = jnp.concatenate([rc[:, 0:512], rc[:, 512 + 256 * par:768 + 256 * par]], axis=1)
        val = jnp.dot(lhs, rhs, preferred_element_type=f32)
        for n, i in enumerate(pairs):
            y[2 * i + par, 0:most] = val[:, 128 * n:128 * n + 128].reshape(most, SLAB, 128).astype(bf)
            own = u.at[ch, i, place[2], place[1], place[0], core]
            y[2 * i + par, most, 0:32] = own[32 * par:32 * par + 32, :]
            y[2 * i + par, most, 32:40] = own[64 + 8 * par:72 + 8 * par, :]

    def right_phase(ch, middle):
        for par in range(2):
            if par == 1:
                middle()
            if most < TERMS:
                right_part(ch, par, range(8))
            else:
                @pl.loop(0, 8)
                def _(i):
                    right_part(ch, par, [i])

    def pair_left_phase(ch, zb, half_done):
        low_rows = (iota((256, 256), 0) & 15) < 8
        deep = 8 if most < TERMS else 2

        @pl.loop(0, DEVS // deep)
        def _(g):
            for s in range(deep):
                k = g * deep + s
                first, second = [table[TABLE_ROW[most], 2 * k + t] for t in range(2)]

                def tile(at, row):
                    return y[:, at, row:row + 16, :].reshape(256, 128)

                z01 = jnp.dot(wi[k, 0], jnp.concatenate([tile(first, 0), tile(first, 16)], axis=1), preferred_element_type=f32).astype(bf)
                mixed = jnp.where(low_rows, wi[k, 0], wi[k, 1])
                ends = jnp.concatenate([y[:, at, 32:40, :] for at in (first, second)], axis=1).reshape(256, 128)
                z2 = jnp.dot(mixed, ends, preferred_element_type=f32).reshape(16, 2, 8, 128)
                z34 = jnp.dot(wi[k, 1], jnp.concatenate([tile(second, 0), tile(second, 16)], axis=1), preferred_element_type=f32).astype(bf)
                zb[s, 0:256, 0:128] = z01[:, 0:128]
                zb[s, 256:512, 0:128] = z01[:, 128:256]
                zb[s, 512:640, 0:128] = z2[:, 0].reshape(128, 128).astype(bf)
                zb[s, 0:256, 128:256] = z34[:, 0:128]
                zb[s, 256:512, 128:256] = z34[:, 128:256]
                zb[s, 512:640, 128:256] = z2[:, 1].reshape(128, 128).astype(bf)
            lhs = jnp.concatenate([zb[s] for s in range(deep)], axis=1)
            rows = pl.ds(pl.multiple_of(ch * 128, 128), 128)
            rhs = []
            for s in range(deep):
                for t in range(2):
                    at = (g, s // 4, s // 2 % 2) if deep == 8 else (lax.div(g, 4), lax.rem(lax.div(g, 2), 2), lax.rem(g, 2))
                    rhs.append(lft[at + (s % 2, t, rows)])
            acc[...] += jnp.dot(lhs, jnp.concatenate(rhs, axis=0), preferred_element_type=f32)

            @pl.when(g == 8 // deep - 1)
            def _():
                half_done()

    def turn(vec, turned):
        shifted = [lax.rem(q + DEVS - me, DEVS) for q in range(PAIR)]
        for lt in range(5):
            rows = []
            for n in range(16 * lt, 16 * lt + 16):
                q, part = shifted[n // 5], n % 5
                start = 512 + 8 * q if part == 4 else 256 * (part // 2) + 16 * q + 8 * (part % 2)
                rows.append(vec[pl.ds(pl.multiple_of(start, 8), 8), :])
            turned[:, 128 * lt:128 * lt + 128] = jnp.concatenate(rows, axis=0).T

    def flipped(mask):
        dev = me
        for n, bit in enumerate((core,) + place):
            if mask >> n & 1:
                dev = dev + (1 << n) * (1 - 2 * bit)
        return dev

    def out_copy(turned, vec, mask, final, arriving=False):
        dev = flipped(mask)
        src = dev if arriving else me
        rows = pl.ds(pl.multiple_of(dev * SLAB, 8), SLAB)
        return remote(turned.at[rows], gathered.at[vec, src], out_send.at[mask], out_recv.at[final, mask], dev)

    def own_copy(turned, vec):
        rows = pl.ds(pl.multiple_of(me * SLAB, 8), SLAB)
        return pltpu.make_async_copy(turned.at[rows], gathered.at[vec, me], own_sem)

    def send_out(turned, vec, masks, final=0):
        for mask in masks:
            out_copy(turned, vec, mask, final).start()

    def finish_out(turned, vec, final=0):
        own_copy(turned, vec).wait()
        for mask in range(1, DEVS):
            out_copy(turned, vec, mask, final, True).wait_recv()
        for mask in range(1, DEVS):
            out_copy(turned, vec, mask, final).wait_send()

    def build_right():
        for n in range(most):
            for t in range(5):
                rc[SLAB * n:SLAB * n + SLAB, 128 * t:128 * t + 128] = y[t, table[1, n]]
        tails = rc[:, 512:640]
        src = iota((128, 256), 0)
        spot = 16 * (src >> 3) + (src & 7)
        for par in range(2):
            widen = (spot + 8 * par == iota((128, 256), 1)).astype(bf)
            rc[:, 512 + 256 * par:768 + 256 * par] = jnp.dot(tails, widen, preferred_element_type=f32).astype(bf)

    def mirror_left(ch):
        @pl.loop(0, 8)
        def _(g):
            for n in range(4):
                at = (g // 4, lax.rem(g // 2, 2), lax.rem(g, 2), n // 2, n % 2)
                for other in range(ch + 1, CHUNKS):
                    block = lft[at + (slice(128 * ch, 128 * ch + 128), slice(128 * other, 128 * other + 128))]
                    lft[at + (slice(128 * other, 128 * other + 128), slice(128 * ch, 128 * ch + 128))] = block.T

    left_load = pltpu.make_async_copy(left_hbm.at[:, 128:BOND], lft.at[net.slots(()) + (slice(None), slice(128, BOND))], load_sem.at[0])
    right_load = pltpu.make_async_copy(right_hbm, y.at[0:5, 0:TERMS], load_sem.at[1])
    wi_load = pltpu.make_async_copy(wi_hbm, wi, load_sem.at[2])
    slab_load = pltpu.make_async_copy(slab_hbm, cur, load_sem.at[3])
    first_load = pltpu.make_async_copy(first_left, lft.at[:, :, :, :, :, 0:128], load_sem.at[4])

    def vector_load(ch):
        return pltpu.make_async_copy(u_hbm.at[ch], u.at[ch], load_sem.at[5 + ch])

    left_load.start()
    right_load.start()
    vector_load(0).start()
    wi_load.start()
    first_load.start()
    for ch in range(1, CHUNKS):
        vector_load(ch).start()
    slab_load.start()
    entry_barrier(me)
    left_load.wait()
    net.own_out(left_view, net.at(1))
    right_load.wait()
    build_right()
    prev[...] = jnp.zeros_like(prev)

    def step(zb, turned, j, beta_prev):
        later = j > 0

        @pl.when(later)
        def _():
            zero, one = net.at(0), net.at(1)
            turn(cur, turned)
            own_copy(turned, j - 1).start()
            net.relay_first(vec_view, zero)
            net.relay_second(vec_view, zero)
            net.relay_last(vec_view, zero)
            net.own_out(vec_view, one)
            net.relay_third(vec_view, zero)
            net.take_pairs(vec_view, zero)
            net.take_last(vec_view, zero)
            net.relay_first(vec_view, one)
            net.chunk_ready(vec_view, zero)

        acc[...] = jnp.zeros_like(acc)

        @pl.loop(0, CHUNKS)
        def _(ch):
            next_spot, after_spot = net.at(ch + 1), net.at(ch + 2)

            @pl.when(later & (ch + 1 < CHUNKS))
            def _():
                net.relay_second(vec_view, next_spot)

            @pl.when(later & (ch == 4))
            def _():
                send_out(turned, j - 1, (7, 13, 11))

            @pl.when(j == 0)
            def _():
                vector_load(ch).wait()

            def middle():
                @pl.when(later & (ch + 1 < CHUNKS))
                def _():
                    net.relay_third(vec_view, next_spot)
                    net.relay_last(vec_view, next_spot)

                    @pl.when(ch + 2 < CHUNKS)
                    def _():
                        net.own_out(vec_view, after_spot)

                    @pl.when(ch == 3)
                    def _():
                        send_out(turned, j - 1, (1, 3, 5, 9, 14, 15))

                @pl.when((j == 0) & (ch > 0))
                def _():
                    def take(view, spot):
                        if spot.ch > 0:
                            mirror_left(spot.ch - 1)
                        net.take_pairs(view, spot)
                        net.take_last(view, spot)

                    for_left(ch, take)

            right_phase(ch, middle)

            @pl.when(j == 0)
            def _():
                @pl.when(ch == 0)
                def _():
                    wi_load.wait()
                    first_load.wait()

                def left_ready(view, spot):
                    if spot.ch > 0:
                        net.chunk_ready(view, spot)

                for_left(ch, left_ready)
                for_left(ch + 1, net.relay_first)

            def half_done():
                @pl.when(later & (ch + 1 < CHUNKS))
                def _():
                    net.take_pairs(vec_view, next_spot)
                    net.take_last(vec_view, next_spot)

                    @pl.when(ch + 2 < CHUNKS)
                    def _():
                        net.relay_first(vec_view, after_spot)

                    @pl.when(ch == 2)
                    def _():
                        send_out(turned, j - 1, (2, 4, 8))

                    @pl.when(ch == 3)
                    def _():
                        send_out(turned, j - 1, (6, 12, 10))

                @pl.when(j == 0)
                def _():
                    for_left(ch + 1, net.relay_second)

            pair_left_phase(ch, zb, half_done)

            @pl.when(later & (ch + 1 < CHUNKS))
            def _():
                net.chunk_ready(vec_view, next_spot)

            @pl.when(j == 0)
            def _():
                def advance(view, spot):
                    net.relay_third(view, spot)
                    net.relay_last(view, spot)

                for_left(ch + 1, advance)
                for_left(ch + 2, net.own_out)

                @pl.when(ch == CHUNKS - 2)
                def _():
                    slab_load.wait()
                    send_partial(0, dots(lambda rows: (acc[rows, :] * cur[rows, :],), 1))

        @pl.when(j == 0)
        def _():
            for c in range(1, CHUNKS):
                net.drain_sends(left_view, net.at(c))

        @pl.when(later)
        def _():
            @pl.loop(0, CHUNKS)
            def _(ch):
                net.drain_sends(vec_view, net.at(ch))

        @pl.when(j == 0)
        def _():
            betas[0, LANCZOS_STEPS + 1] = total_of(0, 1)[0] * (CHUNKS / (CHUNKS - 1))

        shift = betas[0, LANCZOS_STEPS + 1]

        def products(rows):
            v, v_prev = cur[rows, :], prev[rows, :]
            w = acc[rows, :] - shift * v - beta_prev * v_prev
            acc[rows, :] = w
            return w * w, w * v, v * v, v * v_prev

        send_partial(1, dots(products, 4))

        @pl.when(later)
        def _():
            finish_out(turned, j - 1)

        @pl.when(j + 1 == LANCZOS_STEPS)
        def _():
            turn(acc, turned)
            own_copy(turned, j).start()
            send_out(turned, j, (14, 15, 6, 12, 10, 7, 13, 11, 2, 4, 8, 3, 5, 9, 1), 1)

        ww, wv, vv, vp = total_of(1, 4)
        alpha = wv + shift * vv + beta_prev * vp
        extra = alpha - shift
        beta = jnp.sqrt(ww - 2.0 * extra * wv + extra * extra * vv)
        alphas[0, j] = alpha
        betas[0, j] = beta
        betas[0, LANCZOS_STEPS] = extra
        betas[0, LANCZOS_STEPS + 1] = alpha

        @pl.when(j + 1 < LANCZOS_STEPS)
        def _():
            next_vector(0, extra, beta)
            net.own_out(vec_view, net.at(0))

            @pl.loop(1, CHUNKS)
            def _(ch):
                next_vector(ch, extra, beta)

        return beta

    def all_steps(zb, turned):
        lax.fori_loop(0, LANCZOS_STEPS, functools.partial(step, zb, turned), jnp.zeros((), f32))
        finish_out(turned, LANCZOS_STEPS - 1, 1)

    pl.run_scoped(all_steps, pltpu.VMEM((8, BOND, 256), bf), pltpu.VMEM((BOND, BOND), f32))


def run_lanczos(most, table, u_hbm, slab_hbm, wi_hbm, right_hbm, first_left, left_loc):
    smem = pl.BlockSpec(memory_space=pltpu.SMEM)
    hbm = pl.BlockSpec(memory_space=pltpu.HBM)
    dma = pltpu.SemaphoreType.DMA
    return pl.pallas_call(
        functools.partial(lanczos_kernel, most),
        out_shape=(jax.ShapeDtypeStruct((LANCZOS_STEPS, DEVS, SLAB, BOND), f32), jax.ShapeDtypeStruct((1, 8), f32), jax.ShapeDtypeStruct((1, 8), f32)),
        in_specs=[smem] + [hbm] * 6,
        out_specs=(hbm, smem, smem),
        scratch_shapes=[
            pltpu.VMEM(VECTOR_SHAPE, bf),
            pltpu.VMEM((2, 2, 2, 2, 2, BOND, BOND), bf),
            pltpu.VMEM((PAIR, TERMS + 1, SLAB, LANES), bf),
            pltpu.VMEM((BOND, BOND), f32),
            pltpu.VMEM((BOND, BOND), f32),
            pltpu.VMEM((BOND, BOND), f32),
            pltpu.VMEM((2, DEVS, 8, LANES), f32),
            pltpu.VMEM((most * SLAB, 1024), bf),
            pltpu.VMEM((DEVS, 2, 256, 256), bf),
            dma((5 + CHUNKS,)), dma, dma((CHUNKS, 3, 7)), dma((CHUNKS, 3, 7)), dma((CHUNKS, 8)), dma((CHUNKS, 8)),
            dma((2, DEVS)), dma((2, DEVS)), dma((DEVS,)), dma((2, DEVS)),
        ],
        compiler_params=pltpu.CompilerParams(collective_id=most, has_side_effects=True, vmem_limit_bytes=67043328),
    )(table, u_hbm, slab_hbm, wi_hbm, right_hbm, first_left, left_loc)


def place_kernel(alphas, betas, norm_hbm, psi, gathered, krylov, alpha_out, beta_out, norm, rows, src, dst, load_sem, store_sem):
    me = lax.axis_index(AXIS_NAME)

    def load(vec):
        return pltpu.make_async_copy(gathered.at[vec], src.at[vec], load_sem.at[vec])

    def store(vec):
        return pltpu.make_async_copy(dst.at[vec], krylov.at[vec], store_sem.at[vec])

    def placed(vec, r, q):
        lane = iota((8, LANES), 1)
        tiles = []
        for t in range(5):
            tile = None
            for m in range(128 * t // SLAB, min(DEVS, (128 * t + 127) // SLAB + 1)):
                val = src[vec, (m - q) % DEVS, pl.ds(r, 8), 128 * t:128 * t + 128]
                tile = val if tile is None else jnp.where(lane >= SLAB * m - 128 * t, val, tile)
            tiles.append(tile)
        skip, rest = SLAB * q // 128, SLAB * q % 128
        if rest:
            tiles = [pltpu.roll(tile, 128 - rest, 1) for tile in tiles]
        return [tiles[(t + skip) % 5] if not rest else jnp.where(lane < 128 - rest, tiles[(t + skip) % 5], tiles[(t + skip + 1) % 5]) for t in range(5)]

    def blocks(vec):
        for r in range(0, SLAB, 8):
            for half in range(0, PAIR, 8):
                found = [placed(vec, r, q) for q in range(half, half + 8)]
                for t in range(5):
                    block = jnp.stack([tiles[t] for tiles in found], axis=0).transpose(1, 0, 2)
                    yield (slice(r, r + 8), slice(half, half + 8), slice(128 * t, 128 * t + 128)), block

    rows_load = pltpu.make_async_copy(psi.at[pl.ds(me * SLAB, SLAB)], rows, load_sem.at[LANCZOS_STEPS])
    rows_load.start()
    norm_load = pltpu.make_async_copy(norm_hbm, norm, load_sem.at[LANCZOS_STEPS + 1])
    norm_load.start()
    for vec in range(LANCZOS_STEPS):
        load(vec).start()
    for n in range(LANCZOS_STEPS):
        alpha_out[n] = alphas[0, n]
        beta_out[n] = betas[0, n]
    rows_load.wait()
    norm_load.wait()
    dst[0] = rows[...] / norm[0, 0]
    store(0).start()

    @pl.loop(0, LANCZOS_STEPS - 1)
    def _(vec):
        load(vec).wait()
        for at, block in blocks(vec):
            dst[(vec + 1,) + at] = block
        store(vec + 1).start()

    load(LANCZOS_STEPS - 1).wait()
    for at, block in blocks(LANCZOS_STEPS - 1):
        dst[(LANCZOS_STEPS,) + at] = (block - betas[0, LANCZOS_STEPS] * dst[(LANCZOS_STEPS - 1,) + at]) / betas[0, LANCZOS_STEPS - 1]
    store(LANCZOS_STEPS).start()
    for vec in range(LANCZOS_STEPS + 1):
        store(vec).wait()


def place_outputs(norm, alphas, betas, wavefunction, gathered):
    smem = pl.BlockSpec(memory_space=pltpu.SMEM)
    hbm = pl.BlockSpec(memory_space=pltpu.HBM)
    dma = pltpu.SemaphoreType.DMA
    return pl.pallas_call(
        place_kernel,
        out_shape=(jax.ShapeDtypeStruct((LANCZOS_STEPS + 1, SLAB, PAIR, BOND), f32), jax.ShapeDtypeStruct((LANCZOS_STEPS,), f32), jax.ShapeDtypeStruct((LANCZOS_STEPS,), f32)),
        in_specs=[smem, smem, hbm, hbm, hbm],
        out_specs=(hbm, smem, smem),
        scratch_shapes=[
            pltpu.SMEM((8, LANES), f32),
            pltpu.VMEM((SLAB, PAIR, BOND), f32),
            pltpu.VMEM((LANCZOS_STEPS, DEVS, SLAB, BOND), f32),
            pltpu.VMEM((LANCZOS_STEPS + 1, SLAB, PAIR, BOND), f32),
            dma((LANCZOS_STEPS + 2,)), dma((LANCZOS_STEPS + 1,)),
        ],
        compiler_params=pltpu.CompilerParams(vmem_limit_bytes=67043328),
    )(alphas, betas, norm, wavefunction, gathered)


def solution(mesh):
    def device_body(wavefunction, left_loc, pair_loc, right_loc, flag_loc):
        table, few, norm, *operands = prepare(flag_loc, wavefunction, pair_loc, right_loc, left_loc)
        kernels = [functools.partial(run_lanczos, most) for most in (TERMS, FEW, FEWER)]
        vecs, alphas, betas = lax.switch(few[0], kernels, table, *operands, left_loc)
        return place_outputs(norm, alphas, betas, wavefunction, vecs)

    return jax.shard_map(device_body, mesh=mesh, in_specs=(P(), P(AXIS_NAME), P(AXIS_NAME), P(AXIS_NAME), P(AXIS_NAME)), out_specs=(P(None, AXIS_NAME), P(), P()), check_vma=False)
```
